768 devices in a mesh: gx: 96 (over y, z_hi, x), gy: 8 (over z_lo, core).
Axes of the slice: x: 4, y: 8, z: 12 (z_hi: 3, z_lo: 4; z = z_hi * 4 + z_lo), core: 2. Of those that a mesh axis runs over, the one named last changes fastest.
Arguments:
- u_now_c: float32 [3, 192, 32, 128], P(None, 'gx', 'gy'), may hold values from -6 to 6
- u_prev_c: float32 [3, 192, 32, 128], P(None, 'gx', 'gy'), may hold values from -6 to 6
- memory_c: float32 [3, 3, 192, 32, 128], P(None, None, 'gx', 'gy'), may hold values from -3 to 3
- mu_c: float32 [192, 32, 128], P('gx', 'gy'), may hold values from 0.5 to 1.5
- lam_c: float32 [192, 32, 128], P('gx', 'gy'), may hold values from 0.5 to 1.5
- rho_c: float32 [192, 32, 128], P('gx', 'gy'), may hold values from 1 to 2
- q_c: float32 [3, 192, 32, 128], P(None, 'gx', 'gy'), may hold values from 0.05 to 0.4
- omega_c: float32 [3, 192, 32, 128], P(None, 'gx', 'gy'), may hold values from 0.1 to 8
- u_now_f: float32 [3, 384, 64, 128], P(None, 'gx', 'gy'), may hold values from -6 to 6
- u_prev_f: float32 [3, 384, 64, 128], P(None, 'gx', 'gy'), may hold values from -6 to 6
- memory_f: float32 [3, 3, 384, 64, 128], P(None, None, 'gx', 'gy'), may hold values from -3 to 3
- mu_f: float32 [384, 64, 128], P('gx', 'gy'), may hold values from 0.5 to 1.5
- lam_f: float32 [384, 64, 128], P('gx', 'gy'), may hold values from 0.5 to 1.5
- rho_f: float32 [384, 64, 128], P('gx', 'gy'), may hold values from 1 to 2
- q_f: float32 [3, 384, 64, 128], P(None, 'gx', 'gy'), may hold values from 0.05 to 0.4
- omega_f: float32 [3, 384, 64, 128], P(None, 'gx', 'gy'), may hold values from 0.1 to 8
- stretch_f: float32 [384, 64], P('gx', 'gy'), may hold values from 0.35 to 0.7
Outputs:
- u_out_c: float32 [3, 192, 32, 128], P(None, 'gx', 'gy')
- u_out_f: float32 [3, 384, 64, 128], P(None, 'gx', 'gy')
- memory_out_c: float32 [3, 3, 192, 32, 128], P(None, None, 'gx', 'gy')
- memory_out_f: float32 [3, 3, 384, 64, 128], P(None, None, 'gx', 'gy')
The draws below stay inside these ranges and needn't reach their ends.
All inputs are finite; a program needn't handle non-finite values.
Results may differ from the reference program's by a relative error of at most 0.0001.
Values sent between devices are 32-bit elements; how exact they have to be, the bound alone decides.
No kernel may reach another device: no remote copies, remote signals or barrier semaphores. Data moves between devices by JAX's collectives and lax.ppermute only.
A program may use at most 32 MiB of HBM per device.

```python
import math
import jax
import jax.numpy as jnp

NZC = 128
NZF = 128
STEPS = 2
NX = 192
NY = 32
FX = 384
FY = 64


def level_of(rng, dims, shards, smallest, largest):
    factor_of = 1.0
    for position, shards_of in shards:
        draws = jax.random.uniform(jax.random.fold_in(jax.random.fold_in(rng, 6), position), (shards_of,), jnp.float32, smallest / len(shards), largest / len(shards))
        factor_of = factor_of * jnp.repeat(jnp.exp(draws), dims[position] // shards_of).reshape((-1,) + (1,) * (len(dims) - 1 - position))
    return factor_of


def scatter_about(own_key, dims, deviation, bound, split=(), dtype=jnp.bfloat16):
    gain = level_of(own_key, dims, split, -0.22, 0.18) if split else 1.0
    array = jax.random.normal(own_key, dims, jnp.float32) * deviation * gain
    return jnp.minimum(jnp.maximum(array, -bound), bound).astype(dtype)


def setup_inputs(seed: int = 0) -> dict:
    seeds = jax.random.split(jax.random.key(seed), 18)
    return {
        "u_now_c": scatter_about(seeds[0], (3, NX, NY, NZC), 1.0, 6.0, ((1, 96), (2, 8)), jnp.float32),
        "u_prev_c": scatter_about(seeds[1], (3, NX, NY, NZC), 1.0, 6.0, ((1, 96), (2, 8)), jnp.float32),
        "memory_c": scatter_about(seeds[2], (3, 3, NX, NY, NZC), 0.5, 3.0, ((2, 96), (3, 8)), jnp.float32),
        "mu_c": jnp.clip(0.5 + 1.0 * jax.random.uniform(seeds[3], (NX, NY, NZC), jnp.float32) ** level_of(seeds[3], (NX, NY, NZC), ((0, 96), (1, 8)), -0.2, 0.2), 0.5, 1.5),
        "lam_c": jnp.clip(0.5 + 1.0 * jax.random.uniform(seeds[4], (NX, NY, NZC), jnp.float32) ** level_of(seeds[4], (NX, NY, NZC), ((0, 96), (1, 8)), -0.2, 0.2), 0.5, 1.5),
        "rho_c": jnp.clip(1.0 + 1.0 * jax.random.uniform(seeds[5], (NX, NY, NZC), jnp.float32) ** level_of(seeds[5], (NX, NY, NZC), ((0, 96), (1, 8)), -0.2, 0.2), 1.0, 2.0),
        "q_c": jnp.clip(jnp.exp(math.log(0.4) - 2.0794415 * jax.random.uniform(seeds[6], (3, NX, NY, NZC), jnp.float32) ** level_of(seeds[6], (3, NX, NY, NZC), ((1, 96), (2, 8)), -0.2, 0.2)), 0.05, 0.4),
        "omega_c": jnp.clip(jnp.exp(math.log(8.0) - 4.3820266 * jax.random.uniform(seeds[7], (3, NX, NY, NZC), jnp.float32) ** level_of(seeds[7], (3, NX, NY, NZC), ((1, 96), (2, 8)), -0.2, 0.2)), 0.1, 8.0),
        "u_now_f": scatter_about(seeds[8], (3, FX, FY, NZF), 1.0, 6.0, ((1, 96), (2, 8)), jnp.float32),
        "u_prev_f": scatter_about(seeds[9], (3, FX, FY, NZF), 1.0, 6.0, ((1, 96), (2, 8)), jnp.float32),
        "memory_f": scatter_about(seeds[10], (3, 3, FX, FY, NZF), 0.5, 3.0, ((2, 96), (3, 8)), jnp.float32),
        "mu_f": jnp.clip(0.5 + 1.0 * jax.random.uniform(seeds[11], (FX, FY, NZF), jnp.float32) ** level_of(seeds[11], (FX, FY, NZF), ((0, 96), (1, 8)), -0.2, 0.2), 0.5, 1.5),
        "lam_f": jnp.clip(0.5 + 1.0 * jax.random.uniform(seeds[12], (FX, FY, NZF), jnp.float32) ** level_of(seeds[12], (FX, FY, NZF), ((0, 96), (1, 8)), -0.2, 0.2), 0.5, 1.5),
        "rho_f": jnp.clip(1.0 + 1.0 * jax.random.uniform(seeds[13], (FX, FY, NZF), jnp.float32) ** level_of(seeds[13], (FX, FY, NZF), ((0, 96), (1, 8)), -0.2, 0.2), 1.0, 2.0),
        "q_f": jnp.clip(jnp.exp(math.log(0.4) - 2.0794415 * jax.random.uniform(seeds[14], (3, FX, FY, NZF), jnp.float32) ** level_of(seeds[14], (3, FX, FY, NZF), ((1, 96), (2, 8)), -0.2, 0.2)), 0.05, 0.4),
        "omega_f": jnp.clip(jnp.exp(math.log(8.0) - 4.3820266 * jax.random.uniform(seeds[15], (3, FX, FY, NZF), jnp.float32) ** level_of(seeds[15], (3, FX, FY, NZF), ((1, 96), (2, 8)), -0.2, 0.2)), 0.1, 8.0),
        "stretch_f": jnp.clip(0.35 + 0.35 * jax.random.uniform(seeds[16], (FX, FY), jnp.float32) ** level_of(seeds[16], (FX, FY), ((0, 96), (1, 8)), -0.2, 0.2), 0.35, 0.7),
    }


DT = 0.1


def restrict(plane):
    comps, wide, tall = plane.shape
    return plane.reshape(comps, wide // 2, 2, tall // 2, 2).mean(axis=(2, 4))


def prolong(plane):
    comps = plane.shape[0]
    even = 0.75 * plane[:, 1:-1] + 0.25 * plane[:, :-2]
    odd = 0.75 * plane[:, 1:-1] + 0.25 * plane[:, 2:]
    rows = jnp.stack([even, odd], axis=2).reshape(comps, -1, plane.shape[2])
    even = 0.75 * rows[:, :, 1:-1] + 0.25 * rows[:, :, :-2]
    odd = 0.75 * rows[:, :, 1:-1] + 0.25 * rows[:, :, 2:]
    return jnp.stack([even, odd], axis=3).reshape(comps, rows.shape[1], -1)


def coarse_extend(field_c, fine_plane):
    top = restrict(fine_plane)[..., None]
    return jnp.concatenate([top, field_c, jnp.zeros_like(top)], axis=3)


def fine_extend(field_f, coarse_padded):
    bottom = prolong(coarse_padded[..., 1])[..., None]
    return jnp.concatenate([field_f[..., :1], field_f, bottom], axis=3)


def shifted(padded, offx, offy, offz):
    sizes = padded.shape
    return padded[:, 1 + offx:sizes[1] - 1 + offx, 1 + offy:sizes[2] - 1 + offy, 1 + offz:sizes[3] - 1 + offz]


def mixed(padded, comp, first, second):
    plus_plus = [0, 0, 0]
    plus_plus[first] = 1
    plus_plus[second] = 1
    plus_minus = [0, 0, 0]
    plus_minus[first] = 1
    plus_minus[second] = -1
    minus_plus = [0, 0, 0]
    minus_plus[first] = -1
    minus_plus[second] = 1
    minus_minus = [0, 0, 0]
    minus_minus[first] = -1
    minus_minus[second] = -1
    total = shifted(padded[comp:comp + 1], *plus_plus) - shifted(padded[comp:comp + 1], *plus_minus)
    total = total - shifted(padded[comp:comp + 1], *minus_plus) + shifted(padded[comp:comp + 1], *minus_minus)
    return total[0]


def operator(padded, shear, lame, level_h, level_hz):
    across = level_h * level_h
    vertical = level_hz * level_hz
    center = shifted(padded, 0, 0, 0)
    dxx = (shifted(padded, 1, 0, 0) + shifted(padded, -1, 0, 0) - 2.0 * center) / across
    dyy = (shifted(padded, 0, 1, 0) + shifted(padded, 0, -1, 0) - 2.0 * center) / across
    dzz = (shifted(padded, 0, 0, 1) + shifted(padded, 0, 0, -1) - 2.0 * center) / vertical
    flat = 4.0 * across
    slant = 4.0 * level_h * level_hz
    grad_x = dxx[0] + mixed(padded, 1, 0, 1) / flat + mixed(padded, 2, 0, 2) / slant
    grad_y = mixed(padded, 0, 0, 1) / flat + dyy[1] + mixed(padded, 2, 1, 2) / slant
    grad_z = mixed(padded, 0, 0, 2) / slant + mixed(padded, 1, 1, 2) / slant + dzz[2]
    return shear * (dxx + dyy + dzz) + (lame + shear) * jnp.stack([grad_x, grad_y, grad_z])


def level_force(full, shear, lame, level_h, level_hz):
    force = operator(full[:3], shear, lame, level_h, level_hz)
    for mech in range(3):
        force = force - operator(full[3 + 3 * mech:6 + 3 * mech], shear, lame, level_h, level_hz)
    return force


def pad_sides(field):
    return jnp.pad(field, ((0, 0), (1, 1), (1, 1), (0, 0)))


def reference(u_now_c, u_prev_c, memory_c, mu_c, lam_c, rho_c, q_c, omega_c, u_now_f, u_prev_f, memory_f, mu_f, lam_f, rho_f, q_f, omega_f, stretch_f):
    height_f = stretch_f[:, :, None]
    for step in range(STEPS):
        prod_c = (q_c[:, None] * memory_c).reshape((9,) + u_now_c.shape[1:])
        prod_f = (q_f[:, None] * memory_f).reshape((9,) + u_now_f.shape[1:])
        field_c = jnp.concatenate([u_now_c, prod_c], axis=0)
        field_f = jnp.concatenate([u_now_f, prod_f], axis=0)
        full_c = pad_sides(coarse_extend(field_c, field_f[..., -1]))
        full_f = pad_sides(fine_extend(field_f, full_c))
        force_c = level_force(full_c, mu_c, lam_c, 1.0, 1.0)
        force_f = level_force(full_f, mu_f, lam_f, 0.5, height_f)
        next_c = 2.0 * u_now_c - u_prev_c + (DT * DT / rho_c) * force_c
        next_f = 2.0 * u_now_f - u_prev_f + (DT * DT / rho_f) * force_f
        memory_c = memory_c + DT * omega_c[:, None] * (u_now_c[None] - memory_c)
        memory_f = memory_f + DT * omega_f[:, None] * (u_now_f[None] - memory_f)
        u_prev_c, u_now_c = u_now_c, next_c
        u_prev_f, u_now_f = u_now_f, next_f
    return u_now_c, u_now_f, memory_c, memory_f
```

```python
import jax
import jax.numpy as jnp
from jax import lax
from jax.experimental import pallas as pl
from jax.experimental.pallas import tpu as pltpu
from jax.sharding import PartitionSpec as P

DT = 0.1
F32 = jnp.float32
LANES = 128

YT = 44
XT = 35


def lane_roll(tile, by):
    return pltpu.roll(tile, by % LANES, axis=1)


def row_roll(tile, by):
    return pltpu.roll(tile, by % tile.shape[0], axis=0)


def relax(u, mem, q, om):
    nxt = [[mem[l][c] + DT * om[l] * (u[c] - mem[l][c]) for c in range(3)] for l in range(3)]
    old = [sum(q[l] * mem[l][c] for l in range(3)) for c in range(3)]
    new = [sum(q[l] * nxt[l][c] for l in range(3)) for c in range(3)]
    return old, nxt, new


def pre_kernel(uc, pc, mc, muc, lamc, rhoc, qc, omc, uf, pf, mf, muf, lamf, rhof, qf, omf, st, out1, out2, own_f, own_c):
    even = lax.rem(lax.axis_index("gy"), 2) == 0
    eye = lax.broadcasted_iota(jnp.int32, (8, 8), 0) == lax.broadcasted_iota(jnp.int32, (8, 8), 1)

    def level(u_r, p_r, m_r, mu_r, lam_r, rho_r, q_r, om_r, own, wide):
        for x in range(wide):
            u = [u_r[c, x] for c in range(3)]
            mem = [[m_r[l, c, x] for c in range(3)] for l in range(3)]
            old, _, new = relax(u, mem, [q_r[l, x] for l in range(3)], [om_r[l, x] for l in range(3)])
            scale = (DT * DT) / rho_r[x]
            mu = mu_r[x]
            for c in range(3):
                own[c * wide + x] = u[c] - old[c]
                own[(3 + c) * wide + x] = 2.0 * u[c] - p_r[c, x] - new[c]
            own[6 * wide + x] = scale * mu
            own[7 * wide + x] = scale * (lam_r[x] + mu)

    level(uf, pf, mf, muf, lamf, rhof, qf, omf, own_f, 4)
    level(uc, pc, mc, muc, lamc, rhoc, qc, omc, own_c, 2)
    for x in range(4):
        row = jnp.broadcast_to(st[x : x + 1, :], (8, 8))
        col = jnp.sum(jnp.where(eye, row, 0.0), axis=1, keepdims=True)
        own_f[32 + x] = 1.0 / jnp.broadcast_to(col, (8, LANES))

    def message(out, up):
        for k in range(36):
            out[k] = own_f[k, 4:8] if up else own_f[k, 0:4]
        for f in range(8):
            for x in range(2):
                out[36 + f, 2 * x : 2 * x + 2] = own_c[2 * f + x, 2:4] if up else own_c[2 * f + x, 0:2]

    @pl.when(even)
    def _():
        message(out1, True)
        message(out2, False)

    @pl.when(jnp.logical_not(even))
    def _():
        message(out1, False)
        message(out2, True)


def mid_kernel(own_f, own_c, r1, r2, ext_f, ext_c, out1, out2):
    even_y = lax.rem(lax.axis_index("gy"), 2) == 0
    even_x = lax.rem(lax.axis_index("gx"), 2) == 0
    for k in range(36):
        ext_f[k, 0:8] = own_f[k]
    for k in range(16):
        ext_c[k, 0:4] = own_c[k]

    def place(above, below):
        for k in range(36):
            ext_f[k, 8:12] = above[k]
            ext_f[k, 12:16] = below[k]
        for f in range(8):
            for x in range(2):
                ext_c[2 * f + x, 4:6] = above[36 + f, 2 * x : 2 * x + 2]
                ext_c[2 * f + x, 6:8] = below[36 + f, 2 * x : 2 * x + 2]

    @pl.when(even_y)
    def _():
        place(r1, r2)

    @pl.when(jnp.logical_not(even_y))
    def _():
        place(r2, r1)

    lane = lax.broadcasted_iota(jnp.int32, (16, LANES), 1)

    def message(out, right):
        def col(ring):
            return 4 - ring if right else ring - 1

        near = 1 if right else 0
        for c in range(3):
            for x in range(2):
                out[2 * c + x] = ext_c[2 * c + x]
            out[6 + c] = ext_c[2 * (3 + c) + near]
        out[9] = ext_c[12 + near]
        out[10] = ext_c[14 + near]

        def put(k, tile):
            out[11 + 2 * k] = tile[0:8]
            out[12 + 2 * k] = tile[8:16]

        for c in range(3):
            put(c, ext_f[4 * c + col(1)])
            put(3 + c, ext_f[4 * c + col(2)])
            put(6 + c, ext_f[4 * (3 + c) + col(1)])
        put(9, ext_f[24 + col(1)])
        put(10, ext_f[28 + col(1)])
        bits = jnp.where(lane == 17, ext_f[32 + col(1)], ext_f[32 + col(2)])
        for c in range(3):
            for r in range(2):
                at = 4 * c + 2 * r
                both = jnp.logical_or(lane == at, lane == at + 1)
                bits = jnp.where(both, lane_roll(ext_f[4 * c + col(3 + r)], at + 2), bits)
            bits = jnp.where(lane == 12 + c, lane_roll(ext_f[4 * (3 + c) + col(2)], 13 + c), bits)
        bits = jnp.where(lane == 15, lane_roll(ext_f[24 + col(2)], 16), bits)
        bits = jnp.where(lane == 16, lane_roll(ext_f[28 + col(2)], 17), bits)
        put(11, bits)

    @pl.when(even_x)
    def _():
        message(out1, True)
        message(out2, False)

    @pl.when(jnp.logical_not(even_x))
    def _():
        message(out1, False)
        message(out2, True)


def operator(w, zp, zm, x, inv_h2, inv_flat, inv_slant, inv_hz2):
    def dz(c, at):
        return zp[c, at] - zm[c, at]

    def up(tile):
        return row_roll(tile, -1)

    def down(tile):
        return row_roll(tile, 1)

    def dy(c, at):
        return up(w[c, at]) - down(w[c, at])

    dxx = [w[c, x + 1] + w[c, x - 1] - 2.0 * w[c, x] for c in range(3)]
    dyy = [up(w[c, x]) + down(w[c, x]) - 2.0 * w[c, x] for c in range(3)]
    dzz = [zp[c, x] + zm[c, x] - 2.0 * w[c, x] for c in range(3)]
    lap = [(dxx[c] + dyy[c]) * inv_h2 + dzz[c] * inv_hz2 for c in range(3)]
    yz = [up(dz(c, x)) - down(dz(c, x)) for c in (1, 2)]
    grad = [
        dxx[0] * inv_h2 + (dy(1, x + 1) - dy(1, x - 1)) * inv_flat + (dz(2, x + 1) - dz(2, x - 1)) * inv_slant,
        (dy(0, x + 1) - dy(0, x - 1)) * inv_flat + dyy[1] * inv_h2 + yz[1] * inv_slant,
        (dz(0, x + 1) - dz(0, x - 1) + yz[0]) * inv_slant + dzz[2] * inv_hz2,
    ]
    return lap, grad


def post_kernel(ext_f, ext_c, r1, r2, uc, mc, qc, omc, uf, mf, qf, omf, uc_out, uf_out, mc_out, mf_out, halo, scr):
    gx, gy = lax.axis_index("gx"), lax.axis_index("gy")
    even_x = lax.rem(gx, 2) == 0

    @pl.when(even_x)
    def _():
        halo[0] = r2[...]
        halo[1] = r1[...]

    @pl.when(jnp.logical_not(even_x))
    def _():
        halo[0] = r1[...]
        halo[1] = r2[...]

    slots = [0]

    def slot():
        slots[0] += 1
        return slots[0] - 1

    lane_f = lax.broadcasted_iota(jnp.int32, (16, LANES), 1)
    lane_c = lax.broadcasted_iota(jnp.int32, (8, LANES), 1)
    row = lax.broadcasted_iota(jnp.int32, (16, LANES), 0)
    outside_y = jnp.logical_or(
        jnp.logical_and(row >= 12, gy == 0),
        jnp.logical_and(jnp.logical_and(row >= 8, row < 12), gy == lax.axis_size("gy") - 1),
    )
    keep_y = jnp.where(outside_y, 0.0, 1.0).astype(F32)
    keep_left = jnp.where(gx == 0, 0.0, 1.0).astype(F32)
    keep_right = jnp.where(gx == lax.axis_size("gx") - 1, 0.0, 1.0).astype(F32)

    def pair(side, k):
        return jnp.concatenate([halo[side, 11 + 2 * k], halo[side, 12 + 2 * k]], axis=0)

    wf, wc, af, ac, cf, cc, rz = {}, {}, {}, {}, {}, {}, {}
    for c in range(3):
        for x in range(4):
            wf[c, x] = ext_f[4 * c + x]
            af[c, x] = ext_f[4 * (3 + c) + x]
        for x in range(2):
            wc[c, x] = ext_c[2 * c + x]
            ac[c, x] = ext_c[2 * (3 + c) + x]
    for t in range(2):
        for x in range(4):
            cf[t, x] = ext_f[4 * (6 + t) + x]
        for x in range(2):
            cc[t, x] = ext_c[2 * (6 + t) + x]
    for x in range(4):
        rz[x] = ext_f[32 + x]
    for side in range(2):

        def col(ring):
            return 3 + ring if side else -ring

        bits = pair(side, 11)
        near = 2 if side else -1
        for c in range(3):
            for x in range(2):
                wc[c, (2 if side else -2) + x] = halo[side, 2 * c + x]
            ac[c, near] = halo[side, 6 + c]
            wf[c, col(1)] = pair(side, c)
            wf[c, col(2)] = pair(side, 3 + c)
            for r in range(2):
                wf[c, col(3 + r)] = lane_roll(bits, 126 - 4 * c - 2 * r)
            af[c, col(1)] = pair(side, 6 + c)
            af[c, col(2)] = lane_roll(bits, 115 - c)
        for t in range(2):
            cc[t, near] = halo[side, 9 + t]
            cf[t, col(1)] = pair(side, 9 + t)
            cf[t, col(2)] = lane_roll(bits, 112 - t)
            rz[col(1 + t)] = jnp.broadcast_to(bits[:, 17 + t : 18 + t], (16, LANES))

    def prolong(field, c, x):
        cx = x // 2
        tile = 0.75 * field[c, cx] + 0.25 * field[c, cx + 1 if x % 2 else cx - 1]
        at = slot()
        scr[at, pl.ds(0, 8, stride=2), :] = 0.75 * tile + 0.25 * row_roll(tile, 1)
        scr[at, pl.ds(1, 8, stride=2), :] = 0.75 * tile + 0.25 * row_roll(tile, -1)
        out = scr[at] * keep_y
        return out * keep_left if x < 0 else out * keep_right if x > 3 else out

    def restrict(field, c, cx):
        at = slot()
        scr[at] = field[c, 2 * cx] + field[c, 2 * cx + 1]
        return 0.25 * (scr[at, pl.ds(0, 8, stride=2), :] + scr[at, pl.ds(1, 8, stride=2), :])

    def neighbours(fine, coarse, reach_f, reach_c):
        zp_f, zm_f, zp_c, zm_c = {}, {}, {}, {}
        for c in range(3):
            for x in reach_f:
                tile = fine[c, x]
                zp_f[c, x] = jnp.where(lane_f == LANES - 1, lane_roll(prolong(coarse, c, x), -1), lane_roll(tile, -1))
                zm_f[c, x] = jnp.where(lane_f == 0, tile, lane_roll(tile, 1))
            for x in reach_c:
                tile = coarse[c, x]
                zp_c[c, x] = jnp.where(lane_c == LANES - 1, 0.0, lane_roll(tile, -1))
                zm_c[c, x] = jnp.where(lane_c == 0, lane_roll(restrict(fine, c, x), 1), lane_roll(tile, 1))
        return zp_f, zm_f, zp_c, zm_c

    zp_f, zm_f, zp_c, zm_c = neighbours(wf, wc, range(-3, 7), range(-2, 4))
    wf1, wc1 = {}, {}
    for x in range(-2, 6):
        lap, grad = operator(wf, zp_f, zm_f, x, 4.0, 1.0, 0.5 * rz[x], rz[x] * rz[x])
        for c in range(3):
            wf1[c, x] = af[c, x] + cf[0, x] * lap[c] + cf[1, x] * grad[c]
    for x in range(-1, 3):
        lap, grad = operator(wc, zp_c, zm_c, x, 1.0, 0.25, 0.25, 1.0)
        for c in range(3):
            wc1[c, x] = ac[c, x] + cc[0, x] * lap[c] + cc[1, x] * grad[c]

    zp_f, zm_f, zp_c, zm_c = neighbours(wf1, wc1, range(-1, 5), range(-1, 3))

    def finish(w1, lap, grad, c0, c1, u_r, m_r, q_r, om_r, u_out, m_out, x, tall):
        u = [u_r[c, x] for c in range(3)]
        om = [om_r[l, x] for l in range(3)]
        mem = [[m_r[l, c, x] for c in range(3)] for l in range(3)]
        _, nxt, new = relax(u, mem, [q_r[l, x] for l in range(3)], om)
        for c in range(3):
            u1 = w1[c, x][0:tall] + new[c]
            u_out[c, x] = 2.0 * u1 - u[c] + (c0 * lap[c] + c1 * grad[c])[0:tall]
            for l in range(3):
                m_out[l, c, x] = nxt[l][c] + DT * om[l] * (u1 - nxt[l][c])

    for x in range(4):
        lap, grad = operator(wf1, zp_f, zm_f, x, 4.0, 1.0, 0.5 * rz[x], rz[x] * rz[x])
        finish(wf1, lap, grad, cf[0, x], cf[1, x], uf, mf, qf, omf, uf_out, mf_out, x, 8)
    for x in range(2):
        lap, grad = operator(wc1, zp_c, zm_c, x, 1.0, 0.25, 0.25, 1.0)
        finish(wc1, lap, grad, cc[0, x], cc[1, x], uc, mc, qc, omc, uc_out, mc_out, x, 4)


SCRATCH = 3 * (10 + 6 + 6 + 4)


def swap(value, axis, first):
    pairs = []
    for i in range(first, lax.axis_size(axis) - 1, 2):
        pairs += [(i, i + 1), (i + 1, i)]
    return lax.ppermute(value, axis, pairs)


def call(kernel, shapes, scratch=()):
    vmem = pl.BlockSpec(memory_space=pltpu.VMEM)

    def run(*args):
        return pl.pallas_call(
            kernel,
            out_shape=[jax.ShapeDtypeStruct(s, F32) for s in shapes],
            in_specs=[vmem] * len(args),
            out_specs=[vmem] * len(shapes),
            scratch_shapes=list(scratch),
        )(*args)

    return run


def shards(
    u_now_c,
    u_prev_c,
    memory_c,
    mu_c,
    lam_c,
    rho_c,
    q_c,
    omega_c,
    u_now_f,
    u_prev_f,
    memory_f,
    mu_f,
    lam_f,
    rho_f,
    q_f,
    omega_f,
    stretch_f,
):
    up, down, own_f, own_c = call(pre_kernel, [(YT, 4, LANES)] * 2 + [(36, 8, LANES), (16, 4, LANES)])(
        u_now_c, u_prev_c, memory_c, mu_c, lam_c, rho_c, q_c, omega_c,
        u_now_f, u_prev_f, memory_f, mu_f, lam_f, rho_f, q_f, omega_f, stretch_f,
    )
    r2 = swap(down, "gy", 1)
    r1 = swap(up, "gy", 0)
    ext_f, ext_c, right, left = call(mid_kernel, [(36, 16, LANES), (16, 8, LANES)] + [(XT, 8, LANES)] * 2)(
        own_f, own_c, r1, r2
    )
    s2 = swap(left, "gx", 1)
    s1 = swap(right, "gx", 0)
    return tuple(
        call(
            post_kernel,
            [u_now_c.shape, u_now_f.shape, memory_c.shape, memory_f.shape],
            [pltpu.VMEM((2, XT, 8, LANES), F32), pltpu.VMEM((SCRATCH, 16, LANES), F32)],
        )(ext_f, ext_c, s1, s2, u_now_c, memory_c, q_c, omega_c, u_now_f, memory_f, q_f, omega_f)
    )


def solution(mesh):
    def level(*lead):
        return P(*lead, "gx", "gy", None)

    inputs = (level(None), level(None), level(None, None), level(), level(), level(), level(None), level(None))
    return jax.shard_map(
        shards,
        mesh=mesh,
        in_specs=inputs + inputs + (P("gx", "gy"),),
        out_specs=(level(None), level(None), level(None, None), level(None, None)),
        check_vma=False,
    )
```

```python
import jax
import jax.numpy as jnp
from jax import lax
from jax.experimental import pallas as pl
from jax.experimental.pallas import tpu as pltpu
from jax.sharding import PartitionSpec as P

DT = 0.1
F32 = jnp.float32
LANES = 128

YT = 44
XT = 35


def lane_roll(tile, by):
    return pltpu.roll(tile, by % LANES, axis=1)


def row_roll(tile, by):
    return pltpu.roll(tile, by % tile.shape[0], axis=0)


def relax(u, mem, q, om):
    nxt = [[mem[l][c] + DT * om[l] * (u[c] - mem[l][c]) for c in range(3)] for l in range(3)]
    old = [sum(q[l] * mem[l][c] for l in range(3)) for c in range(3)]
    new = [sum(q[l] * nxt[l][c] for l in range(3)) for c in range(3)]
    return old, nxt, new


def pre_kernel(uc, pc, mc, muc, lamc, rhoc, qc, omc, uf, pf, mf, muf, lamf, rhof, qf, omf, st, out1, out2, own_f, own_c):
    even = lax.rem(lax.axis_index("gy"), 2) == 0
    eye = lax.broadcasted_iota(jnp.int32, (8, 8), 0) == lax.broadcasted_iota(jnp.int32, (8, 8), 1)

    def level(u_r, p_r, m_r, mu_r, lam_r, rho_r, q_r, om_r, own, wide):
        for x in range(wide):
            u = [u_r[c, x] for c in range(3)]
            mem = [[m_r[l, c, x] for c in range(3)] for l in range(3)]
            old, _, new = relax(u, mem, [q_r[l, x] for l in range(3)], [om_r[l, x] for l in range(3)])
            scale = (DT * DT) / rho_r[x]
            mu = mu_r[x]
            for c in range(3):
                own[c * wide + x] = u[c] - old[c]
                own[(3 + c) * wide + x] = 2.0 * u[c] - p_r[c, x] - new[c]
            own[6 * wide + x] = scale * mu
            own[7 * wide + x] = scale * (lam_r[x] + mu)

    level(uf, pf, mf, muf, lamf, rhof, qf, omf, own_f, 4)
    level(uc, pc, mc, muc, lamc, rhoc, qc, omc, own_c, 2)
    for x in range(4):
        row = jnp.broadcast_to(st[x : x + 1, :], (8, 8))
        col = jnp.sum(jnp.where(eye, row, 0.0), axis=1, keepdims=True)
        own_f[32 + x] = 1.0 / jnp.broadcast_to(col, (8, LANES))

    def message(out, up):
        for k in range(36):
            out[k] = own_f[k, 4:8] if up else own_f[k, 0:4]
        for f in range(8):
            for x in range(2):
                out[36 + f, 2 * x : 2 * x + 2] = own_c[2 * f + x, 2:4] if up else own_c[2 * f + x, 0:2]

    @pl.when(even)
    def _():
        message(out1, True)
        message(out2, False)

    @pl.when(jnp.logical_not(even))
    def _():
        message(out1, False)
        message(out2, True)


def mid_kernel(own_f, own_c, r2, r1, ext_f, ext_c, out1, out2):
    even_y = lax.rem(lax.axis_index("gy"), 2) == 0
    even_x = lax.rem(lax.axis_index("gx"), 2) == 0
    for k in range(36):
        ext_f[k, 0:8] = own_f[k]
    for k in range(16):
        ext_c[k, 0:4] = own_c[k]

    def place(above, below):
        for k in range(36):
            ext_f[k, 8:12] = above[k]
            ext_f[k, 12:16] = below[k]
        for f in range(8):
            for x in range(2):
                ext_c[2 * f + x, 4:6] = above[36 + f, 2 * x : 2 * x + 2]
                ext_c[2 * f + x, 6:8] = below[36 + f, 2 * x : 2 * x + 2]

    @pl.when(even_y)
    def _():
        place(r1, r2)

    @pl.when(jnp.logical_not(even_y))
    def _():
        place(r2, r1)

    lane = lax.broadcasted_iota(jnp.int32, (16, LANES), 1)

    def message(out, right):
        def col(ring):
            return 4 - ring if right else ring - 1

        near = 1 if right else 0
        for c in range(3):
            for x in range(2):
                out[2 * c + x] = ext_c[2 * c + x]
            out[6 + c] = ext_c[2 * (3 + c) + near]
        out[9] = ext_c[12 + near]
        out[10] = ext_c[14 + near]

        def put(k, tile):
            out[11 + 2 * k] = tile[0:8]
            out[12 + 2 * k] = tile[8:16]

        for c in range(3):
            put(c, ext_f[4 * c + col(1)])
            put(3 + c, ext_f[4 * c + col(2)])
            put(6 + c, ext_f[4 * (3 + c) + col(1)])
        put(9, ext_f[24 + col(1)])
        put(10, ext_f[28 + col(1)])
        bits = jnp.where(lane == 17, ext_f[32 + col(1)], ext_f[32 + col(2)])
        for c in range(3):
            for r in range(2):
                at = 4 * c + 2 * r
                both = jnp.logical_or(lane == at, lane == at + 1)
                bits = jnp.where(both, lane_roll(ext_f[4 * c + col(3 + r)], at + 2), bits)
            bits = jnp.where(lane == 12 + c, lane_roll(ext_f[4 * (3 + c) + col(2)], 13 + c), bits)
        bits = jnp.where(lane == 15, lane_roll(ext_f[24 + col(2)], 16), bits)
        bits = jnp.where(lane == 16, lane_roll(ext_f[28 + col(2)], 17), bits)
        put(11, bits)

    @pl.when(even_x)
    def _():
        message(out1, True)
        message(out2, False)

    @pl.when(jnp.logical_not(even_x))
    def _():
        message(out1, False)
        message(out2, True)


def operator(w, zp, zm, x, inv_h2, inv_flat, inv_slant, inv_hz2):
    def dz(c, at):
        return zp[c, at] - zm[c, at]

    def up(tile):
        return row_roll(tile, -1)

    def down(tile):
        return row_roll(tile, 1)

    def dy(c, at):
        return up(w[c, at]) - down(w[c, at])

    dxx = [w[c, x + 1] + w[c, x - 1] - 2.0 * w[c, x] for c in range(3)]
    dyy = [up(w[c, x]) + down(w[c, x]) - 2.0 * w[c, x] for c in range(3)]
    dzz = [zp[c, x] + zm[c, x] - 2.0 * w[c, x] for c in range(3)]
    lap = [(dxx[c] + dyy[c]) * inv_h2 + dzz[c] * inv_hz2 for c in range(3)]
    yz = [up(dz(c, x)) - down(dz(c, x)) for c in (1, 2)]
    grad = [
        dxx[0] * inv_h2 + (dy(1, x + 1) - dy(1, x - 1)) * inv_flat + (dz(2, x + 1) - dz(2, x - 1)) * inv_slant,
        (dy(0, x + 1) - dy(0, x - 1)) * inv_flat + dyy[1] * inv_h2 + yz[1] * inv_slant,
        (dz(0, x + 1) - dz(0, x - 1) + yz[0]) * inv_slant + dzz[2] * inv_hz2,
    ]
    return lap, grad


def post_kernel(ext_f, ext_c, r2, r1, uc, mc, qc, omc, uf, mf, qf, omf, uc_out, uf_out, mc_out, mf_out, halo, scr):
    gx, gy = lax.axis_index("gx"), lax.axis_index("gy")
    even_x = lax.rem(gx, 2) == 0

    @pl.when(even_x)
    def _():
        halo[0] = r2[...]
        halo[1] = r1[...]

    @pl.when(jnp.logical_not(even_x))
    def _():
        halo[0] = r1[...]
        halo[1] = r2[...]

    slots = [0]

    def slot():
        slots[0] += 1
        return slots[0] - 1

    lane_f = lax.broadcasted_iota(jnp.int32, (16, LANES), 1)
    lane_c = lax.broadcasted_iota(jnp.int32, (8, LANES), 1)
    row = lax.broadcasted_iota(jnp.int32, (16, LANES), 0)
    outside_y = jnp.logical_or(
        jnp.logical_and(row >= 12, gy == 0),
        jnp.logical_and(jnp.logical_and(row >= 8, row < 12), gy == lax.axis_size("gy") - 1),
    )
    keep_y = jnp.where(outside_y, 0.0, 1.0).astype(F32)
    keep_left = jnp.where(gx == 0, 0.0, 1.0).astype(F32)
    keep_right = jnp.where(gx == lax.axis_size("gx") - 1, 0.0, 1.0).astype(F32)

    def pair(side, k):
        return jnp.concatenate([halo[side, 11 + 2 * k], halo[side, 12 + 2 * k]], axis=0)

    wf, wc, af, ac, cf, cc, rz = {}, {}, {}, {}, {}, {}, {}
    for c in range(3):
        for x in range(4):
            wf[c, x] = ext_f[4 * c + x]
            af[c, x] = ext_f[4 * (3 + c) + x]
        for x in range(2):
            wc[c, x] = ext_c[2 * c + x]
            ac[c, x] = ext_c[2 * (3 + c) + x]
    for t in range(2):
        for x in range(4):
            cf[t, x] = ext_f[4 * (6 + t) + x]
        for x in range(2):
            cc[t, x] = ext_c[2 * (6 + t) + x]
    for x in range(4):
        rz[x] = ext_f[32 + x]
    for side in range(2):

        def col(ring):
            return 3 + ring if side else -ring

        bits = pair(side, 11)
        near = 2 if side else -1
        for c in range(3):
            for x in range(2):
                wc[c, (2 if side else -2) + x] = halo[side, 2 * c + x]
            ac[c, near] = halo[side, 6 + c]
            wf[c, col(1)] = pair(side, c)
            wf[c, col(2)] = pair(side, 3 + c)
            for r in range(2):
                wf[c, col(3 + r)] = lane_roll(bits, 126 - 4 * c - 2 * r)
            af[c, col(1)] = pair(side, 6 + c)
            af[c, col(2)] = lane_roll(bits, 115 - c)
        for t in range(2):
            cc[t, near] = halo[side, 9 + t]
            cf[t, col(1)] = pair(side, 9 + t)
            cf[t, col(2)] = lane_roll(bits, 112 - t)
            rz[col(1 + t)] = jnp.broadcast_to(bits[:, 17 + t : 18 + t], (16, LANES))

    def prolong(field, c, x):
        cx = x // 2
        tile = 0.75 * field[c, cx] + 0.25 * field[c, cx + 1 if x % 2 else cx - 1]
        at = slot()
        scr[at, pl.ds(0, 8, stride=2), :] = 0.75 * tile + 0.25 * row_roll(tile, 1)
        scr[at, pl.ds(1, 8, stride=2), :] = 0.75 * tile + 0.25 * row_roll(tile, -1)
        out = scr[at] * keep_y
        return out * keep_left if x < 0 else out * keep_right if x > 3 else out

    def restrict(field, c, cx):
        at = slot()
        scr[at] = field[c, 2 * cx] + field[c, 2 * cx + 1]
        return 0.25 * (scr[at, pl.ds(0, 8, stride=2), :] + scr[at, pl.ds(1, 8, stride=2), :])

    def neighbours(fine, coarse, reach_f, reach_c):
        zp_f, zm_f, zp_c, zm_c = {}, {}, {}, {}
        for c in range(3):
            for x in reach_f:
                tile = fine[c, x]
                zp_f[c, x] = jnp.where(lane_f == LANES - 1, lane_roll(prolong(coarse, c, x), -1), lane_roll(tile, -1))
                zm_f[c, x] = jnp.where(lane_f == 0, tile, lane_roll(tile, 1))
            for x in reach_c:
                tile = coarse[c, x]
                zp_c[c, x] = jnp.where(lane_c == LANES - 1, 0.0, lane_roll(tile, -1))
                zm_c[c, x] = jnp.where(lane_c == 0, lane_roll(restrict(fine, c, x), 1), lane_roll(tile, 1))
        return zp_f, zm_f, zp_c, zm_c

    zp_f, zm_f, zp_c, zm_c = neighbours(wf, wc, range(-3, 7), range(-2, 4))
    wf1, wc1 = {}, {}
    for x in range(-2, 6):
        lap, grad = operator(wf, zp_f, zm_f, x, 4.0, 1.0, 0.5 * rz[x], rz[x] * rz[x])
        for c in range(3):
            wf1[c, x] = af[c, x] + cf[0, x] * lap[c] + cf[1, x] * grad[c]
    for x in range(-1, 3):
        lap, grad = operator(wc, zp_c, zm_c, x, 1.0, 0.25, 0.25, 1.0)
        for c in range(3):
            wc1[c, x] = ac[c, x] + cc[0, x] * lap[c] + cc[1, x] * grad[c]

    zp_f, zm_f, zp_c, zm_c = neighbours(wf1, wc1, range(-1, 5), range(-1, 3))

    def finish(w1, lap, grad, c0, c1, u_r, m_r, q_r, om_r, u_out, m_out, x, tall):
        u = [u_r[c, x] for c in range(3)]
        om = [om_r[l, x] for l in range(3)]
        mem = [[m_r[l, c, x] for c in range(3)] for l in range(3)]
        _, nxt, new = relax(u, mem, [q_r[l, x] for l in range(3)], om)
        for c in range(3):
            u1 = w1[c, x][0:tall] + new[c]
            u_out[c, x] = 2.0 * u1 - u[c] + (c0 * lap[c] + c1 * grad[c])[0:tall]
            for l in range(3):
                m_out[l, c, x] = nxt[l][c] + DT * om[l] * (u1 - nxt[l][c])

    for x in range(4):
        lap, grad = operator(wf1, zp_f, zm_f, x, 4.0, 1.0, 0.5 * rz[x], rz[x] * rz[x])
        finish(wf1, lap, grad, cf[0, x], cf[1, x], uf, mf, qf, omf, uf_out, mf_out, x, 8)
    for x in range(2):
        lap, grad = operator(wc1, zp_c, zm_c, x, 1.0, 0.25, 0.25, 1.0)
        finish(wc1, lap, grad, cc[0, x], cc[1, x], uc, mc, qc, omc, uc_out, mc_out, x, 4)


SCRATCH = 3 * (10 + 6 + 6 + 4)


def swap(value, axis, first):
    pairs = []
    for i in range(first, lax.axis_size(axis) - 1, 2):
        pairs += [(i, i + 1), (i + 1, i)]
    return lax.ppermute(value, axis, pairs)


def call(kernel, shapes, scratch=(), first=False, last=False):
    vmem = pl.BlockSpec(memory_space=pltpu.VMEM)

    def run(*args):
        if not first:
            args = [pltpu.with_memory_space_constraint(a, pltpu.VMEM) for a in args]
        return pl.pallas_call(
            kernel,
            out_shape=[(jax.ShapeDtypeStruct if last else pltpu.VMEM)(s, F32) for s in shapes],
            in_specs=[vmem] * len(args),
            out_specs=[vmem] * len(shapes),
            scratch_shapes=list(scratch),
        )(*args)

    return run


def shards(
    u_now_c,
    u_prev_c,
    memory_c,
    mu_c,
    lam_c,
    rho_c,
    q_c,
    omega_c,
    u_now_f,
    u_prev_f,
    memory_f,
    mu_f,
    lam_f,
    rho_f,
    q_f,
    omega_f,
    stretch_f,
):
    up, down, own_f, own_c = call(pre_kernel, [(YT, 4, LANES)] * 2 + [(36, 8, LANES), (16, 4, LANES)], first=True)(
        u_now_c, u_prev_c, memory_c, mu_c, lam_c, rho_c, q_c, omega_c,
        u_now_f, u_prev_f, memory_f, mu_f, lam_f, rho_f, q_f, omega_f, stretch_f,
    )
    r2 = swap(down, "gy", 1)
    r1 = swap(up, "gy", 0)
    ext_f, ext_c, right, left = call(mid_kernel, [(36, 16, LANES), (16, 8, LANES)] + [(XT, 8, LANES)] * 2)(
        own_f, own_c, r2, r1
    )
    s2 = swap(left, "gx", 1)
    s1 = swap(right, "gx", 0)
    return tuple(
        call(
            post_kernel,
            [u_now_c.shape, u_now_f.shape, memory_c.shape, memory_f.shape],
            [pltpu.VMEM((2, XT, 8, LANES), F32), pltpu.VMEM((SCRATCH, 16, LANES), F32)],
            last=True,
        )(ext_f, ext_c, s2, s1, u_now_c, memory_c, q_c, omega_c, u_now_f, memory_f, q_f, omega_f)
    )


def solution(mesh):
    def level(*lead):
        return P(*lead, "gx", "gy", None)

    inputs = (level(None), level(None), level(None, None), level(), level(), level(), level(None), level(None))
    return jax.shard_map(
        shards,
        mesh=mesh,
        in_specs=inputs + inputs + (P("gx", "gy"),),
        out_specs=(level(None), level(None), level(None, None), level(None, None)),
        check_vma=False,
    )
```

```python
import jax
import jax.numpy as jnp
from jax import lax
from jax.experimental import pallas as pl
from jax.experimental.pallas import tpu as pltpu
from jax.sharding import PartitionSpec as P

DT = 0.1
F32 = jnp.float32
LANES = 128

def layout(pieces):
    table, at = {}, 0
    for key, rows in pieces:
        table[key] = (at, rows)
        at += rows
    return table, -(-at // 8) * 8


X_AT, X_ROWS = layout(
    [(("f", c, r), 8) for r in (1, 2) for c in range(3)]
    + [(("f", f, 1), 8) for f in range(3, 8)]
    + [("bits", 8)]
    + [(("c", c, x), 4) for c in range(3) for x in range(2)]
    + [(("c", f, None), 4) for f in range(3, 8)]
)
Y_F = (
    [(("f", c, x), 4) for c in range(3) for x in range(-2, 6)]
    + [(("bits", side), 4) for side in range(2)]
    + [(("f", f, x), 2) for f in range(3, 8) for x in range(-1, 5)]
    + [(("f", 8, x), 2) for x in range(4)]
)
Y_C = [(("c", c, x), 2) for c in range(3) for x in range(-2, 4)] + [
    (("c", f, x), 2) for f in range(3, 8) for x in range(-1, 3)
]
Y_AT, Y_ROWS = layout(Y_F + Y_C)


def lane_roll(tile, by):
    return pltpu.roll(tile, by % LANES, axis=1)


def row_roll(tile, by):
    return pltpu.roll(tile, by % tile.shape[0], axis=0)


def relax(u, mem, q, om):
    nxt = [[mem[l][c] + DT * om[l] * (u[c] - mem[l][c]) for c in range(3)] for l in range(3)]
    old = [sum(q[l] * mem[l][c] for l in range(3)) for c in range(3)]
    new = [sum(q[l] * nxt[l][c] for l in range(3)) for c in range(3)]
    return old, nxt, new


def pre_kernel(uc, pc, mc, muc, lamc, rhoc, qc, omc, uf, pf, mf, muf, lamf, rhof, qf, omf, st, out1, out2, own_f, own_c):
    even = lax.rem(lax.axis_index("gx"), 2) == 0
    eye = lax.broadcasted_iota(jnp.int32, (8, 8), 0) == lax.broadcasted_iota(jnp.int32, (8, 8), 1)
    lane = lax.broadcasted_iota(jnp.int32, (8, LANES), 1)

    def level(u_r, p_r, m_r, mu_r, lam_r, rho_r, q_r, om_r, own, wide):
        for x in range(wide):
            u = [u_r[c, x] for c in range(3)]
            mem = [[m_r[l, c, x] for c in range(3)] for l in range(3)]
            old, _, new = relax(u, mem, [q_r[l, x] for l in range(3)], [om_r[l, x] for l in range(3)])
            scale = (DT * DT) / rho_r[x]
            mu = mu_r[x]
            for c in range(3):
                own[c * wide + x] = u[c] - old[c]
                own[(3 + c) * wide + x] = 2.0 * u[c] - p_r[c, x] - new[c]
            own[6 * wide + x] = scale * mu
            own[7 * wide + x] = scale * (lam_r[x] + mu)

    level(uf, pf, mf, muf, lamf, rhof, qf, omf, own_f, 4)
    level(uc, pc, mc, muc, lamc, rhoc, qc, omc, own_c, 2)
    for x in range(4):
        row = jnp.broadcast_to(st[x : x + 1, :], (8, 8))
        col = jnp.sum(jnp.where(eye, row, 0.0), axis=1, keepdims=True)
        own_f[32 + x] = 1.0 / jnp.broadcast_to(col, (8, LANES))

    def message(out, right):
        def fine(f, ring):
            return own_f[4 * f + (4 - ring if right else ring - 1)]

        for key, (at, rows) in X_AT.items():
            if key[0] == "f":
                out[at : at + rows] = fine(key[1], key[2])
            elif key[0] == "c":
                x = key[2]
                out[at : at + rows] = own_c[2 * key[1] + ((1 if right else 0) if x is None else x)]
        bits = jnp.where(lane == 17, fine(8, 1), fine(8, 2))
        for c in range(3):
            for r in range(2):
                to = 4 * c + 2 * r
                both = jnp.logical_or(lane == to, lane == to + 1)
                bits = jnp.where(both, lane_roll(fine(c, 3 + r), to + 2), bits)
        for f in range(3, 8):
            bits = jnp.where(lane == 9 + f, lane_roll(fine(f, 2), 10 + f), bits)
        at = X_AT["bits"][0]
        out[at : at + 8] = bits

    @pl.when(even)
    def _():
        message(out1, True)
        message(out2, False)

    @pl.when(jnp.logical_not(even))
    def _():
        message(out1, False)
        message(out2, True)


def mid_kernel(own_f, own_c, r2, r1, out2, out1):
    even_x = lax.rem(lax.axis_index("gx"), 2) == 0
    even_y = lax.rem(lax.axis_index("gy"), 2) == 0

    def message(out, up, left, right):
        for key, (at, rows) in Y_AT.items():
            fine = (8 - rows if up else 0), (8 if up else rows)
            coarse = (2, 4) if up else (0, 2)
            if key[0] == "bits":
                src = X_AT["bits"][0]
                out[at : at + rows] = (right if key[1] else left)[src + fine[0] : src + fine[1]]
                continue
            kind, f, x = key
            wide = 4 if kind == "f" else 2
            part = fine if kind == "f" else coarse
            if 0 <= x < wide:
                out[at : at + rows] = (own_f if kind == "f" else own_c)[wide * f + x, part[0] : part[1]]
            else:
                ring = -x if x < 0 else x - wide + 1
                if kind == "f":
                    src = X_AT["f", f, ring][0]
                else:
                    src = X_AT["c", f, x % 2 if f < 3 else None][0]
                out[at : at + rows] = (left if x < 0 else right)[src + part[0] : src + part[1]]

    for y_is_even in (True, False):
        for x_is_even in (True, False):

            @pl.when(jnp.logical_and(even_x == x_is_even, even_y == y_is_even))
            def _(y_is_even=y_is_even, x_is_even=x_is_even):
                left, right = (r2, r1) if x_is_even else (r1, r2)
                message(out1, y_is_even, left, right)
                message(out2, not y_is_even, left, right)


def operator(w, zp, zm, x, inv_h2, inv_flat, inv_slant, inv_hz2):
    def dz(c, at):
        return zp[c, at] - zm[c, at]

    def up(tile):
        return row_roll(tile, -1)

    def down(tile):
        return row_roll(tile, 1)

    def dy(c, at):
        return up(w[c, at]) - down(w[c, at])

    dxx = [w[c, x + 1] + w[c, x - 1] - 2.0 * w[c, x] for c in range(3)]
    dyy = [up(w[c, x]) + down(w[c, x]) - 2.0 * w[c, x] for c in range(3)]
    dzz = [zp[c, x] + zm[c, x] - 2.0 * w[c, x] for c in range(3)]
    lap = [(dxx[c] + dyy[c]) * inv_h2 + dzz[c] * inv_hz2 for c in range(3)]
    yz = [up(dz(c, x)) - down(dz(c, x)) for c in (1, 2)]
    grad = [
        dxx[0] * inv_h2 + (dy(1, x + 1) - dy(1, x - 1)) * inv_flat + (dz(2, x + 1) - dz(2, x - 1)) * inv_slant,
        (dy(0, x + 1) - dy(0, x - 1)) * inv_flat + dyy[1] * inv_h2 + yz[1] * inv_slant,
        (dz(0, x + 1) - dz(0, x - 1) + yz[0]) * inv_slant + dzz[2] * inv_hz2,
    ]
    return lap, grad


def post_kernel(
    own_f, own_c, x2, x1, y2, y1, uc, mc, qc, omc, uf, mf, qf, omf, uc_out, uf_out, mc_out, mf_out, hx, hy, ext_f, ext_c, scr
):
    gx, gy = lax.axis_index("gx"), lax.axis_index("gy")
    even_x = lax.rem(gx, 2) == 0
    even_y = lax.rem(gy, 2) == 0

    def sides(halo, first, second, even):
        @pl.when(even)
        def _():
            halo[0] = second[...]
            halo[1] = first[...]

        @pl.when(jnp.logical_not(even))
        def _():
            halo[0] = first[...]
            halo[1] = second[...]

    sides(hx, x1, x2, even_x)
    sides(hy, y1, y2, even_y)

    index = {}

    def extended(key, own):
        at, rows = Y_AT[key]
        if key[0] == "c":
            ext, tall, far = ext_c, 4, 8
        else:
            ext, tall, far = ext_f, 8, 16
        k = index.setdefault(key, len([i for i in index if (i[0] == "c") == (key[0] == "c")]))
        ext[k, 0:tall] = own
        ext[k, tall : tall + rows] = hy[1, at : at + rows]
        ext[k, far - rows : far] = hy[0, at : at + rows]
        return ext[k]

    def x_rows(side, key):
        at, rows = X_AT[key]
        return hx[side, at : at + rows]

    slots = [0]

    def slot():
        slots[0] += 1
        return slots[0] - 1

    lane_f = lax.broadcasted_iota(jnp.int32, (16, LANES), 1)
    lane_c = lax.broadcasted_iota(jnp.int32, (8, LANES), 1)
    row = lax.broadcasted_iota(jnp.int32, (16, LANES), 0)
    outside_y = jnp.logical_or(
        jnp.logical_and(row >= 12, gy == 0),
        jnp.logical_and(jnp.logical_and(row >= 8, row < 12), gy == lax.axis_size("gy") - 1),
    )
    keep_y = jnp.where(outside_y, 0.0, 1.0).astype(F32)
    keep_left = jnp.where(gx == 0, 0.0, 1.0).astype(F32)
    keep_right = jnp.where(gx == lax.axis_size("gx") - 1, 0.0, 1.0).astype(F32)

    wf, wc, af, ac, cf, cc, rz = {}, {}, {}, {}, {}, {}, {}

    def keep(kind, f, x, own):
        tile = extended((kind, f, x), own)
        if f < 3:
            (wf if kind == "f" else wc)[f, x] = tile
        elif f < 6:
            (af if kind == "f" else ac)[f - 3, x] = tile
        elif f < 8:
            (cf if kind == "f" else cc)[f - 6, x] = tile
        else:
            rz[x] = tile

    for f in range(9):
        for x in range(4):
            keep("f", f, x, own_f[4 * f + x])
    for f in range(8):
        for x in range(2):
            keep("c", f, x, own_c[2 * f + x])
    for side in range(2):

        def col(ring):
            return 3 + ring if side else -ring

        for c in range(3):
            keep("f", c, col(1), x_rows(side, ("f", c, 1)))
            keep("f", c, col(2), x_rows(side, ("f", c, 2)))
            for x in range(2):
                keep("c", c, (2 if side else -2) + x, x_rows(side, ("c", c, x)))
        for f in range(3, 8):
            keep("f", f, col(1), x_rows(side, ("f", f, 1)))
            keep("c", f, 2 if side else -1, x_rows(side, ("c", f, None)))
        bits = extended(("bits", side), x_rows(side, "bits"))
        for c in range(3):
            for r in range(2):
                wf[c, col(3 + r)] = lane_roll(bits, 126 - 4 * c - 2 * r)
            af[c, col(2)] = lane_roll(bits, 115 - c)
        for t in range(2):
            cf[t, col(2)] = lane_roll(bits, 112 - t)
            rz[col(1 + t)] = jnp.broadcast_to(bits[:, 17 + t : 18 + t], (16, LANES))

    def prolong(field, c, x):
        cx = x // 2
        tile = 0.75 * field[c, cx] + 0.25 * field[c, cx + 1 if x % 2 else cx - 1]
        at = slot()
        scr[at, pl.ds(0, 8, stride=2), :] = 0.75 * tile + 0.25 * row_roll(tile, 1)
        scr[at, pl.ds(1, 8, stride=2), :] = 0.75 * tile + 0.25 * row_roll(tile, -1)
        out = scr[at] * keep_y
        return out * keep_left if x < 0 else out * keep_right if x > 3 else out

    def restrict(field, c, cx):
        at = slot()
        scr[at] = field[c, 2 * cx] + field[c, 2 * cx + 1]
        return 0.25 * (scr[at, pl.ds(0, 8, stride=2), :] + scr[at, pl.ds(1, 8, stride=2), :])

    def neighbours(fine, coarse, reach_f, reach_c):
        zp_f, zm_f, zp_c, zm_c = {}, {}, {}, {}
        for c in range(3):
            for x in reach_f:
                tile = fine[c, x]
                zp_f[c, x] = jnp.where(lane_f == LANES - 1, lane_roll(prolong(coarse, c, x), -1), lane_roll(tile, -1))
                zm_f[c, x] = jnp.where(lane_f == 0, tile, lane_roll(tile, 1))
            for x in reach_c:
                tile = coarse[c, x]
                zp_c[c, x] = jnp.where(lane_c == LANES - 1, 0.0, lane_roll(tile, -1))
                zm_c[c, x] = jnp.where(lane_c == 0, lane_roll(restrict(fine, c, x), 1), lane_roll(tile, 1))
        return zp_f, zm_f, zp_c, zm_c

    zp_f, zm_f, zp_c, zm_c = neighbours(wf, wc, range(-3, 7), range(-2, 4))
    wf1, wc1 = {}, {}
    for x in range(-2, 6):
        lap, grad = operator(wf, zp_f, zm_f, x, 4.0, 1.0, 0.5 * rz[x], rz[x] * rz[x])
        for c in range(3):
            wf1[c, x] = af[c, x] + cf[0, x] * lap[c] + cf[1, x] * grad[c]
    for x in range(-1, 3):
        lap, grad = operator(wc, zp_c, zm_c, x, 1.0, 0.25, 0.25, 1.0)
        for c in range(3):
            wc1[c, x] = ac[c, x] + cc[0, x] * lap[c] + cc[1, x] * grad[c]

    zp_f, zm_f, zp_c, zm_c = neighbours(wf1, wc1, range(-1, 5), range(-1, 3))

    def finish(w1, lap, grad, c0, c1, u_r, m_r, q_r, om_r, u_out, m_out, x, tall):
        u = [u_r[c, x] for c in range(3)]
        om = [om_r[l, x] for l in range(3)]
        mem = [[m_r[l, c, x] for c in range(3)] for l in range(3)]
        _, nxt, new = relax(u, mem, [q_r[l, x] for l in range(3)], om)
        for c in range(3):
            u1 = w1[c, x][0:tall] + new[c]
            u_out[c, x] = 2.0 * u1 - u[c] + (c0 * lap[c] + c1 * grad[c])[0:tall]
            for l in range(3):
                m_out[l, c, x] = nxt[l][c] + DT * om[l] * (u1 - nxt[l][c])

    for x in range(4):
        lap, grad = operator(wf1, zp_f, zm_f, x, 4.0, 1.0, 0.5 * rz[x], rz[x] * rz[x])
        finish(wf1, lap, grad, cf[0, x], cf[1, x], uf, mf, qf, omf, uf_out, mf_out, x, 8)
    for x in range(2):
        lap, grad = operator(wc1, zp_c, zm_c, x, 1.0, 0.25, 0.25, 1.0)
        finish(wc1, lap, grad, cc[0, x], cc[1, x], uc, mc, qc, omc, uc_out, mc_out, x, 4)


SCRATCH = 3 * (10 + 6 + 6 + 4)


def swap(value, axis, first):
    pairs = []
    for i in range(first, lax.axis_size(axis) - 1, 2):
        pairs += [(i, i + 1), (i + 1, i)]
    return lax.ppermute(value, axis, pairs)


def call(kernel, shapes, scratch=(), first=False, last=False):
    vmem = pl.BlockSpec(memory_space=pltpu.VMEM)

    def run(*args):
        if not first:
            args = [pltpu.with_memory_space_constraint(a, pltpu.VMEM) for a in args]
        return pl.pallas_call(
            kernel,
            out_shape=[(jax.ShapeDtypeStruct if last else pltpu.VMEM)(s, F32) for s in shapes],
            in_specs=[vmem] * len(args),
            out_specs=[vmem] * len(shapes),
            scratch_shapes=list(scratch),
        )(*args)

    return run


def shards(
    u_now_c,
    u_prev_c,
    memory_c,
    mu_c,
    lam_c,
    rho_c,
    q_c,
    omega_c,
    u_now_f,
    u_prev_f,
    memory_f,
    mu_f,
    lam_f,
    rho_f,
    q_f,
    omega_f,
    stretch_f,
):
    out1, out2, own_f, own_c = call(
        pre_kernel, [(X_ROWS, LANES)] * 2 + [(36, 8, LANES), (16, 4, LANES)], first=True
    )(
        u_now_c, u_prev_c, memory_c, mu_c, lam_c, rho_c, q_c, omega_c,
        u_now_f, u_prev_f, memory_f, mu_f, lam_f, rho_f, q_f, omega_f, stretch_f,
    )
    x2 = swap(out2, "gx", 1)
    x1 = swap(out1, "gx", 0)
    out2, out1 = call(mid_kernel, [(Y_ROWS, LANES)] * 2)(own_f, own_c, x2, x1)
    y2 = swap(out2, "gy", 1)
    y1 = swap(out1, "gy", 0)
    return tuple(
        call(
            post_kernel,
            [u_now_c.shape, u_now_f.shape, memory_c.shape, memory_f.shape],
            [
                pltpu.VMEM((2, X_ROWS, LANES), F32),
                pltpu.VMEM((2, Y_ROWS, LANES), F32),
                pltpu.VMEM((len(Y_F), 16, LANES), F32),
                pltpu.VMEM((len(Y_C), 8, LANES), F32),
                pltpu.VMEM((SCRATCH, 16, LANES), F32),
            ],
            last=True,
        )(own_f, own_c, x2, x1, y2, y1, u_now_c, memory_c, q_c, omega_c, u_now_f, memory_f, q_f, omega_f)
    )


def solution(mesh):
    def level(*lead):
        return P(*lead, "gx", "gy", None)

    inputs = (level(None), level(None), level(None, None), level(), level(), level(), level(None), level(None))
    return jax.shard_map(
        shards,
        mesh=mesh,
        in_specs=inputs + inputs + (P("gx", "gy"),),
        out_specs=(level(None), level(None), level(None, None), level(None, None)),
        check_vma=False,
    )
```

```python
import jax
import jax.numpy as jnp
from jax import lax
from jax.experimental import pallas as pl
from jax.experimental.pallas import tpu as pltpu
from jax.sharding import PartitionSpec as P

DT = 0.1
F32 = jnp.float32
LANES = 128

def layout(pieces):
    table, at = {}, 0
    for key, rows in pieces:
        table[key] = (at, rows)
        at += rows
    return table, -(-at // 8) * 8


X_AT, X_ROWS = layout(
    [(("f", c, r), 8) for r in (1, 2) for c in range(3)]
    + [(("f", f, 1), 8) for f in range(3, 8)]
    + [("bits", 8)]
    + [(("c", c, x), 4) for c in range(3) for x in range(2)]
    + [(("c", f, None), 4) for f in range(3, 8)]
)
Y_F = (
    [(("f", c, x), 4) for c in range(3) for x in range(-2, 6)]
    + [(("bits", side), 4) for side in range(2)]
    + [(("f", f, x), 2) for f in range(3, 8) for x in range(-1, 5)]
    + [(("f", 8, x), 2) for x in range(4)]
)
Y_C = [(("c", c, x), 2) for c in range(3) for x in range(-2, 4)] + [
    (("c", f, x), 2) for f in range(3, 8) for x in range(-1, 3)
]
Y_AT, Y_ROWS = layout(Y_F + Y_C)


def lane_roll(tile, by):
    return pltpu.roll(tile, by % LANES, axis=1)


def row_roll(tile, by):
    return pltpu.roll(tile, by % tile.shape[0], axis=0)


def relax(u, mem, q, om):
    nxt = [[mem[l][c] + DT * om[l] * (u[c] - mem[l][c]) for c in range(3)] for l in range(3)]
    old = [sum(q[l] * mem[l][c] for l in range(3)) for c in range(3)]
    new = [sum(q[l] * nxt[l][c] for l in range(3)) for c in range(3)]
    return old, nxt, new


def pre_kernel(uc, pc, mc, muc, lamc, rhoc, qc, omc, uf, pf, mf, muf, lamf, rhof, qf, omf, st, out1, out2, out3, own_f, own_c):
    even = lax.rem(lax.axis_index("gx"), 2) == 0
    outer_first = far_first(lax.axis_index("gy"))
    eye = lax.broadcasted_iota(jnp.int32, (8, 8), 0) == lax.broadcasted_iota(jnp.int32, (8, 8), 1)
    lane = lax.broadcasted_iota(jnp.int32, (8, LANES), 1)

    def level(u_r, p_r, m_r, mu_r, lam_r, rho_r, q_r, om_r, own, wide):
        for x in range(wide):
            u = [u_r[c, x] for c in range(3)]
            mem = [[m_r[l, c, x] for c in range(3)] for l in range(3)]
            old, _, new = relax(u, mem, [q_r[l, x] for l in range(3)], [om_r[l, x] for l in range(3)])
            scale = (DT * DT) / rho_r[x]
            mu = mu_r[x]
            for c in range(3):
                own[c * wide + x] = u[c] - old[c]
                own[(3 + c) * wide + x] = 2.0 * u[c] - p_r[c, x] - new[c]
            own[6 * wide + x] = scale * mu
            own[7 * wide + x] = scale * (lam_r[x] + mu)

    level(uf, pf, mf, muf, lamf, rhof, qf, omf, own_f, 4)
    level(uc, pc, mc, muc, lamc, rhoc, qc, omc, own_c, 2)
    for x in range(4):
        row = jnp.broadcast_to(st[x : x + 1, :], (8, 8))
        col = jnp.sum(jnp.where(eye, row, 0.0), axis=1, keepdims=True)
        own_f[32 + x] = 1.0 / jnp.broadcast_to(col, (8, LANES))

    def message(out, right):
        def fine(f, ring):
            return own_f[4 * f + (4 - ring if right else ring - 1)]

        for key, (at, rows) in X_AT.items():
            if key[0] == "f":
                out[at : at + rows] = fine(key[1], key[2])
            elif key[0] == "c":
                x = key[2]
                out[at : at + rows] = own_c[2 * key[1] + ((1 if right else 0) if x is None else x)]
        bits = jnp.where(lane == 17, fine(8, 1), fine(8, 2))
        for c in range(3):
            for r in range(2):
                to = 4 * c + 2 * r
                both = jnp.logical_or(lane == to, lane == to + 1)
                bits = jnp.where(both, lane_roll(fine(c, 3 + r), to + 2), bits)
        for f in range(3, 8):
            bits = jnp.where(lane == 9 + f, lane_roll(fine(f, 2), 10 + f), bits)
        at = X_AT["bits"][0]
        out[at : at + 8] = bits

    for is_even in (True, False):
        for is_first in (True, False):

            @pl.when(jnp.logical_and(even == is_even, outer_first == is_first))
            def _(is_even=is_even, is_first=is_first):
                message(out1 if is_first else out2, not is_even)
                message(out2 if is_first else out1, is_even)
                message(out3, not is_even)


def mid_kernel(own_f, own_c, r1, r2, r3, out2, out1, halo):
    gx, gy = lax.axis_index("gx"), lax.axis_index("gy")
    even_x = lax.rem(gx, 2) == 0
    even_y = lax.rem(gy, 2) == 0
    inner_at = jnp.where(far_first(gy), 1, 0)
    outer_at = jnp.where(late(gx), 2, 1 - inner_at)
    for side, at in ((0, jnp.where(even_x, outer_at, inner_at)), (1, jnp.where(even_x, inner_at, outer_at))):
        for k, r in enumerate((r1, r2, r3)):

            @pl.when(at == k)
            def _(side=side, r=r):
                halo[side] = r[...]

    def message(out, up):
        for key, (at, rows) in Y_AT.items():
            fine = (8 - rows if up else 0), (8 if up else rows)
            coarse = (2, 4) if up else (0, 2)
            if key[0] == "bits":
                src = X_AT["bits"][0]
                out[at : at + rows] = halo[key[1], src + fine[0] : src + fine[1]]
                continue
            kind, f, x = key
            wide = 4 if kind == "f" else 2
            part = fine if kind == "f" else coarse
            if 0 <= x < wide:
                out[at : at + rows] = (own_f if kind == "f" else own_c)[wide * f + x, part[0] : part[1]]
            else:
                ring = -x if x < 0 else x - wide + 1
                if kind == "f":
                    src = X_AT["f", f, ring][0]
                else:
                    src = X_AT["c", f, x % 2 if f < 3 else None][0]
                out[at : at + rows] = halo[0 if x < 0 else 1, src + part[0] : src + part[1]]

    @pl.when(even_y)
    def _():
        message(out1, True)
        message(out2, False)

    @pl.when(jnp.logical_not(even_y))
    def _():
        message(out1, False)
        message(out2, True)


def operator(w, zp, zm, x, inv_h2, inv_flat, inv_slant, inv_hz2):
    def dz(c, at):
        return zp[c, at] - zm[c, at]

    def up(tile):
        return row_roll(tile, -1)

    def down(tile):
        return row_roll(tile, 1)

    def dy(c, at):
        return up(w[c, at]) - down(w[c, at])

    dxx = [w[c, x + 1] + w[c, x - 1] - 2.0 * w[c, x] for c in range(3)]
    dyy = [up(w[c, x]) + down(w[c, x]) - 2.0 * w[c, x] for c in range(3)]
    dzz = [zp[c, x] + zm[c, x] - 2.0 * w[c, x] for c in range(3)]
    lap = [(dxx[c] + dyy[c]) * inv_h2 + dzz[c] * inv_hz2 for c in range(3)]
    yz = [up(dz(c, x)) - down(dz(c, x)) for c in (1, 2)]
    grad = [
        dxx[0] * inv_h2 + (dy(1, x + 1) - dy(1, x - 1)) * inv_flat + (dz(2, x + 1) - dz(2, x - 1)) * inv_slant,
        (dy(0, x + 1) - dy(0, x - 1)) * inv_flat + dyy[1] * inv_h2 + yz[1] * inv_slant,
        (dz(0, x + 1) - dz(0, x - 1) + yz[0]) * inv_slant + dzz[2] * inv_hz2,
    ]
    return lap, grad


def post_kernel(
    own_f, own_c, hx, y2, y1, uc, mc, qc, omc, uf, mf, qf, omf, uc_out, uf_out, mc_out, mf_out, hy, ext_f, ext_c, scr
):
    gx, gy = lax.axis_index("gx"), lax.axis_index("gy")
    even_y = lax.rem(gy, 2) == 0

    def sides(halo, first, second, even):
        @pl.when(even)
        def _():
            halo[0] = second[...]
            halo[1] = first[...]

        @pl.when(jnp.logical_not(even))
        def _():
            halo[0] = first[...]
            halo[1] = second[...]

    sides(hy, y1, y2, even_y)

    index = {}

    def extended(key, own):
        at, rows = Y_AT[key]
        if key[0] == "c":
            ext, tall, far = ext_c, 4, 8
        else:
            ext, tall, far = ext_f, 8, 16
        k = index.setdefault(key, len([i for i in index if (i[0] == "c") == (key[0] == "c")]))
        ext[k, 0:tall] = own
        ext[k, tall : tall + rows] = hy[1, at : at + rows]
        ext[k, far - rows : far] = hy[0, at : at + rows]
        return ext[k]

    def x_rows(side, key):
        at, rows = X_AT[key]
        return hx[side, at : at + rows]

    slots = [0]

    def slot():
        slots[0] += 1
        return slots[0] - 1

    lane_f = lax.broadcasted_iota(jnp.int32, (16, LANES), 1)
    lane_c = lax.broadcasted_iota(jnp.int32, (8, LANES), 1)
    row = lax.broadcasted_iota(jnp.int32, (16, LANES), 0)
    outside_y = jnp.logical_or(
        jnp.logical_and(row >= 12, gy == 0),
        jnp.logical_and(jnp.logical_and(row >= 8, row < 12), gy == lax.axis_size("gy") - 1),
    )
    keep_y = jnp.where(outside_y, 0.0, 1.0).astype(F32)
    keep_left = jnp.where(gx == 0, 0.0, 1.0).astype(F32)
    keep_right = jnp.where(gx == lax.axis_size("gx") - 1, 0.0, 1.0).astype(F32)

    wf, wc, af, ac, cf, cc, rz = {}, {}, {}, {}, {}, {}, {}

    def keep(kind, f, x, own):
        tile = extended((kind, f, x), own)
        if f < 3:
            (wf if kind == "f" else wc)[f, x] = tile
        elif f < 6:
            (af if kind == "f" else ac)[f - 3, x] = tile
        elif f < 8:
            (cf if kind == "f" else cc)[f - 6, x] = tile
        else:
            rz[x] = tile

    for f in range(9):
        for x in range(4):
            keep("f", f, x, own_f[4 * f + x])
    for f in range(8):
        for x in range(2):
            keep("c", f, x, own_c[2 * f + x])
    for side in range(2):

        def col(ring):
            return 3 + ring if side else -ring

        for c in range(3):
            keep("f", c, col(1), x_rows(side, ("f", c, 1)))
            keep("f", c, col(2), x_rows(side, ("f", c, 2)))
            for x in range(2):
                keep("c", c, (2 if side else -2) + x, x_rows(side, ("c", c, x)))
        for f in range(3, 8):
            keep("f", f, col(1), x_rows(side, ("f", f, 1)))
            keep("c", f, 2 if side else -1, x_rows(side, ("c", f, None)))
        bits = extended(("bits", side), x_rows(side, "bits"))
        for c in range(3):
            for r in range(2):
                wf[c, col(3 + r)] = lane_roll(bits, 126 - 4 * c - 2 * r)
            af[c, col(2)] = lane_roll(bits, 115 - c)
        for t in range(2):
            cf[t, col(2)] = lane_roll(bits, 112 - t)
            rz[col(1 + t)] = jnp.broadcast_to(bits[:, 17 + t : 18 + t], (16, LANES))

    def prolong(field, c, x):
        cx = x // 2
        tile = 0.75 * field[c, cx] + 0.25 * field[c, cx + 1 if x % 2 else cx - 1]
        at = slot()
        scr[at, pl.ds(0, 8, stride=2), :] = 0.75 * tile + 0.25 * row_roll(tile, 1)
        scr[at, pl.ds(1, 8, stride=2), :] = 0.75 * tile + 0.25 * row_roll(tile, -1)
        out = scr[at] * keep_y
        return out * keep_left if x < 0 else out * keep_right if x > 3 else out

    def restrict(field, c, cx):
        at = slot()
        scr[at] = field[c, 2 * cx] + field[c, 2 * cx + 1]
        return 0.25 * (scr[at, pl.ds(0, 8, stride=2), :] + scr[at, pl.ds(1, 8, stride=2), :])

    def neighbours(fine, coarse, reach_f, reach_c):
        zp_f, zm_f, zp_c, zm_c = {}, {}, {}, {}
        for c in range(3):
            for x in reach_f:
                tile = fine[c, x]
                zp_f[c, x] = jnp.where(lane_f == LANES - 1, lane_roll(prolong(coarse, c, x), -1), lane_roll(tile, -1))
                zm_f[c, x] = jnp.where(lane_f == 0, tile, lane_roll(tile, 1))
            for x in reach_c:
                tile = coarse[c, x]
                zp_c[c, x] = jnp.where(lane_c == LANES - 1, 0.0, lane_roll(tile, -1))
                zm_c[c, x] = jnp.where(lane_c == 0, lane_roll(restrict(fine, c, x), 1), lane_roll(tile, 1))
        return zp_f, zm_f, zp_c, zm_c

    zp_f, zm_f, zp_c, zm_c = neighbours(wf, wc, range(-3, 7), range(-2, 4))
    wf1, wc1 = {}, {}
    for x in range(-2, 6):
        lap, grad = operator(wf, zp_f, zm_f, x, 4.0, 1.0, 0.5 * rz[x], rz[x] * rz[x])
        for c in range(3):
            wf1[c, x] = af[c, x] + cf[0, x] * lap[c] + cf[1, x] * grad[c]
    for x in range(-1, 3):
        lap, grad = operator(wc, zp_c, zm_c, x, 1.0, 0.25, 0.25, 1.0)
        for c in range(3):
            wc1[c, x] = ac[c, x] + cc[0, x] * lap[c] + cc[1, x] * grad[c]

    zp_f, zm_f, zp_c, zm_c = neighbours(wf1, wc1, range(-1, 5), range(-1, 3))

    def finish(w1, lap, grad, c0, c1, u_r, m_r, q_r, om_r, u_out, m_out, x, tall):
        u = [u_r[c, x] for c in range(3)]
        om = [om_r[l, x] for l in range(3)]
        mem = [[m_r[l, c, x] for c in range(3)] for l in range(3)]
        _, nxt, new = relax(u, mem, [q_r[l, x] for l in range(3)], om)
        for c in range(3):
            u1 = w1[c, x][0:tall] + new[c]
            u_out[c, x] = 2.0 * u1 - u[c] + (c0 * lap[c] + c1 * grad[c])[0:tall]
            for l in range(3):
                m_out[l, c, x] = nxt[l][c] + DT * om[l] * (u1 - nxt[l][c])

    for x in range(4):
        lap, grad = operator(wf1, zp_f, zm_f, x, 4.0, 1.0, 0.5 * rz[x], rz[x] * rz[x])
        finish(wf1, lap, grad, cf[0, x], cf[1, x], uf, mf, qf, omf, uf_out, mf_out, x, 8)
    for x in range(2):
        lap, grad = operator(wc1, zp_c, zm_c, x, 1.0, 0.25, 0.25, 1.0)
        finish(wc1, lap, grad, cc[0, x], cc[1, x], uc, mc, qc, omc, uc_out, mc_out, x, 4)


SCRATCH = 3 * (10 + 6 + 6 + 4)


X_RUN, SEAM = 4, 12


def late(gx):
    at = gx % SEAM
    if isinstance(gx, int):
        return at == SEAM - 1 or (at != 0 and at % X_RUN == 0)
    return jnp.logical_or(at == SEAM - 1, jnp.logical_and(at != 0, lax.rem(at, X_RUN) == 0))


def far_first(gy):
    return gy < -(-5 * lax.axis_size("gy") // 8)


def x_exchange(first, second, third):
    nx, ny = lax.axis_size("gx"), lax.axis_size("gy")
    pairs = [[], [], []]
    for i in range(nx - 1):
        for j in range(ny):
            outer = i % 2 == 1
            turn = 0 if outer == far_first(j) else 1
            for source, target in ((i, i + 1), (i + 1, i)):
                held = outer and i % X_RUN == X_RUN - 1 and late(target)
                pairs[2 if held else turn].append((source * ny + j, target * ny + j))
    return [lax.ppermute(v, ("gx", "gy"), p) for v, p in zip((first, second, third), pairs)]


def swap(value, axis, first):
    pairs = []
    for i in range(first, lax.axis_size(axis) - 1, 2):
        pairs += [(i, i + 1), (i + 1, i)]
    return lax.ppermute(value, axis, pairs)


def call(kernel, shapes, scratch=(), first=False, last=False):
    vmem = pl.BlockSpec(memory_space=pltpu.VMEM)

    def run(*args):
        if not first:
            args = [pltpu.with_memory_space_constraint(a, pltpu.VMEM) for a in args]
        return pl.pallas_call(
            kernel,
            out_shape=[(jax.ShapeDtypeStruct if last else pltpu.VMEM)(s, F32) for s in shapes],
            in_specs=[vmem] * len(args),
            out_specs=[vmem] * len(shapes),
            scratch_shapes=list(scratch),
        )(*args)

    return run


def shards(
    u_now_c,
    u_prev_c,
    memory_c,
    mu_c,
    lam_c,
    rho_c,
    q_c,
    omega_c,
    u_now_f,
    u_prev_f,
    memory_f,
    mu_f,
    lam_f,
    rho_f,
    q_f,
    omega_f,
    stretch_f,
):
    out1, out2, out3, own_f, own_c = call(
        pre_kernel, [(X_ROWS, LANES)] * 3 + [(36, 8, LANES), (16, 4, LANES)], first=True
    )(
        u_now_c, u_prev_c, memory_c, mu_c, lam_c, rho_c, q_c, omega_c,
        u_now_f, u_prev_f, memory_f, mu_f, lam_f, rho_f, q_f, omega_f, stretch_f,
    )
    out2, out1, halo = call(mid_kernel, [(Y_ROWS, LANES)] * 2 + [(2, X_ROWS, LANES)])(
        own_f, own_c, *x_exchange(out1, out2, out3)
    )
    y2 = swap(out2, "gy", 1)
    y1 = swap(out1, "gy", 0)
    return tuple(
        call(
            post_kernel,
            [u_now_c.shape, u_now_f.shape, memory_c.shape, memory_f.shape],
            [
                pltpu.VMEM((2, Y_ROWS, LANES), F32),
                pltpu.VMEM((len(Y_F), 16, LANES), F32),
                pltpu.VMEM((len(Y_C), 8, LANES), F32),
                pltpu.VMEM((SCRATCH, 16, LANES), F32),
            ],
            last=True,
        )(own_f, own_c, halo, y2, y1, u_now_c, memory_c, q_c, omega_c, u_now_f, memory_f, q_f, omega_f)
    )


def solution(mesh):
    def level(*lead):
        return P(*lead, "gx", "gy", None)

    inputs = (level(None), level(None), level(None, None), level(), level(), level(), level(None), level(None))
    return jax.shard_map(
        shards,
        mesh=mesh,
        in_specs=inputs + inputs + (P("gx", "gy"),),
        out_specs=(level(None), level(None), level(None, None), level(None, None)),
        check_vma=False,
    )
```

```python
import jax
import jax.numpy as jnp
from jax import lax
from jax.experimental import pallas as pl
from jax.experimental.pallas import tpu as pltpu
from jax.sharding import PartitionSpec as P

DT = 0.1
F32 = jnp.float32
LANES = 128

def layout(pieces):
    table, at = {}, 0
    for key, rows in pieces:
        table[key] = (at, rows)
        at += rows
    return table, -(-at // 8) * 8


X_AT, X_ROWS = layout(
    [(("f", c, r), 8) for r in (1, 2) for c in range(3)]
    + [(("f", f, 1), 8) for f in range(3, 8)]
    + [("bits", 8)]
    + [(("c", c, x), 4) for c in range(3) for x in range(2)]
    + [(("c", f, None), 4) for f in range(3, 8)]
)
Y_F = (
    [(("f", c, x), 4) for c in range(3) for x in range(-2, 6)]
    + [(("bits", side), 4) for side in range(2)]
    + [(("f", f, x), 2) for f in range(3, 8) for x in range(-1, 5)]
    + [(("f", 8, x), 2) for x in range(4)]
)
Y_C = [(("c", c, x), 2) for c in range(3) for x in range(-2, 4)] + [
    (("c", f, x), 2) for f in range(3, 8) for x in range(-1, 3)
]
Y_AT, Y_ROWS = layout(Y_F + Y_C)


def lane_roll(tile, by):
    return pltpu.roll(tile, by % LANES, axis=1)


def row_roll(tile, by):
    return pltpu.roll(tile, by % tile.shape[0], axis=0)


def relax(u, mem, q, om):
    nxt = [[mem[l][c] + DT * om[l] * (u[c] - mem[l][c]) for c in range(3)] for l in range(3)]
    old = [sum(q[l] * mem[l][c] for l in range(3)) for c in range(3)]
    new = [sum(q[l] * nxt[l][c] for l in range(3)) for c in range(3)]
    return old, nxt, new


def pre_kernel(uc, pc, mc, muc, lamc, rhoc, qc, omc, uf, pf, mf, muf, lamf, rhof, qf, omf, st, out1, out2, own_f, own_c):
    even = lax.rem(lax.axis_index("gx"), 2) == 0
    outer_first = far_first(lax.axis_index("gy"))
    eye = lax.broadcasted_iota(jnp.int32, (8, 8), 0) == lax.broadcasted_iota(jnp.int32, (8, 8), 1)
    lane = lax.broadcasted_iota(jnp.int32, (8, LANES), 1)

    def level(u_r, p_r, m_r, mu_r, lam_r, rho_r, q_r, om_r, own, wide):
        for x in range(wide):
            u = [u_r[c, x] for c in range(3)]
            mem = [[m_r[l, c, x] for c in range(3)] for l in range(3)]
            old, _, new = relax(u, mem, [q_r[l, x] for l in range(3)], [om_r[l, x] for l in range(3)])
            scale = (DT * DT) / rho_r[x]
            mu = mu_r[x]
            for c in range(3):
                own[c * wide + x] = u[c] - old[c]
                own[(3 + c) * wide + x] = 2.0 * u[c] - p_r[c, x] - new[c]
            own[6 * wide + x] = scale * mu
            own[7 * wide + x] = scale * (lam_r[x] + mu)

    level(uf, pf, mf, muf, lamf, rhof, qf, omf, own_f, 4)
    level(uc, pc, mc, muc, lamc, rhoc, qc, omc, own_c, 2)
    for x in range(4):
        row = jnp.broadcast_to(st[x : x + 1, :], (8, 8))
        col = jnp.sum(jnp.where(eye, row, 0.0), axis=1, keepdims=True)
        own_f[32 + x] = 1.0 / jnp.broadcast_to(col, (8, LANES))

    def message(out, right):
        def fine(f, ring):
            return own_f[4 * f + (4 - ring if right else ring - 1)]

        for key, (at, rows) in X_AT.items():
            if key[0] == "f":
                out[at : at + rows] = fine(key[1], key[2])
            elif key[0] == "c":
                x = key[2]
                out[at : at + rows] = own_c[2 * key[1] + ((1 if right else 0) if x is None else x)]
        bits = jnp.where(lane == 17, fine(8, 1), fine(8, 2))
        for c in range(3):
            for r in range(2):
                to = 4 * c + 2 * r
                both = jnp.logical_or(lane == to, lane == to + 1)
                bits = jnp.where(both, lane_roll(fine(c, 3 + r), to + 2), bits)
        for f in range(3, 8):
            bits = jnp.where(lane == 9 + f, lane_roll(fine(f, 2), 10 + f), bits)
        at = X_AT["bits"][0]
        out[at : at + 8] = bits

    for is_even in (True, False):
        for is_first in (True, False):

            @pl.when(jnp.logical_and(even == is_even, outer_first == is_first))
            def _(is_even=is_even, is_first=is_first):
                message(out1 if is_first else out2, not is_even)
                message(out2 if is_first else out1, is_even)


def mid_kernel(own_f, own_c, r1, r2, out2, out1, halo):
    gx, gy = lax.axis_index("gx"), lax.axis_index("gy")
    even_x = lax.rem(gx, 2) == 0
    even_y = lax.rem(gy, 2) == 0
    left_first = even_x == far_first(gy)

    @pl.when(left_first)
    def _():
        halo[0] = r1[...]
        halo[1] = r2[...]

    @pl.when(jnp.logical_not(left_first))
    def _():
        halo[0] = r2[...]
        halo[1] = r1[...]

    def message(out, up):
        for key, (at, rows) in Y_AT.items():
            fine = (8 - rows if up else 0), (8 if up else rows)
            coarse = (2, 4) if up else (0, 2)
            if key[0] == "bits":
                src = X_AT["bits"][0]
                out[at : at + rows] = halo[key[1], src + fine[0] : src + fine[1]]
                continue
            kind, f, x = key
            wide = 4 if kind == "f" else 2
            part = fine if kind == "f" else coarse
            if 0 <= x < wide:
                out[at : at + rows] = (own_f if kind == "f" else own_c)[wide * f + x, part[0] : part[1]]
            else:
                ring = -x if x < 0 else x - wide + 1
                if kind == "f":
                    src = X_AT["f", f, ring][0]
                else:
                    src = X_AT["c", f, x % 2 if f < 3 else None][0]
                out[at : at + rows] = halo[0 if x < 0 else 1, src + part[0] : src + part[1]]

    @pl.when(even_y)
    def _():
        message(out1, True)
        message(out2, False)

    @pl.when(jnp.logical_not(even_y))
    def _():
        message(out1, False)
        message(out2, True)


def operator(w, zp, zm, x, inv_h2, inv_flat, inv_slant, inv_hz2):
    def dz(c, at):
        return zp[c, at] - zm[c, at]

    def up(tile):
        return row_roll(tile, -1)

    def down(tile):
        return row_roll(tile, 1)

    def dy(c, at):
        return up(w[c, at]) - down(w[c, at])

    dxx = [w[c, x + 1] + w[c, x - 1] - 2.0 * w[c, x] for c in range(3)]
    dyy = [up(w[c, x]) + down(w[c, x]) - 2.0 * w[c, x] for c in range(3)]
    dzz = [zp[c, x] + zm[c, x] - 2.0 * w[c, x] for c in range(3)]
    lap = [(dxx[c] + dyy[c]) * inv_h2 + dzz[c] * inv_hz2 for c in range(3)]
    yz = [up(dz(c, x)) - down(dz(c, x)) for c in (1, 2)]
    grad = [
        dxx[0] * inv_h2 + (dy(1, x + 1) - dy(1, x - 1)) * inv_flat + (dz(2, x + 1) - dz(2, x - 1)) * inv_slant,
        (dy(0, x + 1) - dy(0, x - 1)) * inv_flat + dyy[1] * inv_h2 + yz[1] * inv_slant,
        (dz(0, x + 1) - dz(0, x - 1) + yz[0]) * inv_slant + dzz[2] * inv_hz2,
    ]
    return lap, grad


def post_kernel(
    own_f, own_c, hx, y2, y1, uc, mc, qc, omc, uf, mf, qf, omf, uc_out, uf_out, mc_out, mf_out, hy, ext_f, ext_c, scr
):
    gx, gy = lax.axis_index("gx"), lax.axis_index("gy")
    even_y = lax.rem(gy, 2) == 0

    def sides(halo, first, second, even):
        @pl.when(even)
        def _():
            halo[0] = second[...]
            halo[1] = first[...]

        @pl.when(jnp.logical_not(even))
        def _():
            halo[0] = first[...]
            halo[1] = second[...]

    sides(hy, y1, y2, even_y)

    index = {}

    def extended(key, own):
        at, rows = Y_AT[key]
        if key[0] == "c":
            ext, tall, far = ext_c, 4, 8
        else:
            ext, tall, far = ext_f, 8, 16
        k = index.setdefault(key, len([i for i in index if (i[0] == "c") == (key[0] == "c")]))
        ext[k, 0:tall] = own
        ext[k, tall : tall + rows] = hy[1, at : at + rows]
        ext[k, far - rows : far] = hy[0, at : at + rows]
        return ext[k]

    def x_rows(side, key):
        at, rows = X_AT[key]
        return hx[side, at : at + rows]

    slots = [0]

    def slot():
        slots[0] += 1
        return slots[0] - 1

    lane_f = lax.broadcasted_iota(jnp.int32, (16, LANES), 1)
    lane_c = lax.broadcasted_iota(jnp.int32, (8, LANES), 1)
    row = lax.broadcasted_iota(jnp.int32, (16, LANES), 0)
    outside_y = jnp.logical_or(
        jnp.logical_and(row >= 12, gy == 0),
        jnp.logical_and(jnp.logical_and(row >= 8, row < 12), gy == lax.axis_size("gy") - 1),
    )
    keep_y = jnp.where(outside_y, 0.0, 1.0).astype(F32)
    keep_left = jnp.where(gx == 0, 0.0, 1.0).astype(F32)
    keep_right = jnp.where(gx == lax.axis_size("gx") - 1, 0.0, 1.0).astype(F32)

    wf, wc, af, ac, cf, cc, rz = {}, {}, {}, {}, {}, {}, {}

    def keep(kind, f, x, own):
        tile = extended((kind, f, x), own)
        if f < 3:
            (wf if kind == "f" else wc)[f, x] = tile
        elif f < 6:
            (af if kind == "f" else ac)[f - 3, x] = tile
        elif f < 8:
            (cf if kind == "f" else cc)[f - 6, x] = tile
        else:
            rz[x] = tile

    for f in range(9):
        for x in range(4):
            keep("f", f, x, own_f[4 * f + x])
    for f in range(8):
        for x in range(2):
            keep("c", f, x, own_c[2 * f + x])
    for side in range(2):

        def col(ring):
            return 3 + ring if side else -ring

        for c in range(3):
            keep("f", c, col(1), x_rows(side, ("f", c, 1)))
            keep("f", c, col(2), x_rows(side, ("f", c, 2)))
            for x in range(2):
                keep("c", c, (2 if side else -2) + x, x_rows(side, ("c", c, x)))
        for f in range(3, 8):
            keep("f", f, col(1), x_rows(side, ("f", f, 1)))
            keep("c", f, 2 if side else -1, x_rows(side, ("c", f, None)))
        bits = extended(("bits", side), x_rows(side, "bits"))
        for c in range(3):
            for r in range(2):
                wf[c, col(3 + r)] = lane_roll(bits, 126 - 4 * c - 2 * r)
            af[c, col(2)] = lane_roll(bits, 115 - c)
        for t in range(2):
            cf[t, col(2)] = lane_roll(bits, 112 - t)
            rz[col(1 + t)] = jnp.broadcast_to(bits[:, 17 + t : 18 + t], (16, LANES))

    def prolong(field, c, x):
        cx = x // 2
        tile = 0.75 * field[c, cx] + 0.25 * field[c, cx + 1 if x % 2 else cx - 1]
        at = slot()
        scr[at, pl.ds(0, 8, stride=2), :] = 0.75 * tile + 0.25 * row_roll(tile, 1)
        scr[at, pl.ds(1, 8, stride=2), :] = 0.75 * tile + 0.25 * row_roll(tile, -1)
        out = scr[at] * keep_y
        return out * keep_left if x < 0 else out * keep_right if x > 3 else out

    def restrict(field, c, cx):
        at = slot()
        scr[at] = field[c, 2 * cx] + field[c, 2 * cx + 1]
        return 0.25 * (scr[at, pl.ds(0, 8, stride=2), :] + scr[at, pl.ds(1, 8, stride=2), :])

    def neighbours(fine, coarse, reach_f, reach_c):
        zp_f, zm_f, zp_c, zm_c = {}, {}, {}, {}
        for c in range(3):
            for x in reach_f:
                tile = fine[c, x]
                zp_f[c, x] = jnp.where(lane_f == LANES - 1, lane_roll(prolong(coarse, c, x), -1), lane_roll(tile, -1))
                zm_f[c, x] = jnp.where(lane_f == 0, tile, lane_roll(tile, 1))
            for x in reach_c:
                tile = coarse[c, x]
                zp_c[c, x] = jnp.where(lane_c == LANES - 1, 0.0, lane_roll(tile, -1))
                zm_c[c, x] = jnp.where(lane_c == 0, lane_roll(restrict(fine, c, x), 1), lane_roll(tile, 1))
        return zp_f, zm_f, zp_c, zm_c

    zp_f, zm_f, zp_c, zm_c = neighbours(wf, wc, range(-3, 7), range(-2, 4))
    wf1, wc1 = {}, {}
    for x in range(-2, 6):
        lap, grad = operator(wf, zp_f, zm_f, x, 4.0, 1.0, 0.5 * rz[x], rz[x] * rz[x])
        for c in range(3):
            wf1[c, x] = af[c, x] + cf[0, x] * lap[c] + cf[1, x] * grad[c]
    for x in range(-1, 3):
        lap, grad = operator(wc, zp_c, zm_c, x, 1.0, 0.25, 0.25, 1.0)
        for c in range(3):
            wc1[c, x] = ac[c, x] + cc[0, x] * lap[c] + cc[1, x] * grad[c]

    zp_f, zm_f, zp_c, zm_c = neighbours(wf1, wc1, range(-1, 5), range(-1, 3))

    def finish(w1, lap, grad, c0, c1, u_r, m_r, q_r, om_r, u_out, m_out, x, tall):
        u = [u_r[c, x] for c in range(3)]
        om = [om_r[l, x] for l in range(3)]
        mem = [[m_r[l, c, x] for c in range(3)] for l in range(3)]
        _, nxt, new = relax(u, mem, [q_r[l, x] for l in range(3)], om)
        for c in range(3):
            u1 = w1[c, x][0:tall] + new[c]
            u_out[c, x] = 2.0 * u1 - u[c] + (c0 * lap[c] + c1 * grad[c])[0:tall]
            for l in range(3):
                m_out[l, c, x] = nxt[l][c] + DT * om[l] * (u1 - nxt[l][c])

    for x in range(4):
        lap, grad = operator(wf1, zp_f, zm_f, x, 4.0, 1.0, 0.5 * rz[x], rz[x] * rz[x])
        finish(wf1, lap, grad, cf[0, x], cf[1, x], uf, mf, qf, omf, uf_out, mf_out, x, 8)
    for x in range(2):
        lap, grad = operator(wc1, zp_c, zm_c, x, 1.0, 0.25, 0.25, 1.0)
        finish(wc1, lap, grad, cc[0, x], cc[1, x], uc, mc, qc, omc, uc_out, mc_out, x, 4)


SCRATCH = 3 * (10 + 6 + 6 + 4)


def far_first(gy):
    return gy < -(-5 * lax.axis_size("gy") // 8)


def x_exchange(first, second):
    nx, ny = lax.axis_size("gx"), lax.axis_size("gy")
    pairs = [[], []]
    for i in range(nx - 1):
        for j in range(ny):
            turn = 0 if (i % 2 == 1) == far_first(j) else 1
            pairs[turn] += [(i * ny + j, (i + 1) * ny + j), ((i + 1) * ny + j, i * ny + j)]
    return [lax.ppermute(v, ("gx", "gy"), p) for v, p in zip((first, second), pairs)]


def swap(value, axis, first):
    pairs = []
    for i in range(first, lax.axis_size(axis) - 1, 2):
        pairs += [(i, i + 1), (i + 1, i)]
    return lax.ppermute(value, axis, pairs)


def call(kernel, shapes, scratch=(), first=False, last=False):
    vmem = pl.BlockSpec(memory_space=pltpu.VMEM)

    def run(*args):
        if not first:
            args = [pltpu.with_memory_space_constraint(a, pltpu.VMEM) for a in args]
        return pl.pallas_call(
            kernel,
            out_shape=[(jax.ShapeDtypeStruct if last else pltpu.VMEM)(s, F32) for s in shapes],
            in_specs=[vmem] * len(args),
            out_specs=[vmem] * len(shapes),
            scratch_shapes=list(scratch),
        )(*args)

    return run


def shards(
    u_now_c,
    u_prev_c,
    memory_c,
    mu_c,
    lam_c,
    rho_c,
    q_c,
    omega_c,
    u_now_f,
    u_prev_f,
    memory_f,
    mu_f,
    lam_f,
    rho_f,
    q_f,
    omega_f,
    stretch_f,
):
    out1, out2, own_f, own_c = call(
        pre_kernel, [(X_ROWS, LANES)] * 2 + [(36, 8, LANES), (16, 4, LANES)], first=True
    )(
        u_now_c, u_prev_c, memory_c, mu_c, lam_c, rho_c, q_c, omega_c,
        u_now_f, u_prev_f, memory_f, mu_f, lam_f, rho_f, q_f, omega_f, stretch_f,
    )
    out2, out1, halo = call(mid_kernel, [(Y_ROWS, LANES)] * 2 + [(2, X_ROWS, LANES)])(
        own_f, own_c, *x_exchange(out1, out2)
    )
    y2 = swap(out2, "gy", 1)
    y1 = swap(out1, "gy", 0)
    return tuple(
        call(
            post_kernel,
            [u_now_c.shape, u_now_f.shape, memory_c.shape, memory_f.shape],
            [
                pltpu.VMEM((2, Y_ROWS, LANES), F32),
                pltpu.VMEM((len(Y_F), 16, LANES), F32),
                pltpu.VMEM((len(Y_C), 8, LANES), F32),
                pltpu.VMEM((SCRATCH, 16, LANES), F32),
            ],
            last=True,
        )(own_f, own_c, halo, y2, y1, u_now_c, memory_c, q_c, omega_c, u_now_f, memory_f, q_f, omega_f)
    )


def solution(mesh):
    def level(*lead):
        return P(*lead, "gx", "gy", None)

    inputs = (level(None), level(None), level(None, None), level(), level(), level(), level(None), level(None))
    return jax.shard_map(
        shards,
        mesh=mesh,
        in_specs=inputs + inputs + (P("gx", "gy"),),
        out_specs=(level(None), level(None), level(None, None), level(None, None)),
        check_vma=False,
    )
```

```python
import jax
import jax.numpy as jnp
from jax import lax
from jax.experimental import pallas as pl
from jax.experimental.pallas import tpu as pltpu
from jax.sharding import PartitionSpec as P

DT = 0.1
F32 = jnp.float32
LANES = 128

def layout(pieces):
    table, at = {}, 0
    for key, rows in pieces:
        table[key] = (at, rows)
        at += rows
    return table, -(-at // 8) * 8


X_AT, X_ROWS = layout(
    [(("f", c, r), 8) for r in (1, 2) for c in range(3)]
    + [(("f", f, 1), 8) for f in range(3, 8)]
    + [("bits", 8)]
    + [(("c", c, x), 4) for c in range(3) for x in range(2)]
    + [(("c", f, None), 4) for f in range(3, 8)]
)
Y_F = (
    [(("f", c, x), 4) for c in range(3) for x in range(-2, 6)]
    + [(("bits", side), 4) for side in range(2)]
    + [(("f", f, x), 2) for f in range(3, 8) for x in range(-1, 5)]
    + [(("f", 8, x), 2) for x in range(4)]
)
Y_C = [(("c", c, x), 2) for c in range(3) for x in range(-2, 4)] + [
    (("c", f, x), 2) for f in range(3, 8) for x in range(-1, 3)
]
Y_AT, Y_ROWS = layout(Y_F + Y_C)


def lane_roll(tile, by):
    return pltpu.roll(tile, by % LANES, axis=1)


def row_roll(tile, by):
    return pltpu.roll(tile, by % tile.shape[0], axis=0)


def relax(u, mem, q, om):
    nxt = [[mem[l][c] + DT * om[l] * (u[c] - mem[l][c]) for c in range(3)] for l in range(3)]
    old = [sum(q[l] * mem[l][c] for l in range(3)) for c in range(3)]
    new = [sum(q[l] * nxt[l][c] for l in range(3)) for c in range(3)]
    return old, nxt, new


def pre_kernel(uc, pc, mc, muc, lamc, rhoc, qc, omc, uf, pf, mf, muf, lamf, rhof, qf, omf, st, out1, out2, out3, own_f, own_c):
    gx = lax.axis_index("gx")
    even = lax.rem(gx, 2) == 0
    outer_turn, inner_turn = x_turns(gx, lax.axis_index("gy"))
    eye = lax.broadcasted_iota(jnp.int32, (8, 8), 0) == lax.broadcasted_iota(jnp.int32, (8, 8), 1)
    lane = lax.broadcasted_iota(jnp.int32, (8, LANES), 1)

    def level(u_r, p_r, m_r, mu_r, lam_r, rho_r, q_r, om_r, own, wide):
        for x in range(wide):
            u = [u_r[c, x] for c in range(3)]
            mem = [[m_r[l, c, x] for c in range(3)] for l in range(3)]
            old, _, new = relax(u, mem, [q_r[l, x] for l in range(3)], [om_r[l, x] for l in range(3)])
            scale = (DT * DT) / rho_r[x]
            mu = mu_r[x]
            for c in range(3):
                own[c * wide + x] = u[c] - old[c]
                own[(3 + c) * wide + x] = 2.0 * u[c] - p_r[c, x] - new[c]
            own[6 * wide + x] = scale * mu
            own[7 * wide + x] = scale * (lam_r[x] + mu)

    level(uf, pf, mf, muf, lamf, rhof, qf, omf, own_f, 4)
    level(uc, pc, mc, muc, lamc, rhoc, qc, omc, own_c, 2)
    for x in range(4):
        row = jnp.broadcast_to(st[x : x + 1, :], (8, 8))
        col = jnp.sum(jnp.where(eye, row, 0.0), axis=1, keepdims=True)
        own_f[32 + x] = 1.0 / jnp.broadcast_to(col, (8, LANES))

    def message(out, right):
        def fine(f, ring):
            return own_f[4 * f + (4 - ring if right else ring - 1)]

        for key, (at, rows) in X_AT.items():
            if key[0] == "f":
                out[at : at + rows] = fine(key[1], key[2])
            elif key[0] == "c":
                x = key[2]
                out[at : at + rows] = own_c[2 * key[1] + ((1 if right else 0) if x is None else x)]
        bits = jnp.where(lane == 17, fine(8, 1), fine(8, 2))
        for c in range(3):
            for r in range(2):
                to = 4 * c + 2 * r
                both = jnp.logical_or(lane == to, lane == to + 1)
                bits = jnp.where(both, lane_roll(fine(c, 3 + r), to + 2), bits)
        for f in range(3, 8):
            bits = jnp.where(lane == 9 + f, lane_roll(fine(f, 2), 10 + f), bits)
        at = X_AT["bits"][0]
        out[at : at + 8] = bits

    for turn, out in enumerate((out1, out2, out3)):
        go_left = jnp.where(even, outer_turn, inner_turn) == turn
        go_right = jnp.where(even, inner_turn, outer_turn) == turn

        @pl.when(go_left)
        def _(out=out):
            message(out, False)

        @pl.when(go_right)
        def _(out=out):
            message(out, True)


def mid_kernel(own_f, own_c, r1, r2, r3, out2, out1, halo):
    gx, gy = lax.axis_index("gx"), lax.axis_index("gy")
    even_x = lax.rem(gx, 2) == 0
    even_y = lax.rem(gy, 2) == 0
    outer_turn, inner_turn = x_turns(gx, gy)
    for turn, r in enumerate((r1, r2, r3)):
        from_left = jnp.where(even_x, outer_turn, inner_turn) == turn
        from_right = jnp.where(even_x, inner_turn, outer_turn) == turn

        @pl.when(from_left)
        def _(r=r):
            halo[0] = r[...]

        @pl.when(from_right)
        def _(r=r):
            halo[1] = r[...]

    def message(out, up):
        for key, (at, rows) in Y_AT.items():
            fine = (8 - rows if up else 0), (8 if up else rows)
            coarse = (2, 4) if up else (0, 2)
            if key[0] == "bits":
                src = X_AT["bits"][0]
                out[at : at + rows] = halo[key[1], src + fine[0] : src + fine[1]]
                continue
            kind, f, x = key
            wide = 4 if kind == "f" else 2
            part = fine if kind == "f" else coarse
            if 0 <= x < wide:
                out[at : at + rows] = (own_f if kind == "f" else own_c)[wide * f + x, part[0] : part[1]]
            else:
                ring = -x if x < 0 else x - wide + 1
                if kind == "f":
                    src = X_AT["f", f, ring][0]
                else:
                    src = X_AT["c", f, x % 2 if f < 3 else None][0]
                out[at : at + rows] = halo[0 if x < 0 else 1, src + part[0] : src + part[1]]

    @pl.when(even_y)
    def _():
        message(out1, True)
        message(out2, False)

    @pl.when(jnp.logical_not(even_y))
    def _():
        message(out1, False)
        message(out2, True)


def operator(w, zp, zm, x, inv_h2, inv_flat, inv_slant, inv_hz2):
    def dz(c, at):
        return zp[c, at] - zm[c, at]

    def up(tile):
        return row_roll(tile, -1)

    def down(tile):
        return row_roll(tile, 1)

    def dy(c, at):
        return up(w[c, at]) - down(w[c, at])

    dxx = [w[c, x + 1] + w[c, x - 1] - 2.0 * w[c, x] for c in range(3)]
    dyy = [up(w[c, x]) + down(w[c, x]) - 2.0 * w[c, x] for c in range(3)]
    dzz = [zp[c, x] + zm[c, x] - 2.0 * w[c, x] for c in range(3)]
    lap = [(dxx[c] + dyy[c]) * inv_h2 + dzz[c] * inv_hz2 for c in range(3)]
    yz = [up(dz(c, x)) - down(dz(c, x)) for c in (1, 2)]
    grad = [
        dxx[0] * inv_h2 + (dy(1, x + 1) - dy(1, x - 1)) * inv_flat + (dz(2, x + 1) - dz(2, x - 1)) * inv_slant,
        (dy(0, x + 1) - dy(0, x - 1)) * inv_flat + dyy[1] * inv_h2 + yz[1] * inv_slant,
        (dz(0, x + 1) - dz(0, x - 1) + yz[0]) * inv_slant + dzz[2] * inv_hz2,
    ]
    return lap, grad


def post_kernel(
    own_f, own_c, hx, y2, y1, uc, mc, qc, omc, uf, mf, qf, omf, uc_out, uf_out, mc_out, mf_out, hy, ext_f, ext_c, scr
):
    gx, gy = lax.axis_index("gx"), lax.axis_index("gy")
    even_y = lax.rem(gy, 2) == 0

    def sides(halo, first, second, even):
        @pl.when(even)
        def _():
            halo[0] = second[...]
            halo[1] = first[...]

        @pl.when(jnp.logical_not(even))
        def _():
            halo[0] = first[...]
            halo[1] = second[...]

    sides(hy, y1, y2, even_y)

    index = {}

    def extended(key, own):
        at, rows = Y_AT[key]
        if key[0] == "c":
            ext, tall, far = ext_c, 4, 8
        else:
            ext, tall, far = ext_f, 8, 16
        k = index.setdefault(key, len([i for i in index if (i[0] == "c") == (key[0] == "c")]))
        ext[k, 0:tall] = own
        ext[k, tall : tall + rows] = hy[1, at : at + rows]
        ext[k, far - rows : far] = hy[0, at : at + rows]
        return ext[k]

    def x_rows(side, key):
        at, rows = X_AT[key]
        return hx[side, at : at + rows]

    slots = [0]

    def slot():
        slots[0] += 1
        return slots[0] - 1

    lane_f = lax.broadcasted_iota(jnp.int32, (16, LANES), 1)
    lane_c = lax.broadcasted_iota(jnp.int32, (8, LANES), 1)
    row = lax.broadcasted_iota(jnp.int32, (16, LANES), 0)
    outside_y = jnp.logical_or(
        jnp.logical_and(row >= 12, gy == 0),
        jnp.logical_and(jnp.logical_and(row >= 8, row < 12), gy == lax.axis_size("gy") - 1),
    )
    keep_y = jnp.where(outside_y, 0.0, 1.0).astype(F32)
    keep_left = jnp.where(gx == 0, 0.0, 1.0).astype(F32)
    keep_right = jnp.where(gx == lax.axis_size("gx") - 1, 0.0, 1.0).astype(F32)

    wf, wc, af, ac, cf, cc, rz = {}, {}, {}, {}, {}, {}, {}

    def keep(kind, f, x, own):
        tile = extended((kind, f, x), own)
        if f < 3:
            (wf if kind == "f" else wc)[f, x] = tile
        elif f < 6:
            (af if kind == "f" else ac)[f - 3, x] = tile
        elif f < 8:
            (cf if kind == "f" else cc)[f - 6, x] = tile
        else:
            rz[x] = tile

    for f in range(9):
        for x in range(4):
            keep("f", f, x, own_f[4 * f + x])
    for f in range(8):
        for x in range(2):
            keep("c", f, x, own_c[2 * f + x])
    for side in range(2):

        def col(ring):
            return 3 + ring if side else -ring

        for c in range(3):
            keep("f", c, col(1), x_rows(side, ("f", c, 1)))
            keep("f", c, col(2), x_rows(side, ("f", c, 2)))
            for x in range(2):
                keep("c", c, (2 if side else -2) + x, x_rows(side, ("c", c, x)))
        for f in range(3, 8):
            keep("f", f, col(1), x_rows(side, ("f", f, 1)))
            keep("c", f, 2 if side else -1, x_rows(side, ("c", f, None)))
        bits = extended(("bits", side), x_rows(side, "bits"))
        for c in range(3):
            for r in range(2):
                wf[c, col(3 + r)] = lane_roll(bits, 126 - 4 * c - 2 * r)
            af[c, col(2)] = lane_roll(bits, 115 - c)
        for t in range(2):
            cf[t, col(2)] = lane_roll(bits, 112 - t)
            rz[col(1 + t)] = jnp.broadcast_to(bits[:, 17 + t : 18 + t], (16, LANES))

    def prolong(field, c, x):
        cx = x // 2
        tile = 0.75 * field[c, cx] + 0.25 * field[c, cx + 1 if x % 2 else cx - 1]
        at = slot()
        scr[at, pl.ds(0, 8, stride=2), :] = 0.75 * tile + 0.25 * row_roll(tile, 1)
        scr[at, pl.ds(1, 8, stride=2), :] = 0.75 * tile + 0.25 * row_roll(tile, -1)
        out = scr[at] * keep_y
        return out * keep_left if x < 0 else out * keep_right if x > 3 else out

    def restrict(field, c, cx):
        at = slot()
        scr[at] = field[c, 2 * cx] + field[c, 2 * cx + 1]
        return 0.25 * (scr[at, pl.ds(0, 8, stride=2), :] + scr[at, pl.ds(1, 8, stride=2), :])

    def neighbours(fine, coarse, reach_f, reach_c):
        zp_f, zm_f, zp_c, zm_c = {}, {}, {}, {}
        for c in range(3):
            for x in reach_f:
                tile = fine[c, x]
                zp_f[c, x] = jnp.where(lane_f == LANES - 1, lane_roll(prolong(coarse, c, x), -1), lane_roll(tile, -1))
                zm_f[c, x] = jnp.where(lane_f == 0, tile, lane_roll(tile, 1))
            for x in reach_c:
                tile = coarse[c, x]
                zp_c[c, x] = jnp.where(lane_c == LANES - 1, 0.0, lane_roll(tile, -1))
                zm_c[c, x] = jnp.where(lane_c == 0, lane_roll(restrict(fine, c, x), 1), lane_roll(tile, 1))
        return zp_f, zm_f, zp_c, zm_c

    zp_f, zm_f, zp_c, zm_c = neighbours(wf, wc, range(-3, 7), range(-2, 4))
    wf1, wc1 = {}, {}
    for x in range(-2, 6):
        lap, grad = operator(wf, zp_f, zm_f, x, 4.0, 1.0, 0.5 * rz[x], rz[x] * rz[x])
        for c in range(3):
            wf1[c, x] = af[c, x] + cf[0, x] * lap[c] + cf[1, x] * grad[c]
    for x in range(-1, 3):
        lap, grad = operator(wc, zp_c, zm_c, x, 1.0, 0.25, 0.25, 1.0)
        for c in range(3):
            wc1[c, x] = ac[c, x] + cc[0, x] * lap[c] + cc[1, x] * grad[c]

    zp_f, zm_f, zp_c, zm_c = neighbours(wf1, wc1, range(-1, 5), range(-1, 3))

    def finish(w1, lap, grad, c0, c1, u_r, m_r, q_r, om_r, u_out, m_out, x, tall):
        u = [u_r[c, x] for c in range(3)]
        om = [om_r[l, x] for l in range(3)]
        mem = [[m_r[l, c, x] for c in range(3)] for l in range(3)]
        _, nxt, new = relax(u, mem, [q_r[l, x] for l in range(3)], om)
        for c in range(3):
            u1 = w1[c, x][0:tall] + new[c]
            u_out[c, x] = 2.0 * u1 - u[c] + (c0 * lap[c] + c1 * grad[c])[0:tall]
            for l in range(3):
                m_out[l, c, x] = nxt[l][c] + DT * om[l] * (u1 - nxt[l][c])

    for x in range(4):
        lap, grad = operator(wf1, zp_f, zm_f, x, 4.0, 1.0, 0.5 * rz[x], rz[x] * rz[x])
        finish(wf1, lap, grad, cf[0, x], cf[1, x], uf, mf, qf, omf, uf_out, mf_out, x, 8)
    for x in range(2):
        lap, grad = operator(wc1, zp_c, zm_c, x, 1.0, 0.25, 0.25, 1.0)
        finish(wc1, lap, grad, cc[0, x], cc[1, x], uc, mc, qc, omc, uc_out, mc_out, x, 4)


SCRATCH = 3 * (10 + 6 + 6 + 4)


X_RUN, SEAM = 4, 12


def x_turns(gx, gy):
    at = gx % SEAM
    early = (at == 0) | (at == 1) | (at == 2) | (at == 3) | (at == 6) | (at == 7)
    soon = gy < -(-5 * lax.axis_size("gy") // 8)
    if isinstance(gx, int):
        return (1 if soon else 2), (0 if early else 2 if soon else 1)
    return jnp.where(soon, 1, 2), jnp.where(early, 0, jnp.where(soon, 2, 1))


def x_exchange(messages):
    nx, ny = lax.axis_size("gx"), lax.axis_size("gy")
    pairs = [[], [], []]
    for i in range(nx - 1):
        for j in range(ny):
            turn = x_turns(i, j)[0 if i % 2 == 1 else 1]
            pairs[turn] += [(i * ny + j, (i + 1) * ny + j), ((i + 1) * ny + j, i * ny + j)]
    return [lax.ppermute(v, ("gx", "gy"), p) for v, p in zip(messages, pairs)]


def swap(value, axis, first):
    pairs = []
    for i in range(first, lax.axis_size(axis) - 1, 2):
        pairs += [(i, i + 1), (i + 1, i)]
    return lax.ppermute(value, axis, pairs)


def call(kernel, shapes, scratch=(), first=False, last=False):
    vmem = pl.BlockSpec(memory_space=pltpu.VMEM)

    def run(*args):
        if not first:
            args = [pltpu.with_memory_space_constraint(a, pltpu.VMEM) for a in args]
        return pl.pallas_call(
            kernel,
            out_shape=[(jax.ShapeDtypeStruct if last else pltpu.VMEM)(s, F32) for s in shapes],
            in_specs=[vmem] * len(args),
            out_specs=[vmem] * len(shapes),
            scratch_shapes=list(scratch),
        )(*args)

    return run


def shards(
    u_now_c,
    u_prev_c,
    memory_c,
    mu_c,
    lam_c,
    rho_c,
    q_c,
    omega_c,
    u_now_f,
    u_prev_f,
    memory_f,
    mu_f,
    lam_f,
    rho_f,
    q_f,
    omega_f,
    stretch_f,
):
    out1, out2, out3, own_f, own_c = call(
        pre_kernel, [(X_ROWS, LANES)] * 3 + [(36, 8, LANES), (16, 4, LANES)], first=True
    )(
        u_now_c, u_prev_c, memory_c, mu_c, lam_c, rho_c, q_c, omega_c,
        u_now_f, u_prev_f, memory_f, mu_f, lam_f, rho_f, q_f, omega_f, stretch_f,
    )
    out2, out1, halo = call(mid_kernel, [(Y_ROWS, LANES)] * 2 + [(2, X_ROWS, LANES)])(
        own_f, own_c, *x_exchange((out1, out2, out3))
    )
    y2 = swap(out2, "gy", 1)
    y1 = swap(out1, "gy", 0)
    return tuple(
        call(
            post_kernel,
            [u_now_c.shape, u_now_f.shape, memory_c.shape, memory_f.shape],
            [
                pltpu.VMEM((2, Y_ROWS, LANES), F32),
                pltpu.VMEM((len(Y_F), 16, LANES), F32),
                pltpu.VMEM((len(Y_C), 8, LANES), F32),
                pltpu.VMEM((SCRATCH, 16, LANES), F32),
            ],
            last=True,
        )(own_f, own_c, halo, y2, y1, u_now_c, memory_c, q_c, omega_c, u_now_f, memory_f, q_f, omega_f)
    )


def solution(mesh):
    def level(*lead):
        return P(*lead, "gx", "gy", None)

    inputs = (level(None), level(None), level(None, None), level(), level(), level(), level(None), level(None))
    return jax.shard_map(
        shards,
        mesh=mesh,
        in_specs=inputs + inputs + (P("gx", "gy"),),
        out_specs=(level(None), level(None), level(None, None), level(None, None)),
        check_vma=False,
    )
```

```python
import jax
import jax.numpy as jnp
from jax import lax
from jax.experimental import pallas as pl
from jax.experimental.pallas import tpu as pltpu
from jax.sharding import PartitionSpec as P

DT = 0.1
F32 = jnp.float32
LANES = 128

def layout(pieces):
    table, at = {}, 0
    for key, rows in pieces:
        table[key] = (at, rows)
        at += rows
    return table, -(-at // 8) * 8


X_AT, X_ROWS = layout(
    [(("f", c, r), 8) for r in (1, 2) for c in range(3)]
    + [(("f", f, 1), 8) for f in range(3, 8)]
    + [("bits", 8)]
    + [(("c", c, x), 4) for c in range(3) for x in range(2)]
    + [(("c", f, None), 4) for f in range(3, 8)]
)
Y_F = (
    [(("f", c, x), 4) for c in range(3) for x in range(-2, 6)]
    + [(("bits", side), 4) for side in range(2)]
    + [(("f", f, x), 2) for f in range(3, 8) for x in range(-1, 5)]
    + [(("f", 8, x), 2) for x in range(4)]
)
Y_C = [(("c", c, x), 2) for c in range(3) for x in range(-2, 4)] + [
    (("c", f, x), 2) for f in range(3, 8) for x in range(-1, 3)
]
Y_AT, Y_ROWS = layout(Y_F + Y_C)


def lane_roll(tile, by):
    return pltpu.roll(tile, by % LANES, axis=1)


def row_roll(tile, by):
    return pltpu.roll(tile, by % tile.shape[0], axis=0)


def relax(u, mem, q, om):
    nxt = [[mem[l][c] + DT * om[l] * (u[c] - mem[l][c]) for c in range(3)] for l in range(3)]
    old = [sum(q[l] * mem[l][c] for l in range(3)) for c in range(3)]
    new = [sum(q[l] * nxt[l][c] for l in range(3)) for c in range(3)]
    return old, nxt, new


def pre_kernel(uc, pc, mc, muc, lamc, rhoc, qc, omc, uf, pf, mf, muf, lamf, rhof, qf, omf, st, inner, outer, own_f, own_c):
    even = lax.rem(lax.axis_index("gx"), 2) == 0
    eye = lax.broadcasted_iota(jnp.int32, (8, 8), 0) == lax.broadcasted_iota(jnp.int32, (8, 8), 1)
    lane = lax.broadcasted_iota(jnp.int32, (8, LANES), 1)

    def level(u_r, p_r, m_r, mu_r, lam_r, rho_r, q_r, om_r, own, wide):
        for x in range(wide):
            u = [u_r[c, x] for c in range(3)]
            mem = [[m_r[l, c, x] for c in range(3)] for l in range(3)]
            old, _, new = relax(u, mem, [q_r[l, x] for l in range(3)], [om_r[l, x] for l in range(3)])
            scale = (DT * DT) / rho_r[x]
            mu = mu_r[x]
            for c in range(3):
                own[c * wide + x] = u[c] - old[c]
                own[(3 + c) * wide + x] = 2.0 * u[c] - p_r[c, x] - new[c]
            own[6 * wide + x] = scale * mu
            own[7 * wide + x] = scale * (lam_r[x] + mu)

    level(uf, pf, mf, muf, lamf, rhof, qf, omf, own_f, 4)
    level(uc, pc, mc, muc, lamc, rhoc, qc, omc, own_c, 2)
    for x in range(4):
        row = jnp.broadcast_to(st[x : x + 1, :], (8, 8))
        col = jnp.sum(jnp.where(eye, row, 0.0), axis=1, keepdims=True)
        own_f[32 + x] = 1.0 / jnp.broadcast_to(col, (8, LANES))

    def message(out, right):
        def fine(f, ring):
            return own_f[4 * f + (4 - ring if right else ring - 1)]

        for key, (at, rows) in X_AT.items():
            if key[0] == "f":
                out[at : at + rows] = fine(key[1], key[2])
            elif key[0] == "c":
                x = key[2]
                out[at : at + rows] = own_c[2 * key[1] + ((1 if right else 0) if x is None else x)]
        bits = jnp.where(lane == 17, fine(8, 1), fine(8, 2))
        for c in range(3):
            for r in range(2):
                to = 4 * c + 2 * r
                both = jnp.logical_or(lane == to, lane == to + 1)
                bits = jnp.where(both, lane_roll(fine(c, 3 + r), to + 2), bits)
        for f in range(3, 8):
            bits = jnp.where(lane == 9 + f, lane_roll(fine(f, 2), 10 + f), bits)
        at = X_AT["bits"][0]
        out[at : at + 8] = bits

    @pl.when(even)
    def _():
        message(inner, True)
        message(outer, False)

    @pl.when(jnp.logical_not(even))
    def _():
        message(inner, False)
        message(outer, True)


def mid_kernel(own_f, own_c, before, both, after, out2, out1, halo):
    gx, gy = lax.axis_index("gx"), lax.axis_index("gy")
    even_x = lax.rem(gx, 2) == 0
    even_y = lax.rem(gy, 2) == 0
    even_side = jnp.where(even_x, 1, 0)

    @pl.when(inner_before(gx, gy))
    def _():
        halo[even_side] = before[...]

    @pl.when(jnp.logical_not(inner_before(gx, gy)))
    def _():
        halo[even_side] = after[...]

    at_end = jnp.logical_or(gx == 0, gx == lax.axis_size("gx") - 1)

    @pl.when(at_end)
    def _():
        halo[1 - even_side] = jnp.zeros((X_ROWS, LANES), F32)

    @pl.when(jnp.logical_and(even_x, jnp.logical_not(at_end)))
    def _():
        halo[0] = both[0:X_ROWS]

    @pl.when(jnp.logical_not(jnp.logical_or(even_x, at_end)))
    def _():
        halo[1] = both[X_ROWS : 2 * X_ROWS]

    def message(out, up):
        for key, (at, rows) in Y_AT.items():
            fine = (8 - rows if up else 0), (8 if up else rows)
            coarse = (2, 4) if up else (0, 2)
            if key[0] == "bits":
                src = X_AT["bits"][0]
                out[at : at + rows] = halo[key[1], src + fine[0] : src + fine[1]]
                continue
            kind, f, x = key
            wide = 4 if kind == "f" else 2
            part = fine if kind == "f" else coarse
            if 0 <= x < wide:
                out[at : at + rows] = (own_f if kind == "f" else own_c)[wide * f + x, part[0] : part[1]]
            else:
                ring = -x if x < 0 else x - wide + 1
                if kind == "f":
                    src = X_AT["f", f, ring][0]
                else:
                    src = X_AT["c", f, x % 2 if f < 3 else None][0]
                out[at : at + rows] = halo[0 if x < 0 else 1, src + part[0] : src + part[1]]

    @pl.when(even_y)
    def _():
        message(out1, True)
        message(out2, False)

    @pl.when(jnp.logical_not(even_y))
    def _():
        message(out1, False)
        message(out2, True)


def operator(w, zp, zm, x, inv_h2, inv_flat, inv_slant, inv_hz2):
    def dz(c, at):
        return zp[c, at] - zm[c, at]

    def up(tile):
        return row_roll(tile, -1)

    def down(tile):
        return row_roll(tile, 1)

    def dy(c, at):
        return up(w[c, at]) - down(w[c, at])

    dxx = [w[c, x + 1] + w[c, x - 1] - 2.0 * w[c, x] for c in range(3)]
    dyy = [up(w[c, x]) + down(w[c, x]) - 2.0 * w[c, x] for c in range(3)]
    dzz = [zp[c, x] + zm[c, x] - 2.0 * w[c, x] for c in range(3)]
    lap = [(dxx[c] + dyy[c]) * inv_h2 + dzz[c] * inv_hz2 for c in range(3)]
    yz = [up(dz(c, x)) - down(dz(c, x)) for c in (1, 2)]
    grad = [
        dxx[0] * inv_h2 + (dy(1, x + 1) - dy(1, x - 1)) * inv_flat + (dz(2, x + 1) - dz(2, x - 1)) * inv_slant,
        (dy(0, x + 1) - dy(0, x - 1)) * inv_flat + dyy[1] * inv_h2 + yz[1] * inv_slant,
        (dz(0, x + 1) - dz(0, x - 1) + yz[0]) * inv_slant + dzz[2] * inv_hz2,
    ]
    return lap, grad


def post_kernel(
    own_f, own_c, hx, y2, y1, uc, mc, qc, omc, uf, mf, qf, omf, uc_out, uf_out, mc_out, mf_out, hy, ext_f, ext_c, scr
):
    gx, gy = lax.axis_index("gx"), lax.axis_index("gy")
    even_y = lax.rem(gy, 2) == 0

    @pl.when(even_y)
    def _():
        hy[0] = y2[0:Y_ROWS]
        hy[1] = y1[Y_ROWS : 2 * Y_ROWS]

    @pl.when(jnp.logical_not(even_y))
    def _():
        hy[0] = y1[0:Y_ROWS]
        hy[1] = y2[Y_ROWS : 2 * Y_ROWS]

    @pl.when(gy == 0)
    def _():
        hy[0] = jnp.zeros((Y_ROWS, LANES), F32)

    @pl.when(gy == lax.axis_size("gy") - 1)
    def _():
        hy[1] = jnp.zeros((Y_ROWS, LANES), F32)

    index = {}

    def extended(key, own):
        at, rows = Y_AT[key]
        if key[0] == "c":
            ext, tall, far = ext_c, 4, 8
        else:
            ext, tall, far = ext_f, 8, 16
        k = index.setdefault(key, len([i for i in index if (i[0] == "c") == (key[0] == "c")]))
        ext[k, 0:tall] = own
        ext[k, tall : tall + rows] = hy[1, at : at + rows]
        ext[k, far - rows : far] = hy[0, at : at + rows]
        return ext[k]

    def x_rows(side, key):
        at, rows = X_AT[key]
        return hx[side, at : at + rows]

    slots = [0]

    def slot():
        slots[0] += 1
        return slots[0] - 1

    lane_f = lax.broadcasted_iota(jnp.int32, (16, LANES), 1)
    lane_c = lax.broadcasted_iota(jnp.int32, (8, LANES), 1)
    row = lax.broadcasted_iota(jnp.int32, (16, LANES), 0)
    outside_y = jnp.logical_or(
        jnp.logical_and(row >= 12, gy == 0),
        jnp.logical_and(jnp.logical_and(row >= 8, row < 12), gy == lax.axis_size("gy") - 1),
    )
    keep_y = jnp.where(outside_y, 0.0, 1.0).astype(F32)
    keep_left = jnp.where(gx == 0, 0.0, 1.0).astype(F32)
    keep_right = jnp.where(gx == lax.axis_size("gx") - 1, 0.0, 1.0).astype(F32)

    wf, wc, af, ac, cf, cc, rz = {}, {}, {}, {}, {}, {}, {}

    def keep(kind, f, x, own):
        tile = extended((kind, f, x), own)
        if f < 3:
            (wf if kind == "f" else wc)[f, x] = tile
        elif f < 6:
            (af if kind == "f" else ac)[f - 3, x] = tile
        elif f < 8:
            (cf if kind == "f" else cc)[f - 6, x] = tile
        else:
            rz[x] = tile

    for f in range(9):
        for x in range(4):
            keep("f", f, x, own_f[4 * f + x])
    for f in range(8):
        for x in range(2):
            keep("c", f, x, own_c[2 * f + x])
    for side in range(2):

        def col(ring):
            return 3 + ring if side else -ring

        for c in range(3):
            keep("f", c, col(1), x_rows(side, ("f", c, 1)))
            keep("f", c, col(2), x_rows(side, ("f", c, 2)))
            for x in range(2):
                keep("c", c, (2 if side else -2) + x, x_rows(side, ("c", c, x)))
        for f in range(3, 8):
            keep("f", f, col(1), x_rows(side, ("f", f, 1)))
            keep("c", f, 2 if side else -1, x_rows(side, ("c", f, None)))
        bits = extended(("bits", side), x_rows(side, "bits"))
        for c in range(3):
            for r in range(2):
                wf[c, col(3 + r)] = lane_roll(bits, 126 - 4 * c - 2 * r)
            af[c, col(2)] = lane_roll(bits, 115 - c)
        for t in range(2):
            cf[t, col(2)] = lane_roll(bits, 112 - t)
            rz[col(1 + t)] = jnp.broadcast_to(bits[:, 17 + t : 18 + t], (16, LANES))

    def prolong(field, c, x):
        cx = x // 2
        tile = 0.75 * field[c, cx] + 0.25 * field[c, cx + 1 if x % 2 else cx - 1]
        at = slot()
        scr[at, pl.ds(0, 8, stride=2), :] = 0.75 * tile + 0.25 * row_roll(tile, 1)
        scr[at, pl.ds(1, 8, stride=2), :] = 0.75 * tile + 0.25 * row_roll(tile, -1)
        out = scr[at] * keep_y
        return out * keep_left if x < 0 else out * keep_right if x > 3 else out

    def restrict(field, c, cx):
        at = slot()
        scr[at] = field[c, 2 * cx] + field[c, 2 * cx + 1]
        return 0.25 * (scr[at, pl.ds(0, 8, stride=2), :] + scr[at, pl.ds(1, 8, stride=2), :])

    def neighbours(fine, coarse, reach_f, reach_c):
        zp_f, zm_f, zp_c, zm_c = {}, {}, {}, {}
        for c in range(3):
            for x in reach_f:
                tile = fine[c, x]
                zp_f[c, x] = jnp.where(lane_f == LANES - 1, lane_roll(prolong(coarse, c, x), -1), lane_roll(tile, -1))
                zm_f[c, x] = jnp.where(lane_f == 0, tile, lane_roll(tile, 1))
            for x in reach_c:
                tile = coarse[c, x]
                zp_c[c, x] = jnp.where(lane_c == LANES - 1, 0.0, lane_roll(tile, -1))
                zm_c[c, x] = jnp.where(lane_c == 0, lane_roll(restrict(fine, c, x), 1), lane_roll(tile, 1))
        return zp_f, zm_f, zp_c, zm_c

    zp_f, zm_f, zp_c, zm_c = neighbours(wf, wc, range(-3, 7), range(-2, 4))
    wf1, wc1 = {}, {}
    for x in range(-2, 6):
        lap, grad = operator(wf, zp_f, zm_f, x, 4.0, 1.0, 0.5 * rz[x], rz[x] * rz[x])
        for c in range(3):
            wf1[c, x] = af[c, x] + cf[0, x] * lap[c] + cf[1, x] * grad[c]
    for x in range(-1, 3):
        lap, grad = operator(wc, zp_c, zm_c, x, 1.0, 0.25, 0.25, 1.0)
        for c in range(3):
            wc1[c, x] = ac[c, x] + cc[0, x] * lap[c] + cc[1, x] * grad[c]

    zp_f, zm_f, zp_c, zm_c = neighbours(wf1, wc1, range(-1, 5), range(-1, 3))

    def finish(w1, lap, grad, c0, c1, u_r, m_r, q_r, om_r, u_out, m_out, x, tall):
        u = [u_r[c, x] for c in range(3)]
        om = [om_r[l, x] for l in range(3)]
        mem = [[m_r[l, c, x] for c in range(3)] for l in range(3)]
        _, nxt, new = relax(u, mem, [q_r[l, x] for l in range(3)], om)
        for c in range(3):
            u1 = w1[c, x][0:tall] + new[c]
            u_out[c, x] = 2.0 * u1 - u[c] + (c0 * lap[c] + c1 * grad[c])[0:tall]
            for l in range(3):
                m_out[l, c, x] = nxt[l][c] + DT * om[l] * (u1 - nxt[l][c])

    for x in range(4):
        lap, grad = operator(wf1, zp_f, zm_f, x, 4.0, 1.0, 0.5 * rz[x], rz[x] * rz[x])
        finish(wf1, lap, grad, cf[0, x], cf[1, x], uf, mf, qf, omf, uf_out, mf_out, x, 8)
    for x in range(2):
        lap, grad = operator(wc1, zp_c, zm_c, x, 1.0, 0.25, 0.25, 1.0)
        finish(wc1, lap, grad, cc[0, x], cc[1, x], uc, mc, qc, omc, uc_out, mc_out, x, 4)


SCRATCH = 3 * (10 + 6 + 6 + 4)


SEAM = 12


def inner_before(gx, gy):
    at = gx % SEAM
    early = (at == 0) | (at == 1) | (at == 2) | (at == 3) | (at == 6) | (at == 7)
    return early | (gy >= -(-5 * lax.axis_size("gy") // 8))


def x_inner(value, before):
    ny = lax.axis_size("gy")
    pairs = []
    for i in range(0, lax.axis_size("gx") - 1, 2):
        for j in range(ny):
            if bool(inner_before(i, j)) == before:
                pairs += [(i * ny + j, (i + 1) * ny + j), ((i + 1) * ny + j, i * ny + j)]
    return lax.ppermute(value, ("gx", "gy"), pairs)


def gather_pairs(value, axis, first):
    nx, ny = lax.axis_size("gx"), lax.axis_size("gy")
    size, other = (nx, ny) if axis == "gx" else (ny, nx)

    def flat(i, k):
        return i * ny + k if axis == "gx" else k * ny + i

    groups = [[flat(i, k), flat(i + 1, k)] for k in range(other) for i in range(first, size - 1, 2)]
    if first:
        groups += [[flat(i, k), flat(i, k + 1)] for i in (0, size - 1) for k in range(0, other, 2)]
    return lax.all_gather(value, ("gx", "gy"), axis_index_groups=sorted(groups), tiled=True)


def call(kernel, shapes, scratch=(), first=False, last=False):
    vmem = pl.BlockSpec(memory_space=pltpu.VMEM)

    def run(*args):
        if not first:
            args = [pltpu.with_memory_space_constraint(a, pltpu.VMEM) for a in args]
        return pl.pallas_call(
            kernel,
            out_shape=[(jax.ShapeDtypeStruct if last else pltpu.VMEM)(s, F32) for s in shapes],
            in_specs=[vmem] * len(args),
            out_specs=[vmem] * len(shapes),
            scratch_shapes=list(scratch),
        )(*args)

    return run


def shards(
    u_now_c,
    u_prev_c,
    memory_c,
    mu_c,
    lam_c,
    rho_c,
    q_c,
    omega_c,
    u_now_f,
    u_prev_f,
    memory_f,
    mu_f,
    lam_f,
    rho_f,
    q_f,
    omega_f,
    stretch_f,
):
    inner, outer, own_f, own_c = call(
        pre_kernel, [(X_ROWS, LANES)] * 2 + [(36, 8, LANES), (16, 4, LANES)], first=True
    )(
        u_now_c, u_prev_c, memory_c, mu_c, lam_c, rho_c, q_c, omega_c,
        u_now_f, u_prev_f, memory_f, mu_f, lam_f, rho_f, q_f, omega_f, stretch_f,
    )
    before, outer = lax.optimization_barrier((x_inner(inner, True), outer))
    both, inner = lax.optimization_barrier((gather_pairs(outer, "gx", 1), inner))
    after = x_inner(inner, False)
    out2, out1, halo = call(mid_kernel, [(Y_ROWS, LANES)] * 2 + [(2, X_ROWS, LANES)])(own_f, own_c, before, both, after)
    y2, out1 = lax.optimization_barrier((gather_pairs(out2, "gy", 1), out1))
    y1 = gather_pairs(out1, "gy", 0)
    return tuple(
        call(
            post_kernel,
            [u_now_c.shape, u_now_f.shape, memory_c.shape, memory_f.shape],
            [
                pltpu.VMEM((2, Y_ROWS, LANES), F32),
                pltpu.VMEM((len(Y_F), 16, LANES), F32),
                pltpu.VMEM((len(Y_C), 8, LANES), F32),
                pltpu.VMEM((SCRATCH, 16, LANES), F32),
            ],
            last=True,
        )(own_f, own_c, halo, y2, y1, u_now_c, memory_c, q_c, omega_c, u_now_f, memory_f, q_f, omega_f)
    )


def solution(mesh):
    def level(*lead):
        return P(*lead, "gx", "gy", None)

    inputs = (level(None), level(None), level(None, None), level(), level(), level(), level(None), level(None))
    return jax.shard_map(
        shards,
        mesh=mesh,
        in_specs=inputs + inputs + (P("gx", "gy"),),
        out_specs=(level(None), level(None), level(None, None), level(None, None)),
        check_vma=False,
    )
```

```python
import jax
import jax.numpy as jnp
from jax import lax
from jax.experimental import pallas as pl
from jax.experimental.pallas import tpu as pltpu
from jax.sharding import PartitionSpec as P

DT = 0.1
F32 = jnp.float32
LANES = 128


def layout(pieces):
    table, at = {}, 0
    for key, rows in pieces:
        table[key] = (at, rows)
        at += rows
    return table, -(-at // 8) * 8


X_AT, X_ROWS = layout(
    [(("f", c, r), 8) for r in (1, 2) for c in range(3)]
    + [(("f", f, 1), 8) for f in range(3, 8)]
    + [("bits", 8)]
    + [(("c", c, x), 4) for c in range(3) for x in range(2)]
    + [(("c", f, None), 4) for f in range(3, 8)]
)
Y_F = (
    [(("f", c, x), 4) for c in range(3) for x in range(-2, 6)]
    + [(("bits", side), 4) for side in range(2)]
    + [(("f", f, x), 2) for f in range(3, 8) for x in range(-1, 5)]
    + [(("f", 8, x), 2) for x in range(4)]
)
Y_C = [(("c", c, x), 2) for c in range(3) for x in range(-2, 4)] + [
    (("c", f, x), 2) for f in range(3, 8) for x in range(-1, 3)
]
Y_AT, Y_ROWS = layout(Y_F + Y_C)


def lane_roll(tile, by):
    return pltpu.roll(tile, by % LANES, axis=1)


def row_roll(tile, by):
    return pltpu.roll(tile, by % tile.shape[0], axis=0)


def relax(u, mem, q, om):
    nxt = [[mem[l][c] + DT * om[l] * (u[c] - mem[l][c]) for c in range(3)] for l in range(3)]
    old = [sum(q[l] * mem[l][c] for l in range(3)) for c in range(3)]
    new = [sum(q[l] * nxt[l][c] for l in range(3)) for c in range(3)]
    return old, nxt, new


def pre_kernel(uc, pc, mc, muc, lamc, rhoc, qc, omc, uf, pf, mf, muf, lamf, rhof, qf, omf, st, inner, outer, own_f, own_c):
    even = lax.rem(lax.axis_index("gx"), 2) == 0
    eye = lax.broadcasted_iota(jnp.int32, (8, 8), 0) == lax.broadcasted_iota(jnp.int32, (8, 8), 1)
    lane = lax.broadcasted_iota(jnp.int32, (8, LANES), 1)

    def level(u_r, p_r, m_r, mu_r, lam_r, rho_r, q_r, om_r, own, wide):
        for x in range(wide):
            u = [u_r[c, x] for c in range(3)]
            mem = [[m_r[l, c, x] for c in range(3)] for l in range(3)]
            old, _, new = relax(u, mem, [q_r[l, x] for l in range(3)], [om_r[l, x] for l in range(3)])
            scale = (DT * DT) / rho_r[x]
            mu = mu_r[x]
            for c in range(3):
                own[c * wide + x] = u[c] - old[c]
                own[(3 + c) * wide + x] = 2.0 * u[c] - p_r[c, x] - new[c]
            own[6 * wide + x] = scale * mu
            own[7 * wide + x] = scale * (lam_r[x] + mu)

    level(uf, pf, mf, muf, lamf, rhof, qf, omf, own_f, 4)
    level(uc, pc, mc, muc, lamc, rhoc, qc, omc, own_c, 2)
    for x in range(4):
        row = jnp.broadcast_to(st[x : x + 1, :], (8, 8))
        col = jnp.sum(jnp.where(eye, row, 0.0), axis=1, keepdims=True)
        own_f[32 + x] = 1.0 / jnp.broadcast_to(col, (8, LANES))

    def message(out, right):
        def fine(f, ring):
            return own_f[4 * f + (4 - ring if right else ring - 1)]

        for key, (at, rows) in X_AT.items():
            if key[0] == "f":
                out[at : at + rows] = fine(key[1], key[2])
            elif key[0] == "c":
                x = key[2]
                out[at : at + rows] = own_c[2 * key[1] + ((1 if right else 0) if x is None else x)]
        bits = jnp.where(lane == 17, fine(8, 1), fine(8, 2))
        for c in range(3):
            for r in range(2):
                to = 4 * c + 2 * r
                both = jnp.logical_or(lane == to, lane == to + 1)
                bits = jnp.where(both, lane_roll(fine(c, 3 + r), to + 2), bits)
        for f in range(3, 8):
            bits = jnp.where(lane == 9 + f, lane_roll(fine(f, 2), 10 + f), bits)
        at = X_AT["bits"][0]
        out[at : at + 8] = bits

    @pl.when(even)
    def _():
        message(inner, True)
        message(outer, False)

    @pl.when(jnp.logical_not(even))
    def _():
        message(inner, False)
        message(outer, True)


def mid_kernel(own_f, own_c, before, both, after, out2, out1, halo):
    gx, gy = lax.axis_index("gx"), lax.axis_index("gy")
    even_x = lax.rem(gx, 2) == 0
    even_y = lax.rem(gy, 2) == 0
    even_side = jnp.where(even_x, 1, 0)

    @pl.when(inner_before(gx, gy))
    def _():
        halo[even_side] = before[...]

    @pl.when(jnp.logical_not(inner_before(gx, gy)))
    def _():
        halo[even_side] = after[...]

    at_end = jnp.logical_or(gx == 0, gx == lax.axis_size("gx") - 1)

    @pl.when(at_end)
    def _():
        halo[1 - even_side] = jnp.zeros((X_ROWS, LANES), F32)

    @pl.when(jnp.logical_and(even_x, jnp.logical_not(at_end)))
    def _():
        halo[0] = both[0:X_ROWS]

    @pl.when(jnp.logical_not(jnp.logical_or(even_x, at_end)))
    def _():
        halo[1] = both[X_ROWS : 2 * X_ROWS]

    def message(out, up):
        for key, (at, rows) in Y_AT.items():
            fine = (8 - rows if up else 0), (8 if up else rows)
            coarse = (2, 4) if up else (0, 2)
            if key[0] == "bits":
                src = X_AT["bits"][0]
                out[at : at + rows] = halo[key[1], src + fine[0] : src + fine[1]]
                continue
            kind, f, x = key
            wide = 4 if kind == "f" else 2
            part = fine if kind == "f" else coarse
            if 0 <= x < wide:
                out[at : at + rows] = (own_f if kind == "f" else own_c)[wide * f + x, part[0] : part[1]]
            else:
                ring = -x if x < 0 else x - wide + 1
                if kind == "f":
                    src = X_AT["f", f, ring][0]
                else:
                    src = X_AT["c", f, x % 2 if f < 3 else None][0]
                out[at : at + rows] = halo[0 if x < 0 else 1, src + part[0] : src + part[1]]

    @pl.when(even_y)
    def _():
        message(out1, True)
        message(out2, False)

    @pl.when(jnp.logical_not(even_y))
    def _():
        message(out1, False)
        message(out2, True)


def operator(w, zp, zm, x, inv_h2, inv_flat, inv_slant, inv_hz2):
    def dz(c, at):
        return zp[c, at] - zm[c, at]

    def up(tile):
        return row_roll(tile, -1)

    def down(tile):
        return row_roll(tile, 1)

    def dy(c, at):
        return up(w[c, at]) - down(w[c, at])

    dxx = [w[c, x + 1] + w[c, x - 1] - 2.0 * w[c, x] for c in range(3)]
    dyy = [up(w[c, x]) + down(w[c, x]) - 2.0 * w[c, x] for c in range(3)]
    dzz = [zp[c, x] + zm[c, x] - 2.0 * w[c, x] for c in range(3)]
    lap = [(dxx[c] + dyy[c]) * inv_h2 + dzz[c] * inv_hz2 for c in range(3)]
    yz = [up(dz(c, x)) - down(dz(c, x)) for c in (1, 2)]
    grad = [
        dxx[0] * inv_h2 + (dy(1, x + 1) - dy(1, x - 1)) * inv_flat + (dz(2, x + 1) - dz(2, x - 1)) * inv_slant,
        (dy(0, x + 1) - dy(0, x - 1)) * inv_flat + dyy[1] * inv_h2 + yz[1] * inv_slant,
        (dz(0, x + 1) - dz(0, x - 1) + yz[0]) * inv_slant + dzz[2] * inv_hz2,
    ]
    return lap, grad


def post_kernel(
    own_f, own_c, hx, y2, y1, uc, mc, qc, omc, uf, mf, qf, omf, uc_out, uf_out, mc_out, mf_out, hy, ext_f, ext_c, scr
):
    gx, gy = lax.axis_index("gx"), lax.axis_index("gy")
    even_y = lax.rem(gy, 2) == 0

    @pl.when(even_y)
    def _():
        hy[0] = y2[...]
        hy[1] = y1[Y_ROWS : 2 * Y_ROWS]

    @pl.when(jnp.logical_not(even_y))
    def _():
        hy[0] = y1[0:Y_ROWS]
        hy[1] = y2[...]

    index = {}

    def extended(key, own):
        at, rows = Y_AT[key]
        if key[0] == "c":
            ext, tall, far = ext_c, 4, 8
        else:
            ext, tall, far = ext_f, 8, 16
        k = index.setdefault(key, len([i for i in index if (i[0] == "c") == (key[0] == "c")]))
        ext[k, 0:tall] = own
        ext[k, tall : tall + rows] = hy[1, at : at + rows]
        ext[k, far - rows : far] = hy[0, at : at + rows]
        return ext[k]

    def x_rows(side, key):
        at, rows = X_AT[key]
        return hx[side, at : at + rows]

    slots = [0]

    def slot():
        slots[0] += 1
        return slots[0] - 1

    lane_f = lax.broadcasted_iota(jnp.int32, (16, LANES), 1)
    lane_c = lax.broadcasted_iota(jnp.int32, (8, LANES), 1)
    row = lax.broadcasted_iota(jnp.int32, (16, LANES), 0)
    outside_y = jnp.logical_or(
        jnp.logical_and(row >= 12, gy == 0),
        jnp.logical_and(jnp.logical_and(row >= 8, row < 12), gy == lax.axis_size("gy") - 1),
    )
    keep_y = jnp.where(outside_y, 0.0, 1.0).astype(F32)
    keep_left = jnp.where(gx == 0, 0.0, 1.0).astype(F32)
    keep_right = jnp.where(gx == lax.axis_size("gx") - 1, 0.0, 1.0).astype(F32)

    wf, wc, af, ac, cf, cc, rz = {}, {}, {}, {}, {}, {}, {}

    def keep(kind, f, x, own):
        tile = extended((kind, f, x), own)
        if f < 3:
            (wf if kind == "f" else wc)[f, x] = tile
        elif f < 6:
            (af if kind == "f" else ac)[f - 3, x] = tile
        elif f < 8:
            (cf if kind == "f" else cc)[f - 6, x] = tile
        else:
            rz[x] = tile

    for f in range(9):
        for x in range(4):
            keep("f", f, x, own_f[4 * f + x])
    for f in range(8):
        for x in range(2):
            keep("c", f, x, own_c[2 * f + x])
    for side in range(2):

        def col(ring):
            return 3 + ring if side else -ring

        for c in range(3):
            keep("f", c, col(1), x_rows(side, ("f", c, 1)))
            keep("f", c, col(2), x_rows(side, ("f", c, 2)))
            for x in range(2):
                keep("c", c, (2 if side else -2) + x, x_rows(side, ("c", c, x)))
        for f in range(3, 8):
            keep("f", f, col(1), x_rows(side, ("f", f, 1)))
            keep("c", f, 2 if side else -1, x_rows(side, ("c", f, None)))
        bits = extended(("bits", side), x_rows(side, "bits"))
        for c in range(3):
            for r in range(2):
                wf[c, col(3 + r)] = lane_roll(bits, 126 - 4 * c - 2 * r)
            af[c, col(2)] = lane_roll(bits, 115 - c)
        for t in range(2):
            cf[t, col(2)] = lane_roll(bits, 112 - t)
            rz[col(1 + t)] = jnp.broadcast_to(bits[:, 17 + t : 18 + t], (16, LANES))

    def prolong(field, c, x):
        cx = x // 2
        tile = 0.75 * field[c, cx] + 0.25 * field[c, cx + 1 if x % 2 else cx - 1]
        at = slot()
        scr[at, pl.ds(0, 8, stride=2), :] = 0.75 * tile + 0.25 * row_roll(tile, 1)
        scr[at, pl.ds(1, 8, stride=2), :] = 0.75 * tile + 0.25 * row_roll(tile, -1)
        out = scr[at] * keep_y
        return out * keep_left if x < 0 else out * keep_right if x > 3 else out

    def restrict(field, c, cx):
        at = slot()
        scr[at] = field[c, 2 * cx] + field[c, 2 * cx + 1]
        return 0.25 * (scr[at, pl.ds(0, 8, stride=2), :] + scr[at, pl.ds(1, 8, stride=2), :])

    def neighbours(fine, coarse, reach_f, reach_c):
        zp_f, zm_f, zp_c, zm_c = {}, {}, {}, {}
        for c in range(3):
            for x in reach_f:
                tile = fine[c, x]
                zp_f[c, x] = jnp.where(lane_f == LANES - 1, lane_roll(prolong(coarse, c, x), -1), lane_roll(tile, -1))
                zm_f[c, x] = jnp.where(lane_f == 0, tile, lane_roll(tile, 1))
            for x in reach_c:
                tile = coarse[c, x]
                zp_c[c, x] = jnp.where(lane_c == LANES - 1, 0.0, lane_roll(tile, -1))
                zm_c[c, x] = jnp.where(lane_c == 0, lane_roll(restrict(fine, c, x), 1), lane_roll(tile, 1))
        return zp_f, zm_f, zp_c, zm_c

    zp_f, zm_f, zp_c, zm_c = neighbours(wf, wc, range(-3, 7), range(-2, 4))
    wf1, wc1 = {}, {}
    for x in range(-2, 6):
        lap, grad = operator(wf, zp_f, zm_f, x, 4.0, 1.0, 0.5 * rz[x], rz[x] * rz[x])
        for c in range(3):
            wf1[c, x] = af[c, x] + cf[0, x] * lap[c] + cf[1, x] * grad[c]
    for x in range(-1, 3):
        lap, grad = operator(wc, zp_c, zm_c, x, 1.0, 0.25, 0.25, 1.0)
        for c in range(3):
            wc1[c, x] = ac[c, x] + cc[0, x] * lap[c] + cc[1, x] * grad[c]

    zp_f, zm_f, zp_c, zm_c = neighbours(wf1, wc1, range(-1, 5), range(-1, 3))

    def finish(w1, lap, grad, c0, c1, u_r, m_r, q_r, om_r, u_out, m_out, x, tall):
        u = [u_r[c, x] for c in range(3)]
        om = [om_r[l, x] for l in range(3)]
        mem = [[m_r[l, c, x] for c in range(3)] for l in range(3)]
        _, nxt, new = relax(u, mem, [q_r[l, x] for l in range(3)], om)
        for c in range(3):
            u1 = w1[c, x][0:tall] + new[c]
            u_out[c, x] = 2.0 * u1 - u[c] + (c0 * lap[c] + c1 * grad[c])[0:tall]
            for l in range(3):
                m_out[l, c, x] = nxt[l][c] + DT * om[l] * (u1 - nxt[l][c])

    for x in range(4):
        lap, grad = operator(wf1, zp_f, zm_f, x, 4.0, 1.0, 0.5 * rz[x], rz[x] * rz[x])
        finish(wf1, lap, grad, cf[0, x], cf[1, x], uf, mf, qf, omf, uf_out, mf_out, x, 8)
    for x in range(2):
        lap, grad = operator(wc1, zp_c, zm_c, x, 1.0, 0.25, 0.25, 1.0)
        finish(wc1, lap, grad, cc[0, x], cc[1, x], uc, mc, qc, omc, uc_out, mc_out, x, 4)


SCRATCH = 3 * (10 + 6 + 6 + 4)


SEAM = 12


def inner_before(gx, gy):
    return (gx % SEAM < SEAM - 2) | (gy >= -(-5 * lax.axis_size("gy") // 8))


def x_inner(value, before):
    ny = lax.axis_size("gy")
    pairs = []
    for i in range(0, lax.axis_size("gx") - 1, 2):
        for j in range(ny):
            if bool(inner_before(i, j)) == before:
                pairs += [(i * ny + j, (i + 1) * ny + j), ((i + 1) * ny + j, i * ny + j)]
    return lax.ppermute(value, ("gx", "gy"), pairs)


def swap(value, axis, first):
    pairs = []
    for i in range(first, lax.axis_size(axis) - 1, 2):
        pairs += [(i, i + 1), (i + 1, i)]
    return lax.ppermute(value, axis, pairs)


def gather_pairs(value, axis, first):
    nx, ny = lax.axis_size("gx"), lax.axis_size("gy")
    size, other = (nx, ny) if axis == "gx" else (ny, nx)

    def flat(i, k):
        return i * ny + k if axis == "gx" else k * ny + i

    groups = [[flat(i, k), flat(i + 1, k)] for k in range(other) for i in range(first, size - 1, 2)]
    if first:
        groups += [[flat(i, k), flat(i, k + 1)] for i in (0, size - 1) for k in range(0, other, 2)]
    return lax.all_gather(value, ("gx", "gy"), axis_index_groups=sorted(groups), tiled=True)


def call(kernel, shapes, scratch=(), first=False, last=False):
    vmem = pl.BlockSpec(memory_space=pltpu.VMEM)

    def run(*args):
        if not first:
            args = [pltpu.with_memory_space_constraint(a, pltpu.VMEM) for a in args]
        return pl.pallas_call(
            kernel,
            out_shape=[(jax.ShapeDtypeStruct if last else pltpu.VMEM)(s, F32) for s in shapes],
            in_specs=[vmem] * len(args),
            out_specs=[vmem] * len(shapes),
            scratch_shapes=list(scratch),
        )(*args)

    return run


def shards(
    u_now_c,
    u_prev_c,
    memory_c,
    mu_c,
    lam_c,
    rho_c,
    q_c,
    omega_c,
    u_now_f,
    u_prev_f,
    memory_f,
    mu_f,
    lam_f,
    rho_f,
    q_f,
    omega_f,
    stretch_f,
):
    inner, outer, own_f, own_c = call(
        pre_kernel, [(X_ROWS, LANES)] * 2 + [(36, 8, LANES), (16, 4, LANES)], first=True
    )(
        u_now_c, u_prev_c, memory_c, mu_c, lam_c, rho_c, q_c, omega_c,
        u_now_f, u_prev_f, memory_f, mu_f, lam_f, rho_f, q_f, omega_f, stretch_f,
    )
    before = x_inner(inner, True)
    both = gather_pairs(outer, "gx", 1)
    both, inner = lax.optimization_barrier((both, inner))
    after = x_inner(inner, False)
    out2, out1, halo = call(mid_kernel, [(Y_ROWS, LANES)] * 2 + [(2, X_ROWS, LANES)])(own_f, own_c, before, both, after)
    y2 = swap(out2, "gy", 1)
    y1 = gather_pairs(out1, "gy", 0)
    return tuple(
        call(
            post_kernel,
            [u_now_c.shape, u_now_f.shape, memory_c.shape, memory_f.shape],
            [
                pltpu.VMEM((2, Y_ROWS, LANES), F32),
                pltpu.VMEM((len(Y_F), 16, LANES), F32),
                pltpu.VMEM((len(Y_C), 8, LANES), F32),
                pltpu.VMEM((SCRATCH, 16, LANES), F32),
            ],
            last=True,
        )(own_f, own_c, halo, y2, y1, u_now_c, memory_c, q_c, omega_c, u_now_f, memory_f, q_f, omega_f)
    )


def solution(mesh):
    def level(*lead):
        return P(*lead, "gx", "gy", None)

    inputs = (level(None), level(None), level(None, None), level(), level(), level(), level(None), level(None))
    return jax.shard_map(
        shards,
        mesh=mesh,
        in_specs=inputs + inputs + (P("gx", "gy"),),
        out_specs=(level(None), level(None), level(None, None), level(None, None)),
        check_vma=False,
    )
```

```python
import jax
import jax.numpy as jnp
from jax import lax
from jax.experimental import pallas as pl
from jax.experimental.pallas import tpu as pltpu
from jax.sharding import PartitionSpec as P

DT = 0.1
F32 = jnp.float32
LANES = 128


def layout(pieces):
    table, at = {}, 0
    for key, rows in pieces:
        table[key] = (at, rows)
        at += rows
    return table, -(-at // 8) * 8


X_AT, X_ROWS = layout(
    [(("f", f, 1), 8) for f in range(8)]
    + [("bits", 8)]
    + [("edge", 4)]
    + [(("c", c, x), 4) for c in range(3) for x in range(2)]
    + [(("c", f, None), 4) for f in range(3, 8)]
)
Y_F = (
    [(("f", c, x), 4) for c in range(3) for x in range(-1, 5)]
    + [(("bits", side), 4) for side in range(2)]
    + [(("f", f, x), 2) for f in range(3, 8) for x in range(-1, 5)]
    + [(("f", 8, x), 2) for x in range(4)]
)
Y_C = [(("c", c, x), 2) for c in range(3) for x in range(-2, 4)] + [
    (("c", f, x), 2) for f in range(3, 8) for x in range(-1, 3)
]
Y_E = [(("edge", side, c), 1) for side in range(2) for c in range(2)]
Y_AT, Y_ROWS = layout(Y_F + Y_C + Y_E)


def lane_roll(tile, by):
    return pltpu.roll(tile, by % LANES, axis=1)


def row_roll(tile, by):
    return pltpu.roll(tile, by % tile.shape[0], axis=0)


def relax(u, mem, q, om):
    nxt = [[mem[l][c] + DT * om[l] * (u[c] - mem[l][c]) for c in range(3)] for l in range(3)]
    old = [sum(q[l] * mem[l][c] for l in range(3)) for c in range(3)]
    new = [sum(q[l] * nxt[l][c] for l in range(3)) for c in range(3)]
    return old, nxt, new


def pre_kernel(uc, pc, mc, muc, lamc, rhoc, qc, omc, uf, pf, mf, muf, lamf, rhof, qf, omf, st, inner, outer, own_f, own_c, rows4, rows8):
    even = lax.rem(lax.axis_index("gx"), 2) == 0
    eye = lax.broadcasted_iota(jnp.int32, (8, 8), 0) == lax.broadcasted_iota(jnp.int32, (8, 8), 1)
    lane = lax.broadcasted_iota(jnp.int32, (8, LANES), 1)
    row = lax.broadcasted_iota(jnp.int32, (8, LANES), 0)
    rows4[...] = jnp.zeros((3, 8, LANES), F32)

    def level(u_r, p_r, m_r, mu_r, lam_r, rho_r, q_r, om_r, own, wide):
        for x in range(wide):
            u = [u_r[c, x] for c in range(3)]
            mem = [[m_r[l, c, x] for c in range(3)] for l in range(3)]
            old, _, new = relax(u, mem, [q_r[l, x] for l in range(3)], [om_r[l, x] for l in range(3)])
            scale = (DT * DT) / rho_r[x]
            mu = mu_r[x]
            for c in range(3):
                own[c * wide + x] = u[c] - old[c]
                own[(3 + c) * wide + x] = 2.0 * u[c] - p_r[c, x] - new[c]
            own[6 * wide + x] = scale * mu
            own[7 * wide + x] = scale * (lam_r[x] + mu)

    level(uf, pf, mf, muf, lamf, rhof, qf, omf, own_f, 4)
    level(uc, pc, mc, muc, lamc, rhoc, qc, omc, own_c, 2)
    for x in range(4):
        heights = jnp.broadcast_to(st[x : x + 1, :], (8, 8))
        col = jnp.sum(jnp.where(eye, heights, 0.0), axis=1, keepdims=True)
        own_f[32 + x] = 1.0 / jnp.broadcast_to(col, (8, LANES))

    def message(out, right):
        def fine(f, ring):
            return own_f[4 * f + (4 - ring if right else ring - 1)]

        shear, lame = fine(6, 1), fine(7, 1)
        sign = -1.0 if right else 1.0
        slant = 0.5 * fine(8, 1)
        ring2 = [fine(c, 2) for c in range(3)]

        def dy(tile):
            return jnp.where(row == 7, 0.0, row_roll(tile, -1)) - jnp.where(row == 0, 0.0, row_roll(tile, 1))

        def dz(c):
            far, close = (own_c[2 * c], own_c[2 * c + 1]) if right else (own_c[2 * c + 1], own_c[2 * c])
            plane, ghost = rows4.at[c], rows8.at[c]
            plane[1:5] = 0.75 * close + 0.25 * far
            ghost[pl.ds(0, 4, stride=2), :] = 0.75 * plane[1:5] + 0.25 * plane[0:4]
            ghost[pl.ds(1, 4, stride=2), :] = 0.75 * plane[1:5] + 0.25 * plane[2:6]
            tile = ring2[c]
            above = jnp.where(lane == LANES - 1, lane_roll(ghost[...], -1), lane_roll(tile, -1))
            return above - jnp.where(lane == 0, tile, lane_roll(tile, 1))

        extra = [
            4.0 * ring2[0] + sign * (dy(ring2[1]) + dz(2) * slant),
            sign * dy(ring2[0]),
            sign * dz(0) * slant,
        ]
        for key, (at, rows) in X_AT.items():
            if key[0] == "f" and 3 <= key[1] < 6:
                c = key[1] - 3
                out[at : at + rows] = fine(key[1], 1) + shear * (4.0 * ring2[c]) + lame * extra[c]
            elif key[0] == "f":
                out[at : at + rows] = fine(key[1], 1)
            elif key[0] == "c":
                x = key[2]
                out[at : at + rows] = own_c[2 * key[1] + ((1 if right else 0) if x is None else x)]
        at = X_AT["edge"][0]
        for c in range(2):
            for k, y in enumerate((0, 7)):
                out[at + 2 * c + k : at + 2 * c + k + 1] = own_f[4 * c + (2 if right else 1), y : y + 1]
        bits = jnp.where(lane == 17, fine(8, 1), fine(8, 2))
        for c in range(3):
            for ring, to in ((2, 19 + 2 * c), (3, 4 * c), (4, 4 * c + 2)):
                both = jnp.logical_or(lane == to, lane == to + 1)
                bits = jnp.where(both, lane_roll(fine(c, ring), to + 2), bits)
        for f in range(3, 8):
            bits = jnp.where(lane == 9 + f, lane_roll(fine(f, 2), 10 + f), bits)
        at = X_AT["bits"][0]
        out[at : at + 8] = bits

    @pl.when(even)
    def _():
        message(inner, True)
        message(outer, False)

    @pl.when(jnp.logical_not(even))
    def _():
        message(inner, False)
        message(outer, True)


def mid_kernel(own_f, own_c, before, both, after, out2, out1, halo):
    gx, gy = lax.axis_index("gx"), lax.axis_index("gy")
    even_x = lax.rem(gx, 2) == 0
    even_y = lax.rem(gy, 2) == 0
    even_side = jnp.where(even_x, 1, 0)

    @pl.when(inner_before(gx, gy))
    def _():
        halo[even_side] = before[...]

    @pl.when(jnp.logical_not(inner_before(gx, gy)))
    def _():
        halo[even_side] = after[...]

    at_end = jnp.logical_or(gx == 0, gx == lax.axis_size("gx") - 1)

    @pl.when(at_end)
    def _():
        halo[1 - even_side] = jnp.zeros((X_ROWS, LANES), F32)

    @pl.when(jnp.logical_and(even_x, jnp.logical_not(at_end)))
    def _():
        halo[0] = both[0:X_ROWS]

    @pl.when(jnp.logical_not(jnp.logical_or(even_x, at_end)))
    def _():
        halo[1] = both[X_ROWS : 2 * X_ROWS]

    def message(out, up):
        for key, (at, rows) in Y_AT.items():
            fine = (8 - rows if up else 0), (8 if up else rows)
            coarse = (2, 4) if up else (0, 2)
            if key[0] == "bits":
                src = X_AT["bits"][0]
                out[at : at + rows] = halo[key[1], src + fine[0] : src + fine[1]]
                continue
            if key[0] == "edge":
                src = X_AT["edge"][0] + 2 * key[2] + (1 if up else 0)
                out[at : at + 1] = halo[key[1], src : src + 1]
                continue
            kind, f, x = key
            wide = 4 if kind == "f" else 2
            part = fine if kind == "f" else coarse
            if 0 <= x < wide:
                out[at : at + rows] = (own_f if kind == "f" else own_c)[wide * f + x, part[0] : part[1]]
            else:
                ring = -x if x < 0 else x - wide + 1
                if kind == "f":
                    src = X_AT["f", f, ring][0]
                else:
                    src = X_AT["c", f, x % 2 if f < 3 else None][0]
                out[at : at + rows] = halo[0 if x < 0 else 1, src + part[0] : src + part[1]]

    @pl.when(even_y)
    def _():
        message(out1, True)
        message(out2, False)

    @pl.when(jnp.logical_not(even_y))
    def _():
        message(out1, False)
        message(out2, True)


def operator(w, zp, zm, x, inv_h2, inv_flat, inv_slant, inv_hz2, given=(None, None, None)):
    given_at, given_dy, given_dz = given

    def wx(c, at):
        return 0.0 if at == given_at else w[c, at]

    def dz(c, at):
        return given_dz[c] if at == given_at else zp[c, at] - zm[c, at]

    def up(tile):
        return row_roll(tile, -1)

    def down(tile):
        return row_roll(tile, 1)

    def dy(c, at):
        return given_dy[c] if at == given_at else up(w[c, at]) - down(w[c, at])

    dxx = [wx(c, x + 1) + wx(c, x - 1) - 2.0 * w[c, x] for c in range(3)]
    dyy = [up(w[c, x]) + down(w[c, x]) - 2.0 * w[c, x] for c in range(3)]
    dzz = [zp[c, x] + zm[c, x] - 2.0 * w[c, x] for c in range(3)]
    lap = [(dxx[c] + dyy[c]) * inv_h2 + dzz[c] * inv_hz2 for c in range(3)]
    yz = [up(dz(c, x)) - down(dz(c, x)) for c in (1, 2)]
    grad = [
        dxx[0] * inv_h2 + (dy(1, x + 1) - dy(1, x - 1)) * inv_flat + (dz(2, x + 1) - dz(2, x - 1)) * inv_slant,
        (dy(0, x + 1) - dy(0, x - 1)) * inv_flat + dyy[1] * inv_h2 + yz[1] * inv_slant,
        (dz(0, x + 1) - dz(0, x - 1) + yz[0]) * inv_slant + dzz[2] * inv_hz2,
    ]
    return lap, grad


def post_kernel(
    own_f, own_c, hx, y2, y1, uc, mc, qc, omc, uf, mf, qf, omf, uc_out, uf_out, mc_out, mf_out, hy, ext_f, ext_c, ext_e, scr
):
    gx, gy = lax.axis_index("gx"), lax.axis_index("gy")
    even_y = lax.rem(gy, 2) == 0

    @pl.when(even_y)
    def _():
        hy[0] = y2[...]
        hy[1] = y1[Y_ROWS : 2 * Y_ROWS]

    @pl.when(jnp.logical_not(even_y))
    def _():
        hy[0] = y1[0:Y_ROWS]
        hy[1] = y2[...]

    index = {}

    def extended(key, own):
        at, rows = Y_AT[key]
        if key[0] == "c":
            ext, tall, far = ext_c, 4, 8
        else:
            ext, tall, far = ext_f, 8, 16
        k = index.setdefault(key, len([i for i in index if (i[0] == "c") == (key[0] == "c")]))
        ext[k, 0:tall] = own
        ext[k, tall : tall + rows] = hy[1, at : at + rows]
        ext[k, far - rows : far] = hy[0, at : at + rows]
        return ext[k]

    def x_rows(side, key):
        at, rows = X_AT[key]
        return hx[side, at : at + rows]

    slots = [0]

    def slot():
        slots[0] += 1
        return slots[0] - 1

    lane_f = lax.broadcasted_iota(jnp.int32, (16, LANES), 1)
    lane_c = lax.broadcasted_iota(jnp.int32, (8, LANES), 1)
    row = lax.broadcasted_iota(jnp.int32, (16, LANES), 0)
    outside_y = jnp.logical_or(
        jnp.logical_and(row >= 12, gy == 0),
        jnp.logical_and(jnp.logical_and(row >= 8, row < 12), gy == lax.axis_size("gy") - 1),
    )
    keep_y = jnp.where(outside_y, 0.0, 1.0).astype(F32)
    keep_left = jnp.where(gx == 0, 0.0, 1.0).astype(F32)
    keep_right = jnp.where(gx == lax.axis_size("gx") - 1, 0.0, 1.0).astype(F32)

    wf, wc, af, ac, cf, cc, rz = {}, {}, {}, {}, {}, {}, {}

    def keep(kind, f, x, own):
        tile = extended((kind, f, x), own)
        if f < 3:
            (wf if kind == "f" else wc)[f, x] = tile
        elif f < 6:
            (af if kind == "f" else ac)[f - 3, x] = tile
        elif f < 8:
            (cf if kind == "f" else cc)[f - 6, x] = tile
        else:
            rz[x] = tile

    for f in range(9):
        for x in range(4):
            keep("f", f, x, own_f[4 * f + x])
    for f in range(8):
        for x in range(2):
            keep("c", f, x, own_c[2 * f + x])
    for side in range(2):

        def col(ring):
            return 3 + ring if side else -ring

        for c in range(3):
            keep("f", c, col(1), x_rows(side, ("f", c, 1)))
            for x in range(2):
                keep("c", c, (2 if side else -2) + x, x_rows(side, ("c", c, x)))
        for f in range(3, 8):
            keep("f", f, col(1), x_rows(side, ("f", f, 1)))
            keep("c", f, 2 if side else -1, x_rows(side, ("c", f, None)))
        bits = extended(("bits", side), x_rows(side, "bits"))
        for c in range(3):
            for r in range(2):
                wf[c, col(3 + r)] = lane_roll(bits, 126 - 4 * c - 2 * r)
            wf[c, col(2)] = lane_roll(bits, 107 - 2 * c)
            af[c, col(2)] = lane_roll(bits, 115 - c)
        for t in range(2):
            cf[t, col(2)] = lane_roll(bits, 112 - t)
            rz[col(1 + t)] = jnp.broadcast_to(bits[:, 17 + t : 18 + t], (16, LANES))

    def prolong(field, c, x):
        cx = x // 2
        tile = 0.75 * field[c, cx] + 0.25 * field[c, cx + 1 if x % 2 else cx - 1]
        at = slot()
        scr[at, pl.ds(0, 8, stride=2), :] = 0.75 * tile + 0.25 * row_roll(tile, 1)
        scr[at, pl.ds(1, 8, stride=2), :] = 0.75 * tile + 0.25 * row_roll(tile, -1)
        out = scr[at] * keep_y
        return out * keep_left if x < 0 else out * keep_right if x > 3 else out

    crosses = (row == 0) | (row == 7) | (row == 8) | (row == 15)
    across = []
    for side in range(2):
        given_dy, given_dz = {}, {}
        for c in range(2):
            k = 2 * side + c
            src, at = X_AT["edge"][0] + 2 * c, Y_AT["edge", side, c][0]
            ext_e[k] = jnp.zeros((16, LANES), F32)
            ext_e[k, 0:1] = hx[side, src : src + 1]
            ext_e[k, 7:8] = hx[side, src + 1 : src + 2]
            ext_e[k, 8:9] = hy[1, at : at + 1]
            ext_e[k, 15:16] = hy[0, at : at + 1]
            tile = ext_e[k]
            given_dy[c] = jnp.where(crosses, row_roll(tile, -1) - row_roll(tile, 1), 0.0)
        for c in (0, 2):
            tile = 0.75 * wc[c, 2 if side else -1] + 0.25 * wc[c, 3 if side else -2]
            at = slot()
            scr[at, pl.ds(0, 8, stride=2), :] = 0.25 * row_roll(tile, 1)
            scr[at, pl.ds(1, 8, stride=2), :] = 0.25 * row_roll(tile, -1)
            given_dz[c] = jnp.where(crosses & (lane_f == LANES - 1), lane_roll(scr[at], -1), 0.0)
        across.append((5 if side else -2, given_dy, given_dz))

    def restrict(field, c, cx):
        at = slot()
        scr[at] = field[c, 2 * cx] + field[c, 2 * cx + 1]
        return 0.25 * (scr[at, pl.ds(0, 8, stride=2), :] + scr[at, pl.ds(1, 8, stride=2), :])

    def neighbours(fine, coarse, reach_f, reach_c):
        zp_f, zm_f, zp_c, zm_c = {}, {}, {}, {}
        for c in range(3):
            for x in reach_f:
                tile = fine[c, x]
                zp_f[c, x] = jnp.where(lane_f == LANES - 1, lane_roll(prolong(coarse, c, x), -1), lane_roll(tile, -1))
                zm_f[c, x] = jnp.where(lane_f == 0, tile, lane_roll(tile, 1))
            for x in reach_c:
                tile = coarse[c, x]
                zp_c[c, x] = jnp.where(lane_c == LANES - 1, 0.0, lane_roll(tile, -1))
                zm_c[c, x] = jnp.where(lane_c == 0, lane_roll(restrict(fine, c, x), 1), lane_roll(tile, 1))
        return zp_f, zm_f, zp_c, zm_c

    zp_f, zm_f, zp_c, zm_c = neighbours(wf, wc, range(-3, 7), range(-2, 4))
    wf1, wc1 = {}, {}
    for x in range(-2, 6):
        given = {-1: across[0], 4: across[1]}.get(x, (None, None, None))
        lap, grad = operator(wf, zp_f, zm_f, x, 4.0, 1.0, 0.5 * rz[x], rz[x] * rz[x], given)
        for c in range(3):
            wf1[c, x] = af[c, x] + cf[0, x] * lap[c] + cf[1, x] * grad[c]
    for x in range(-1, 3):
        lap, grad = operator(wc, zp_c, zm_c, x, 1.0, 0.25, 0.25, 1.0)
        for c in range(3):
            wc1[c, x] = ac[c, x] + cc[0, x] * lap[c] + cc[1, x] * grad[c]

    zp_f, zm_f, zp_c, zm_c = neighbours(wf1, wc1, range(-1, 5), range(-1, 3))

    def finish(w1, lap, grad, c0, c1, u_r, m_r, q_r, om_r, u_out, m_out, x, tall):
        u = [u_r[c, x] for c in range(3)]
        om = [om_r[l, x] for l in range(3)]
        mem = [[m_r[l, c, x] for c in range(3)] for l in range(3)]
        _, nxt, new = relax(u, mem, [q_r[l, x] for l in range(3)], om)
        for c in range(3):
            u1 = w1[c, x][0:tall] + new[c]
            u_out[c, x] = 2.0 * u1 - u[c] + (c0 * lap[c] + c1 * grad[c])[0:tall]
            for l in range(3):
                m_out[l, c, x] = nxt[l][c] + DT * om[l] * (u1 - nxt[l][c])

    for x in range(4):
        lap, grad = operator(wf1, zp_f, zm_f, x, 4.0, 1.0, 0.5 * rz[x], rz[x] * rz[x])
        finish(wf1, lap, grad, cf[0, x], cf[1, x], uf, mf, qf, omf, uf_out, mf_out, x, 8)
    for x in range(2):
        lap, grad = operator(wc1, zp_c, zm_c, x, 1.0, 0.25, 0.25, 1.0)
        finish(wc1, lap, grad, cc[0, x], cc[1, x], uc, mc, qc, omc, uc_out, mc_out, x, 4)


SCRATCH = 3 * (10 + 6 + 6 + 4) + 4


SEAM = 12


def inner_before(gx, gy):
    return (gx % SEAM < SEAM - 2) | (gy >= -(-5 * lax.axis_size("gy") // 8))


def x_inner(value, before):
    ny = lax.axis_size("gy")
    pairs = []
    for i in range(0, lax.axis_size("gx") - 1, 2):
        for j in range(ny):
            if bool(inner_before(i, j)) == before:
                pairs += [(i * ny + j, (i + 1) * ny + j), ((i + 1) * ny + j, i * ny + j)]
    return lax.ppermute(value, ("gx", "gy"), pairs)


def swap(value, axis, first):
    pairs = []
    for i in range(first, lax.axis_size(axis) - 1, 2):
        pairs += [(i, i + 1), (i + 1, i)]
    return lax.ppermute(value, axis, pairs)


def gather_pairs(value, axis, first):
    nx, ny = lax.axis_size("gx"), lax.axis_size("gy")
    size, other = (nx, ny) if axis == "gx" else (ny, nx)

    def flat(i, k):
        return i * ny + k if axis == "gx" else k * ny + i

    groups = [[flat(i, k), flat(i + 1, k)] for k in range(other) for i in range(first, size - 1, 2)]
    if first:
        groups += [[flat(i, k), flat(i, k + 1)] for i in (0, size - 1) for k in range(0, other, 2)]
    return lax.all_gather(value, ("gx", "gy"), axis_index_groups=sorted(groups), tiled=True)


def call(kernel, shapes, scratch=(), first=False, last=False):
    vmem = pl.BlockSpec(memory_space=pltpu.VMEM)

    def run(*args):
        if not first:
            args = [pltpu.with_memory_space_constraint(a, pltpu.VMEM) for a in args]
        return pl.pallas_call(
            kernel,
            out_shape=[(jax.ShapeDtypeStruct if last else pltpu.VMEM)(s, F32) for s in shapes],
            in_specs=[vmem] * len(args),
            out_specs=[vmem] * len(shapes),
            scratch_shapes=list(scratch),
        )(*args)

    return run


def shards(
    u_now_c,
    u_prev_c,
    memory_c,
    mu_c,
    lam_c,
    rho_c,
    q_c,
    omega_c,
    u_now_f,
    u_prev_f,
    memory_f,
    mu_f,
    lam_f,
    rho_f,
    q_f,
    omega_f,
    stretch_f,
):
    inner, outer, own_f, own_c = call(
        pre_kernel,
        [(X_ROWS, LANES)] * 2 + [(36, 8, LANES), (16, 4, LANES)],
        [pltpu.VMEM((3, 8, LANES), F32), pltpu.VMEM((3, 8, LANES), F32)],
        first=True,
    )(
        u_now_c, u_prev_c, memory_c, mu_c, lam_c, rho_c, q_c, omega_c,
        u_now_f, u_prev_f, memory_f, mu_f, lam_f, rho_f, q_f, omega_f, stretch_f,
    )
    before = x_inner(inner, True)
    both = gather_pairs(outer, "gx", 1)
    both, inner = lax.optimization_barrier((both, inner))
    after = x_inner(inner, False)
    out2, out1, halo = call(mid_kernel, [(Y_ROWS, LANES)] * 2 + [(2, X_ROWS, LANES)])(own_f, own_c, before, both, after)
    y2 = swap(out2, "gy", 1)
    y1 = gather_pairs(out1, "gy", 0)
    return tuple(
        call(
            post_kernel,
            [u_now_c.shape, u_now_f.shape, memory_c.shape, memory_f.shape],
            [
                pltpu.VMEM((2, Y_ROWS, LANES), F32),
                pltpu.VMEM((len(Y_F), 16, LANES), F32),
                pltpu.VMEM((len(Y_C), 8, LANES), F32),
                pltpu.VMEM((4, 16, LANES), F32),
                pltpu.VMEM((SCRATCH, 16, LANES), F32),
            ],
            last=True,
        )(own_f, own_c, halo, y2, y1, u_now_c, memory_c, q_c, omega_c, u_now_f, memory_f, q_f, omega_f)
    )


def solution(mesh):
    def level(*lead):
        return P(*lead, "gx", "gy", None)

    inputs = (level(None), level(None), level(None, None), level(), level(), level(), level(None), level(None))
    return jax.shard_map(
        shards,
        mesh=mesh,
        in_specs=inputs + inputs + (P("gx", "gy"),),
        out_specs=(level(None), level(None), level(None, None), level(None, None)),
        check_vma=False,
    )
```

```python
import jax
import jax.numpy as jnp
from jax import lax
from jax.experimental import pallas as pl
from jax.experimental.pallas import tpu as pltpu
from jax.sharding import PartitionSpec as P

DT = 0.1
F32 = jnp.float32
LANES = 128


def layout(pieces):
    table, at = {}, 0
    for key, rows in pieces:
        table[key] = (at, rows)
        at += rows
    return table, -(-at // 8) * 8


X_AT, X_ROWS = layout(
    [(("f", f, 1), 8) for f in range(8)]
    + [("bits", 8)]
    + [("edge", 4)]
    + [(("c", c, x), 4) for c in range(3) for x in range(2)]
    + [(("c", f, None), 4) for f in range(3, 8)]
)
Y_F = (
    [(("f", c, x), 4) for c in range(3) for x in range(-1, 5)]
    + [(("bits", side), 4) for side in range(2)]
    + [(("f", f, x), 2) for f in range(3, 8) for x in range(-1, 5)]
    + [(("f", 8, x), 2) for x in range(4)]
)
Y_C = [(("c", c, x), 2) for c in range(3) for x in range(-2, 4)] + [
    (("c", f, x), 1) for f in range(3, 8) for x in range(-1, 3)
]
Y_E = [(("edge", side, c), 1) for side in range(2) for c in range(2)]
Y_AT, Y_ROWS = layout(Y_F + Y_C + Y_E)


def lane_roll(tile, by):
    return pltpu.roll(tile, by % LANES, axis=1)


def row_roll(tile, by):
    return pltpu.roll(tile, by % tile.shape[0], axis=0)


def relax(u, mem, q, om):
    nxt = [[mem[l][c] + DT * om[l] * (u[c] - mem[l][c]) for c in range(3)] for l in range(3)]
    old = [sum(q[l] * mem[l][c] for l in range(3)) for c in range(3)]
    new = [sum(q[l] * nxt[l][c] for l in range(3)) for c in range(3)]
    return old, nxt, new


def pre_kernel(uc, pc, mc, muc, lamc, rhoc, qc, omc, uf, pf, mf, muf, lamf, rhof, qf, omf, st, inner, outer, own_f, own_c, rows4, rows8):
    even = lax.rem(lax.axis_index("gx"), 2) == 0
    eye = lax.broadcasted_iota(jnp.int32, (8, 8), 0) == lax.broadcasted_iota(jnp.int32, (8, 8), 1)
    lane = lax.broadcasted_iota(jnp.int32, (8, LANES), 1)
    row = lax.broadcasted_iota(jnp.int32, (8, LANES), 0)
    rows4[...] = jnp.zeros((3, 8, LANES), F32)

    def level(u_r, p_r, m_r, mu_r, lam_r, rho_r, q_r, om_r, own, wide):
        for x in range(wide):
            u = [u_r[c, x] for c in range(3)]
            mem = [[m_r[l, c, x] for c in range(3)] for l in range(3)]
            old, _, new = relax(u, mem, [q_r[l, x] for l in range(3)], [om_r[l, x] for l in range(3)])
            scale = (DT * DT) / rho_r[x]
            mu = mu_r[x]
            for c in range(3):
                own[c * wide + x] = u[c] - old[c]
                own[(3 + c) * wide + x] = 2.0 * u[c] - p_r[c, x] - new[c]
            own[6 * wide + x] = scale * mu
            own[7 * wide + x] = scale * (lam_r[x] + mu)

    level(uf, pf, mf, muf, lamf, rhof, qf, omf, own_f, 4)
    level(uc, pc, mc, muc, lamc, rhoc, qc, omc, own_c, 2)
    for x in range(4):
        heights = jnp.broadcast_to(st[x : x + 1, :], (8, 8))
        col = jnp.sum(jnp.where(eye, heights, 0.0), axis=1, keepdims=True)
        own_f[32 + x] = 1.0 / jnp.broadcast_to(col, (8, LANES))

    def message(out, right):
        def fine(f, ring):
            return own_f[4 * f + (4 - ring if right else ring - 1)]

        shear, lame = fine(6, 1), fine(7, 1)
        sign = -1.0 if right else 1.0
        slant = 0.5 * fine(8, 1)
        ring2 = [fine(c, 2) for c in range(3)]

        def dy(tile):
            return jnp.where(row == 7, 0.0, row_roll(tile, -1)) - jnp.where(row == 0, 0.0, row_roll(tile, 1))

        def dz(c):
            far, close = (own_c[2 * c], own_c[2 * c + 1]) if right else (own_c[2 * c + 1], own_c[2 * c])
            plane, ghost = rows4.at[c], rows8.at[c]
            plane[1:5] = 0.75 * close + 0.25 * far
            ghost[pl.ds(0, 4, stride=2), :] = 0.75 * plane[1:5] + 0.25 * plane[0:4]
            ghost[pl.ds(1, 4, stride=2), :] = 0.75 * plane[1:5] + 0.25 * plane[2:6]
            tile = ring2[c]
            above = jnp.where(lane == LANES - 1, lane_roll(ghost[...], -1), lane_roll(tile, -1))
            return above - jnp.where(lane == 0, tile, lane_roll(tile, 1))

        extra = [
            4.0 * ring2[0] + sign * (dy(ring2[1]) + dz(2) * slant),
            sign * dy(ring2[0]),
            sign * dz(0) * slant,
        ]
        for key, (at, rows) in X_AT.items():
            if key[0] == "f" and 3 <= key[1] < 6:
                c = key[1] - 3
                out[at : at + rows] = fine(key[1], 1) + shear * (4.0 * ring2[c]) + lame * extra[c]
            elif key[0] == "f":
                out[at : at + rows] = fine(key[1], 1)
            elif key[0] == "c":
                x = key[2]
                out[at : at + rows] = own_c[2 * key[1] + ((1 if right else 0) if x is None else x)]
        at = X_AT["edge"][0]
        for c in range(2):
            for k, y in enumerate((0, 7)):
                out[at + 2 * c + k : at + 2 * c + k + 1] = own_f[4 * c + (2 if right else 1), y : y + 1]
        bits = jnp.where(lane == 17, fine(8, 1), fine(8, 2))
        for c in range(3):
            for ring, to in ((2, 19 + 2 * c), (3, 4 * c), (4, 4 * c + 2)):
                both = jnp.logical_or(lane == to, lane == to + 1)
                bits = jnp.where(both, lane_roll(fine(c, ring), to + 2), bits)
        for f in range(3, 8):
            bits = jnp.where(lane == 9 + f, lane_roll(fine(f, 2), 10 + f), bits)
        at = X_AT["bits"][0]
        out[at : at + 8] = bits

    @pl.when(even)
    def _():
        message(inner, True)
        message(outer, False)

    @pl.when(jnp.logical_not(even))
    def _():
        message(inner, False)
        message(outer, True)


def mid_kernel(own_f, own_c, before, both, after, out2, out1, halo):
    gx, gy = lax.axis_index("gx"), lax.axis_index("gy")
    even_x = lax.rem(gx, 2) == 0
    even_y = lax.rem(gy, 2) == 0
    even_side = jnp.where(even_x, 1, 0)

    @pl.when(inner_before(gx, gy))
    def _():
        halo[even_side] = before[...]

    @pl.when(jnp.logical_not(inner_before(gx, gy)))
    def _():
        halo[even_side] = after[...]

    at_end = jnp.logical_or(gx == 0, gx == lax.axis_size("gx") - 1)

    @pl.when(at_end)
    def _():
        halo[1 - even_side] = jnp.zeros((X_ROWS, LANES), F32)

    @pl.when(jnp.logical_and(even_x, jnp.logical_not(at_end)))
    def _():
        halo[0] = both[0:X_ROWS]

    @pl.when(jnp.logical_not(jnp.logical_or(even_x, at_end)))
    def _():
        halo[1] = both[X_ROWS : 2 * X_ROWS]

    def message(out, up):
        for key, (at, rows) in Y_AT.items():
            fine = (8 - rows if up else 0), (8 if up else rows)
            coarse = (4 - rows if up else 0), (4 if up else rows)
            if key[0] == "bits":
                src = X_AT["bits"][0]
                out[at : at + rows] = halo[key[1], src + fine[0] : src + fine[1]]
                continue
            if key[0] == "edge":
                src = X_AT["edge"][0] + 2 * key[2] + (1 if up else 0)
                out[at : at + 1] = halo[key[1], src : src + 1]
                continue
            kind, f, x = key
            wide = 4 if kind == "f" else 2
            part = fine if kind == "f" else coarse
            if 0 <= x < wide:
                out[at : at + rows] = (own_f if kind == "f" else own_c)[wide * f + x, part[0] : part[1]]
            else:
                ring = -x if x < 0 else x - wide + 1
                if kind == "f":
                    src = X_AT["f", f, ring][0]
                else:
                    src = X_AT["c", f, x % 2 if f < 3 else None][0]
                out[at : at + rows] = halo[0 if x < 0 else 1, src + part[0] : src + part[1]]

    @pl.when(even_y)
    def _():
        message(out1, True)
        message(out2, False)

    @pl.when(jnp.logical_not(even_y))
    def _():
        message(out1, False)
        message(out2, True)


def operator(w, zp, zm, x, inv_h2, inv_flat, inv_slant, inv_hz2, given=(None, None, None)):
    given_at, given_dy, given_dz = given

    def wx(c, at):
        return 0.0 if at == given_at else w[c, at]

    def dz(c, at):
        return given_dz[c] if at == given_at else zp[c, at] - zm[c, at]

    def up(tile):
        return row_roll(tile, -1)

    def down(tile):
        return row_roll(tile, 1)

    def dy(c, at):
        return given_dy[c] if at == given_at else up(w[c, at]) - down(w[c, at])

    dxx = [wx(c, x + 1) + wx(c, x - 1) - 2.0 * w[c, x] for c in range(3)]
    dyy = [up(w[c, x]) + down(w[c, x]) - 2.0 * w[c, x] for c in range(3)]
    dzz = [zp[c, x] + zm[c, x] - 2.0 * w[c, x] for c in range(3)]
    lap = [(dxx[c] + dyy[c]) * inv_h2 + dzz[c] * inv_hz2 for c in range(3)]
    yz = [up(dz(c, x)) - down(dz(c, x)) for c in (1, 2)]
    grad = [
        dxx[0] * inv_h2 + (dy(1, x + 1) - dy(1, x - 1)) * inv_flat + (dz(2, x + 1) - dz(2, x - 1)) * inv_slant,
        (dy(0, x + 1) - dy(0, x - 1)) * inv_flat + dyy[1] * inv_h2 + yz[1] * inv_slant,
        (dz(0, x + 1) - dz(0, x - 1) + yz[0]) * inv_slant + dzz[2] * inv_hz2,
    ]
    return lap, grad


def post_kernel(
    own_f, own_c, hx, y2, y1, uc, mc, qc, omc, uf, mf, qf, omf, uc_out, uf_out, mc_out, mf_out, hy, ext_f, ext_c, ext_e, scr
):
    gx, gy = lax.axis_index("gx"), lax.axis_index("gy")
    even_y = lax.rem(gy, 2) == 0

    @pl.when(even_y)
    def _():
        hy[0] = y2[...]
        hy[1] = y1[Y_ROWS : 2 * Y_ROWS]

    @pl.when(jnp.logical_not(even_y))
    def _():
        hy[0] = y1[0:Y_ROWS]
        hy[1] = y2[...]

    index = {}

    def extended(key, own):
        at, rows = Y_AT[key]
        if key[0] == "c":
            ext, tall, far = ext_c, 4, 8
        else:
            ext, tall, far = ext_f, 8, 16
        k = index.setdefault(key, len([i for i in index if (i[0] == "c") == (key[0] == "c")]))
        ext[k, 0:tall] = own
        ext[k, tall : tall + rows] = hy[1, at : at + rows]
        ext[k, far - rows : far] = hy[0, at : at + rows]
        return ext[k]

    def x_rows(side, key):
        at, rows = X_AT[key]
        return hx[side, at : at + rows]

    slots = [0]

    def slot():
        slots[0] += 1
        return slots[0] - 1

    lane_f = lax.broadcasted_iota(jnp.int32, (16, LANES), 1)
    lane_c = lax.broadcasted_iota(jnp.int32, (8, LANES), 1)
    row = lax.broadcasted_iota(jnp.int32, (16, LANES), 0)
    outside_y = jnp.logical_or(
        jnp.logical_and(row >= 12, gy == 0),
        jnp.logical_and(jnp.logical_and(row >= 8, row < 12), gy == lax.axis_size("gy") - 1),
    )
    keep_y = jnp.where(outside_y, 0.0, 1.0).astype(F32)
    keep_left = jnp.where(gx == 0, 0.0, 1.0).astype(F32)
    keep_right = jnp.where(gx == lax.axis_size("gx") - 1, 0.0, 1.0).astype(F32)

    wf, wc, af, ac, cf, cc, rz = {}, {}, {}, {}, {}, {}, {}

    def keep(kind, f, x, own):
        tile = extended((kind, f, x), own)
        if f < 3:
            (wf if kind == "f" else wc)[f, x] = tile
        elif f < 6:
            (af if kind == "f" else ac)[f - 3, x] = tile
        elif f < 8:
            (cf if kind == "f" else cc)[f - 6, x] = tile
        else:
            rz[x] = tile

    for f in range(9):
        for x in range(4):
            keep("f", f, x, own_f[4 * f + x])
    for f in range(8):
        for x in range(2):
            keep("c", f, x, own_c[2 * f + x])
    for side in range(2):

        def col(ring):
            return 3 + ring if side else -ring

        for c in range(3):
            keep("f", c, col(1), x_rows(side, ("f", c, 1)))
            for x in range(2):
                keep("c", c, (2 if side else -2) + x, x_rows(side, ("c", c, x)))
        for f in range(3, 8):
            keep("f", f, col(1), x_rows(side, ("f", f, 1)))
            keep("c", f, 2 if side else -1, x_rows(side, ("c", f, None)))
        bits = extended(("bits", side), x_rows(side, "bits"))
        for c in range(3):
            for r in range(2):
                wf[c, col(3 + r)] = lane_roll(bits, 126 - 4 * c - 2 * r)
            wf[c, col(2)] = lane_roll(bits, 107 - 2 * c)
            af[c, col(2)] = lane_roll(bits, 115 - c)
        for t in range(2):
            cf[t, col(2)] = lane_roll(bits, 112 - t)
            rz[col(1 + t)] = jnp.broadcast_to(bits[:, 17 + t : 18 + t], (16, LANES))

    def prolong(field, c, x):
        cx = x // 2
        tile = 0.75 * field[c, cx] + 0.25 * field[c, cx + 1 if x % 2 else cx - 1]
        at = slot()
        scr[at, pl.ds(0, 8, stride=2), :] = 0.75 * tile + 0.25 * row_roll(tile, 1)
        scr[at, pl.ds(1, 8, stride=2), :] = 0.75 * tile + 0.25 * row_roll(tile, -1)
        out = scr[at] * keep_y
        return out * keep_left if x < 0 else out * keep_right if x > 3 else out

    crosses = (row == 0) | (row == 7) | (row == 8) | (row == 15)
    across = []
    for side in range(2):
        given_dy, given_dz = {}, {}
        for c in range(2):
            k = 2 * side + c
            src, at = X_AT["edge"][0] + 2 * c, Y_AT["edge", side, c][0]
            ext_e[k] = jnp.zeros((16, LANES), F32)
            ext_e[k, 0:1] = hx[side, src : src + 1]
            ext_e[k, 7:8] = hx[side, src + 1 : src + 2]
            ext_e[k, 8:9] = hy[1, at : at + 1]
            ext_e[k, 15:16] = hy[0, at : at + 1]
            tile = ext_e[k]
            given_dy[c] = jnp.where(crosses, row_roll(tile, -1) - row_roll(tile, 1), 0.0)
        for c in (0, 2):
            tile = 0.75 * wc[c, 2 if side else -1] + 0.25 * wc[c, 3 if side else -2]
            at = slot()
            scr[at, pl.ds(0, 8, stride=2), :] = 0.25 * row_roll(tile, 1)
            scr[at, pl.ds(1, 8, stride=2), :] = 0.25 * row_roll(tile, -1)
            given_dz[c] = jnp.where(crosses & (lane_f == LANES - 1), lane_roll(scr[at], -1), 0.0)
        across.append((5 if side else -2, given_dy, given_dz))

    def restrict(field, c, cx):
        at = slot()
        scr[at] = field[c, 2 * cx] + field[c, 2 * cx + 1]
        return 0.25 * (scr[at, pl.ds(0, 8, stride=2), :] + scr[at, pl.ds(1, 8, stride=2), :])

    def neighbours(fine, coarse, reach_f, reach_c):
        zp_f, zm_f, zp_c, zm_c = {}, {}, {}, {}
        for c in range(3):
            for x in reach_f:
                tile = fine[c, x]
                zp_f[c, x] = jnp.where(lane_f == LANES - 1, lane_roll(prolong(coarse, c, x), -1), lane_roll(tile, -1))
                zm_f[c, x] = jnp.where(lane_f == 0, tile, lane_roll(tile, 1))
            for x in reach_c:
                tile = coarse[c, x]
                zp_c[c, x] = jnp.where(lane_c == LANES - 1, 0.0, lane_roll(tile, -1))
                zm_c[c, x] = jnp.where(lane_c == 0, lane_roll(restrict(fine, c, x), 1), lane_roll(tile, 1))
        return zp_f, zm_f, zp_c, zm_c

    zp_f, zm_f, zp_c, zm_c = neighbours(wf, wc, range(-3, 7), range(-2, 4))
    wf1, wc1 = {}, {}
    for x in range(-2, 6):
        given = {-1: across[0], 4: across[1]}.get(x, (None, None, None))
        lap, grad = operator(wf, zp_f, zm_f, x, 4.0, 1.0, 0.5 * rz[x], rz[x] * rz[x], given)
        for c in range(3):
            wf1[c, x] = af[c, x] + cf[0, x] * lap[c] + cf[1, x] * grad[c]
    for x in range(-1, 3):
        lap, grad = operator(wc, zp_c, zm_c, x, 1.0, 0.25, 0.25, 1.0)
        for c in range(3):
            wc1[c, x] = ac[c, x] + cc[0, x] * lap[c] + cc[1, x] * grad[c]

    zp_f, zm_f, zp_c, zm_c = neighbours(wf1, wc1, range(-1, 5), range(-1, 3))

    def finish(w1, lap, grad, c0, c1, u_r, m_r, q_r, om_r, u_out, m_out, x, tall):
        u = [u_r[c, x] for c in range(3)]
        om = [om_r[l, x] for l in range(3)]
        mem = [[m_r[l, c, x] for c in range(3)] for l in range(3)]
        _, nxt, new = relax(u, mem, [q_r[l, x] for l in range(3)], om)
        for c in range(3):
            u1 = w1[c, x][0:tall] + new[c]
            u_out[c, x] = 2.0 * u1 - u[c] + (c0 * lap[c] + c1 * grad[c])[0:tall]
            for l in range(3):
                m_out[l, c, x] = nxt[l][c] + DT * om[l] * (u1 - nxt[l][c])

    for x in range(4):
        lap, grad = operator(wf1, zp_f, zm_f, x, 4.0, 1.0, 0.5 * rz[x], rz[x] * rz[x])
        finish(wf1, lap, grad, cf[0, x], cf[1, x], uf, mf, qf, omf, uf_out, mf_out, x, 8)
    for x in range(2):
        lap, grad = operator(wc1, zp_c, zm_c, x, 1.0, 0.25, 0.25, 1.0)
        finish(wc1, lap, grad, cc[0, x], cc[1, x], uc, mc, qc, omc, uc_out, mc_out, x, 4)


SCRATCH = 3 * (10 + 6 + 6 + 4) + 4


SEAM = 12


def inner_before(gx, gy):
    return (gx % SEAM < SEAM - 2) | ((gy >= -(-5 * lax.axis_size("gy") // 8)) & (gy % 2 == 1))


def x_inner(value, before):
    ny = lax.axis_size("gy")
    pairs = []
    for i in range(0, lax.axis_size("gx") - 1, 2):
        for j in range(ny):
            if bool(inner_before(i, j)) == before:
                pairs += [(i * ny + j, (i + 1) * ny + j), ((i + 1) * ny + j, i * ny + j)]
    return lax.ppermute(value, ("gx", "gy"), pairs)


def swap(value, axis, first):
    pairs = []
    for i in range(first, lax.axis_size(axis) - 1, 2):
        pairs += [(i, i + 1), (i + 1, i)]
    return lax.ppermute(value, axis, pairs)


def gather_pairs(value, axis, first):
    nx, ny = lax.axis_size("gx"), lax.axis_size("gy")
    size, other = (nx, ny) if axis == "gx" else (ny, nx)

    def flat(i, k):
        return i * ny + k if axis == "gx" else k * ny + i

    groups = [[flat(i, k), flat(i + 1, k)] for k in range(other) for i in range(first, size - 1, 2)]
    if first:
        groups += [[flat(i, k), flat(i, k + 1)] for i in (0, size - 1) for k in range(0, other, 2)]
    return lax.all_gather(value, ("gx", "gy"), axis_index_groups=sorted(groups), tiled=True)


def call(kernel, shapes, scratch=(), first=False, last=False):
    vmem = pl.BlockSpec(memory_space=pltpu.VMEM)

    def run(*args):
        if not first:
            args = [pltpu.with_memory_space_constraint(a, pltpu.VMEM) for a in args]
        return pl.pallas_call(
            kernel,
            out_shape=[(jax.ShapeDtypeStruct if last else pltpu.VMEM)(s, F32) for s in shapes],
            in_specs=[vmem] * len(args),
            out_specs=[vmem] * len(shapes),
            scratch_shapes=list(scratch),
        )(*args)

    return run


def shards(
    u_now_c,
    u_prev_c,
    memory_c,
    mu_c,
    lam_c,
    rho_c,
    q_c,
    omega_c,
    u_now_f,
    u_prev_f,
    memory_f,
    mu_f,
    lam_f,
    rho_f,
    q_f,
    omega_f,
    stretch_f,
):
    inner, outer, own_f, own_c = call(
        pre_kernel,
        [(X_ROWS, LANES)] * 2 + [(36, 8, LANES), (16, 4, LANES)],
        [pltpu.VMEM((3, 8, LANES), F32), pltpu.VMEM((3, 8, LANES), F32)],
        first=True,
    )(
        u_now_c, u_prev_c, memory_c, mu_c, lam_c, rho_c, q_c, omega_c,
        u_now_f, u_prev_f, memory_f, mu_f, lam_f, rho_f, q_f, omega_f, stretch_f,
    )
    before = x_inner(inner, True)
    both = gather_pairs(outer, "gx", 1)
    both, inner = lax.optimization_barrier((both, inner))
    after = x_inner(inner, False)
    out2, out1, halo = call(mid_kernel, [(Y_ROWS, LANES)] * 2 + [(2, X_ROWS, LANES)])(own_f, own_c, before, both, after)
    y2 = swap(out2, "gy", 1)
    y1 = gather_pairs(out1, "gy", 0)
    return tuple(
        call(
            post_kernel,
            [u_now_c.shape, u_now_f.shape, memory_c.shape, memory_f.shape],
            [
                pltpu.VMEM((2, Y_ROWS, LANES), F32),
                pltpu.VMEM((len(Y_F), 16, LANES), F32),
                pltpu.VMEM((len(Y_C), 8, LANES), F32),
                pltpu.VMEM((4, 16, LANES), F32),
                pltpu.VMEM((SCRATCH, 16, LANES), F32),
            ],
            last=True,
        )(own_f, own_c, halo, y2, y1, u_now_c, memory_c, q_c, omega_c, u_now_f, memory_f, q_f, omega_f)
    )


def solution(mesh):
    def level(*lead):
        return P(*lead, "gx", "gy", None)

    inputs = (level(None), level(None), level(None, None), level(), level(), level(), level(None), level(None))
    return jax.shard_map(
        shards,
        mesh=mesh,
        in_specs=inputs + inputs + (P("gx", "gy"),),
        out_specs=(level(None), level(None), level(None, None), level(None, None)),
        check_vma=False,
    )
```
